128 devices in a mesh: gx: 16 (over y, z), gy: 8 (over x, core).
Axes of the slice: x: 4, y: 4, z: 4, core: 2. Of those that a mesh axis runs over, the one named last changes fastest.
Arguments:
- snapshots: bfloat16 [16, 16, 4, 2048, 512], P('gx', 'gy'), may hold values from -120 to 120
- basis: bfloat16 [16, 16, 4, 24, 2048], P('gx', 'gy'), may hold values from -0.0625 to 0.0625
- node_counts: int32 [16, 16], P('gx', 'gy'), may hold values from 1024 to 2048, as said below
- adjacency: int32 [16, 16, 3], P('gx', 'gy'), may hold values from 0 to 255, as said below
Outputs:
- operator: float32 [16, 16, 397, 24], P('gx', 'gy')
- reduced_states: float32 [16, 16, 24, 512], P('gx', 'gy')
The draws below stay inside these ranges and needn't reach their ends.
Inputs may be any that keep to these rules, and one draw needn't show every extreme that they name: Node slot n of subdomain g is live iff n < node_counts[g]; at least 1024 slots are live, and one subdomain has all 2048 live. Subdomain (row, col) has id row * 16 + col. Each row of adjacency holds 3 distinct ids other than its own subdomain's, each within one subdomain row and one subdomain column of it.
All inputs are finite; a program needn't handle non-finite values.
Results may differ from the reference program's by a relative error of at most 0.0003.
Values sent between devices are 32-bit elements; how exact they have to be, the bound alone decides.
No kernel may reach another device: no remote copies, remote signals or barrier semaphores. Data moves between devices by JAX's collectives and lax.ppermute only.
A program may use at most 64 MiB of HBM per device.

```python
import jax
import jax.numpy as jnp
import numpy as np
from jax import lax

R = 24
NVAR = 4
K = 512
P_SIZE = 2048
NB = 3
GRID_R = 16
GRID_C = 16
NF = 397


def draw_node_counts(key, part):
    first, second = jax.random.split(jax.random.fold_in(key, 11))
    counts = jax.random.randint(first, (GRID_R * GRID_C,), P_SIZE // 2, P_SIZE + 1, dtype=jnp.int32)
    where_full = jax.random.randint(second, (), 0, GRID_R * GRID_C, dtype=jnp.int32)
    counts = jnp.where(jnp.arange(GRID_R * GRID_C, dtype=jnp.int32) == where_full, P_SIZE, counts)
    return counts.reshape(GRID_R, GRID_C).astype(jnp.int32)


def draw_adjacency(key, part):
    offsets = np.array([(a, b) for a in range(-1, 2) for b in range(-1, 2)], dtype=np.int32)
    rows = jnp.arange(GRID_R, dtype=jnp.int32)[:, None, None]
    cols = jnp.arange(GRID_C, dtype=jnp.int32)[None, :, None]
    near_rows = jnp.broadcast_to(rows + jnp.asarray(offsets[:, 0]), (GRID_R, GRID_C, 9))
    near_cols = jnp.broadcast_to(cols + jnp.asarray(offsets[:, 1]), (GRID_R, GRID_C, 9))
    inside = (near_rows >= 0) & (near_rows < GRID_R) & (near_cols >= 0) & (near_cols < GRID_C)
    itself = (near_rows == rows) & (near_cols == cols)
    scores = jax.random.randint(jax.random.fold_in(key, 13), (GRID_R, GRID_C, 9), 0, 1000, dtype=jnp.int32) * 16 + jnp.arange(9, dtype=jnp.int32)
    scores = jnp.where(inside & jnp.logical_not(itself), scores, -1)
    unused, picked = lax.top_k(scores, NB)
    chosen_rows = jnp.take_along_axis(near_rows, picked, axis=2)
    chosen_cols = jnp.take_along_axis(near_cols, picked, axis=2)
    return (chosen_rows * GRID_C + chosen_cols).astype(jnp.int32)


def draw_snapshots(key, part):
    keys = jax.random.split(jax.random.fold_in(key, 17), 3)
    shape = (GRID_R, GRID_C, NVAR, P_SIZE, K)
    ident = jnp.arange(GRID_R * GRID_C, dtype=jnp.float32).reshape(GRID_R, GRID_C) / max(GRID_R * GRID_C - 1, 1)
    var_scale = jnp.exp(jax.random.uniform(keys[0], (NVAR,), jnp.float32, jnp.log(0.5), jnp.log(4.0)))
    rough = jax.random.uniform(keys[1], (GRID_R, GRID_C, NVAR, P_SIZE, 1), jnp.float32, 0.5, 1.5)
    base = jnp.clip(jax.random.normal(keys[2], shape, jnp.float32), -6.0, 6.0)
    rise = 1.0 + 2.0 * ident
    values = base * rough * var_scale[None, None, :, None, None] * rise[:, :, None, None, None]
    return values.astype(jnp.bfloat16)


def shard_levels(rng, shape, shards, least, top_value):
    loudness, own = 1.0, jax.random.fold_in(rng, 6)
    for position, parts in shards:
        steps = jnp.exp(jax.random.uniform(jax.random.fold_in(own, position), (parts,), jnp.float32, least / len(shards), top_value / len(shards)))
        loudness = loudness * jnp.repeat(steps, shape[position] // parts).reshape([-1 if axis == position else 1 for axis in range(len(shape))])
    return loudness


def gaussian(own_key, shape, deviation, reach, cuts=(), kind=jnp.bfloat16):
    result = jax.random.normal(own_key, shape, jnp.float32) * deviation
    if len(cuts) > 0:
        result = shard_levels(own_key, shape, cuts, -0.22, 0.18) * result
    return jnp.clip(result, min=-reach, max=reach).astype(kind)


def setup_inputs(seed: int = 0) -> dict:
    seeds = jax.random.split(jax.random.key(seed), 5)
    return {
        "snapshots": draw_snapshots(jax.random.fold_in(seeds[4], 71), 0),
        "basis": gaussian(seeds[1], (GRID_R, GRID_C, NVAR, R, P_SIZE), (NVAR * P_SIZE) ** -0.5, 0.0625, ((0, 16), (1, 8))),
        "node_counts": draw_node_counts(jax.random.fold_in(seeds[4], 71), 0),
        "adjacency": draw_adjacency(jax.random.fold_in(seeds[4], 71), 0),
    }


beta_linear = 0.5
beta_quad = 0.5

def project_one(items):
    values, modes, count = items
    live = (jnp.arange(values.shape[1], dtype=jnp.int32) < count).astype(jnp.float32)
    masked = modes.astype(jnp.float32) * live[None, None, :]
    proj = jnp.einsum('vrp,vpk->vrk', masked, values.astype(jnp.float32), precision=lax.Precision.HIGHEST)
    valf = values.astype(jnp.float32)
    squares = lax.optimization_barrier(jnp.sum(valf * valf * live[None, :, None], axis=(1, 2)))
    return (proj, squares)

def build_features(state, near):
    ranks = state.shape[0]
    steps = state.shape[1]
    pieces = [jnp.ones((1, steps), jnp.float32), state, near.reshape(-1, steps)]
    for first in range(ranks):
        pieces.append(state[first:first + 1] * state[first:])
    return jnp.concatenate(pieces, axis=0)

def fit_one(state, near, reg_diag):
    feats = build_features(state, near)
    past = feats[:, :-1]
    gram = jnp.dot(past, past.T, precision=lax.Precision.HIGHEST) + jnp.diag(reg_diag)
    rhs = jnp.dot(past, state[:, 1:].T, precision=lax.Precision.HIGHEST)
    factor = jnp.linalg.cholesky(gram)
    middle = jax.scipy.linalg.solve_triangular(factor, rhs, lower=True)
    return jax.scipy.linalg.solve_triangular(factor, middle, lower=True, trans=1)

def reference(snapshots, basis, node_counts, adjacency):
    grid_rows, grid_cols = (snapshots.shape[0], snapshots.shape[1])
    total = grid_rows * grid_cols
    values = snapshots.reshape(total, NVAR, P_SIZE, K)
    modes = basis.reshape(total, NVAR, R, P_SIZE)
    counts = node_counts.reshape(total).astype(jnp.int32)
    proj, squares = lax.map(project_one, (values, modes, counts))
    nodes = jnp.sum(counts.astype(jnp.float32))
    scale = jnp.sqrt(lax.optimization_barrier(jnp.sum(squares, axis=0)) / (nodes * K) + 1e-06)
    states = lax.optimization_barrier(jnp.sum(proj / scale[None, :, None, None], axis=1))
    gnorm = jnp.sum(states * states) / (total * R * K)
    near = states[adjacency.reshape(total, NB).astype(jnp.int32)]
    nlin = 1 + R + NB * R
    nquad = R * (R + 1) // 2
    reg_diag = K * jnp.concatenate([jnp.full((nlin,), beta_linear, jnp.float32) * gnorm, jnp.full((nquad,), beta_quad, jnp.float32) * gnorm * gnorm])
    operator = lax.map(lambda items: fit_one(items[0], items[1], reg_diag), (states, near))
    return (operator.reshape(grid_rows, grid_cols, NF, R), states.reshape(grid_rows, grid_cols, R, K))
```

```python
import jax
import jax.numpy as jnp
from jax import lax
from jax.experimental import pallas as pl
from jax.experimental.pallas import tpu as pltpu
from jax.sharding import Mesh
from jax.sharding import PartitionSpec as P

GX = ("gx_0", "gx_1")
GY = ("gy_0", "gy_1")
GX_GY = ("gx_0", "gx_1", "gy_0", "gy_1")

R = 24
NVAR = 4
K = 512
SLOTS = 2048
COLS = 2
NB = 3
NF = 397
HALF = 0.5
F32 = jnp.float32
HI = lax.Precision.HIGHEST


def iotas(shape):
    return lax.broadcasted_iota(jnp.int32, shape, 0), lax.broadcasted_iota(jnp.int32, shape, 1)


def local_kernel(counts, basis, snaps, proj, stats, acc):
    s = pl.program_id(0)
    v = pl.program_id(1)
    count = counts[s]

    @pl.when((s == 0) & (v == 0))
    def _():
        acc[...] = jnp.zeros_like(acc)

    lane = lax.broadcasted_iota(jnp.int32, (R, SLOTS), 1)
    modes = jnp.where(lane < count, basis[0, 0], jnp.zeros((), jnp.bfloat16))
    proj[s, v] = jnp.dot(modes, snaps[0, 0], preferred_element_type=F32)

    step = 64

    def tile_sum(x):
        x = x * x
        return jnp.sum(x.reshape(step // 8, 8, K), axis=0)

    def full(i, part):
        return part + tile_sum(snaps[0, 0, pl.ds(i * step, step), :].astype(F32))

    whole = count // step
    part = lax.fori_loop(0, whole, full, jnp.zeros((8, K), F32))
    edge = jnp.minimum(whole, SLOTS // step - 1)
    row = lax.broadcasted_iota(jnp.int32, (step, K), 0) + edge * step
    keep = (row < count) & (row >= whole * step)
    last = snaps[0, 0, pl.ds(pl.multiple_of(edge * step, step), step), :].astype(F32)
    part = part + tile_sum(jnp.where(keep, last, 0.0))
    part = part[:, 0:128] + part[:, 128:256] + part[:, 256:384] + part[:, 384:512]
    acc[v] += part

    @pl.when(v == NVAR - 1)
    def _():
        q = NVAR
        for a in range(NVAR):
            pa = proj[s, a]
            for b in range(a, NVAR):
                prod = pa * proj[s, b]
                t = prod[:, 0:128] + prod[:, 128:256] + prod[:, 256:384] + prod[:, 384:512]
                acc[q] += t[0:8] + t[8:16] + t[16:24]
                q += 1

    @pl.when((s == COLS - 1) & (v == NVAR - 1))
    def _():
        rows = jnp.sum(acc[...], axis=1)
        total = jnp.sum(rows, axis=1, keepdims=True)
        i, j = iotas((16, 128))
        flat = jnp.sum(jnp.where(i == j, total, 0.0), axis=0, keepdims=True)
        nodes = (counts[0] + counts[1]).astype(F32)
        _, lane1 = iotas((1, 128))
        stats[...] = jnp.where(lane1 == 14, nodes, flat)


def local_pass(snapshots, basis, counts):
    return pl.pallas_call(
        local_kernel,
        grid_spec=pltpu.PrefetchScalarGridSpec(
            num_scalar_prefetch=1,
            grid=(COLS, NVAR),
            in_specs=[
                pl.BlockSpec((1, 1, R, SLOTS), lambda s, v, c: (s, v, 0, 0)),
                pl.BlockSpec((1, 1, SLOTS, K), lambda s, v, c: (s, v, 0, 0)),
            ],
            out_specs=[
                pl.BlockSpec((COLS, NVAR, R, K), lambda s, v, c: (0, 0, 0, 0)),
                pl.BlockSpec((1, 128), lambda s, v, c: (0, 0)),
            ],
            scratch_shapes=[pltpu.VMEM((16, 8, 128), F32)],
        ),
        out_shape=[
            jax.ShapeDtypeStruct((COLS, NVAR, R, K), F32),
            jax.ShapeDtypeStruct((1, 128), F32),
        ],
        compiler_params=pltpu.CompilerParams(dimension_semantics=("arbitrary", "arbitrary")),
        name="local",
    )(counts, basis, snapshots)


def states_kernel(everyone, proj, states, gnorm):
    total = jnp.sum(everyone[...], axis=0, keepdims=True)
    nodes = total[:, 14:15]
    inv = []
    for v in range(NVAR):
        scale = jnp.sqrt(total[:, v : v + 1] / (nodes * K) + 1e-06)
        inv.append(1.0 / scale)
    g = jnp.zeros((1, 1), F32)
    q = NVAR
    for a in range(NVAR):
        for b in range(a, NVAR):
            term = total[:, q : q + 1] * inv[a] * inv[b]
            g = g + (term if a == b else 2.0 * term)
            q += 1
    gnorm[...] = jnp.broadcast_to(g * (1.0 / (256 * R * K)), (1, 128))
    for s in range(COLS):
        t = proj[s, 0] * inv[0]
        for v in range(1, NVAR):
            t = t + proj[s, v] * inv[v]
        states[s] = t


def global_states(everyone, proj):
    return pl.pallas_call(
        states_kernel,
        out_shape=[
            jax.ShapeDtypeStruct((COLS, R, K), F32),
            jax.ShapeDtypeStruct((1, 128), F32),
        ],
        name="states",
    )(everyone, proj)


LAST = 16
PADDED = 400
NQ = 288
FUT = 384
TAIL = FUT + R
WIDTH = 512


def place(row):
    return row if row < FUT else row + R


def invert_rows(block, tiles, first):
    sub, lane = iotas((8, 128))
    for p in range(tiles):
        base = first + 8 * p
        inside = (lane >= base) & (lane < base + 8)
        unit = jnp.where(lane - base == sub, 1.0, 0.0)
        for m in range(COLS):
            tile = block[m, 8 * p : 8 * p + 8, :]
            col = [jnp.broadcast_to(tile[:, base + k : base + k + 1], (8, 128)) for k in range(8)]
            x = jnp.where(inside, unit, tile)
            recips = jnp.zeros((8, 128), F32)
            for j in range(8):
                r = 1.0 / jnp.broadcast_to(col[j][j : j + 1, :], (8, 128))
                mult = jnp.where(sub == j, 0.0, col[j] * r)
                recips = jnp.where(sub == j, r, recips)
                for k in range(j + 1, 8):
                    col[k] = col[k] - mult * jnp.broadcast_to(col[k][j : j + 1, :], (8, 128))
                x = x - mult * jnp.broadcast_to(x[j : j + 1, :], (8, 128))
            w = x * recips
            block[m, 8 * p : 8 * p + 8, :] = w
            wb = [jnp.broadcast_to(w[j : j + 1, :], (8, 128)) for j in range(8)]
            for t in [t % tiles for t in range(p + 1, p + tiles)]:
                a = block[m, 8 * t : 8 * t + 8, :]
                terms = [jnp.broadcast_to(a[:, base + j : base + j + 1], (8, 128)) * wb[j] for j in range(8)]
                while len(terms) > 1:
                    terms = [terms[i] + terms[i + 1] for i in range(0, len(terms), 2)]
                block[m, 8 * t : 8 * t + 8, :] = jnp.where(inside, 0.0, a) - terms[0]


def mm(a, b):
    return lax.dot_general(a, b, (((1,), (0,)), ((), ())), precision=HI, preferred_element_type=F32)


def fit_kernel(links, gnorm, own, up, down, left, right, out, near, twice, feats, h, block):
    near[0, 1] = up[0]
    near[0, 2] = up[1]
    near[1, 1] = own[0]
    near[1, 2] = own[1]
    near[2, 1] = down[0]
    near[2, 2] = down[1]
    for i in range(3):
        near[i, 0] = left[i]
        near[i, 3] = right[i]
    _, lane = iotas((8, K))
    keep = lane < K - 1
    keep24 = jnp.concatenate([keep] * 3, axis=0)
    for m in range(COLS):
        s = own[m]
        past = jnp.where(keep24, s, 0.0)
        twice[0:R] = past
        twice[R : 2 * R] = past
        for d in range(12):
            feats[m, R * d : R * d + R] = past * twice[d : d + R]
        feats[m, NQ : NQ + R] = past
        row, lane16 = iotas((16, K))
        one = jnp.where((row == 12) & (lane16 < K - 1), 1.0, 0.0)
        feats[m, 312:328] = jnp.where(row < 12, twice[0:16] * twice[12:28], one)
        for b in range(NB):
            block_id = links[m * NB + b]
            v = jnp.where(keep24, near[block_id // 4, block_id % 4], 0.0)
            if b < 2:
                feats[m, 328 + R * b : 328 + R * b + R] = v
            else:
                feats[m, 376:384] = v[0:8]
                feats[m, TAIL : TAIL + 16] = v[8:24]
        feats[m, FUT:TAIL] = pltpu.roll(s, K - 1, 1)
    g = gnorm[...]
    lin = K * (HALF * g)
    quad = K * (HALF * g * g)
    sub, lane = iotas((8, 128))
    for m in range(COLS):
        rhs = feats[m]
        for lo, size, dst in ((0, 384, 0), (TAIL, LAST, FUT)):
            prod = lax.dot_general(
                feats[m, lo : lo + size], rhs, (((1,), (1,)), ((), ())), precision=HI, preferred_element_type=F32
            )
            h[m, dst : dst + size, 0:424] = prod
            h[m, dst : dst + size, 424:512] = jnp.zeros((size, 88), F32)
        for t in range(PADDED // 8):
            row = 8 * t
            if row < NQ:
                reg = quad
            elif row == 312:
                reg = quad
            elif row == 320:
                reg = jnp.where(sub < 4, quad, jnp.where(sub == 4, lin, 1.0))
            else:
                reg = lin
            where = place(row)
            cb = where // 128 * 128
            cell = h[m, row : row + 8, cb : cb + 128]
            h[m, row : row + 8, cb : cb + 128] = cell + jnp.where(lane == sub + (where - cb), reg, 0.0)
        block[m] = h[m, 0:128, 0:128]

    def step(p, carry):
        invert_rows(block, 16, 0)
        for k in range(3):

            @pl.when(p == k)
            def _():
                lo = 128 * k
                hi = lo + 128
                for m in range(COLS):
                    w = mm(block[m], h[m, lo:hi, hi:WIDTH])
                    for a, b in ((0, lo), (hi, PADDED)):
                        if a < b:
                            h[m, a:b, hi:WIDTH] = h[m, a:b, hi:WIDTH] - mm(h[m, a:b, lo:hi], w)
                    h[m, lo:hi, hi:WIDTH] = w
                    if k < 2:
                        block[m] = h[m, hi : hi + 128, hi : hi + 128]
                    else:
                        block[m, 0:LAST] = h[m, FUT:PADDED, FUT:WIDTH]

        return carry

    lax.fori_loop(0, 3, step, 0)
    invert_rows(block, 2, R)
    for m in range(COLS):
        x = block[m, 0:LAST]
        top = h[m, 0:FUT, FUT:WIDTH]
        h[m, 0:FUT, FUT:WIDTH] = top - mm(top[:, R : R + LAST], x)
        h[m, FUT:PADDED, FUT:WIDTH] = x
        out[m, 0:1] = h[m, 324:325, FUT : FUT + R]
        out[m, 1:25] = h[m, NQ : NQ + R, FUT : FUT + R]
        out[m, 25:97] = h[m, 328:400, FUT : FUT + R]
        dst = 97
        for a in range(R):
            for b in range(a, R):
                d = b - a
                if d == 12:
                    src = 312 + a
                elif d < 12:
                    src = R * d + a
                else:
                    src = R * (R - d) + b
                out[m, dst : dst + 1] = h[m, src : src + 1, FUT : FUT + R]
                dst += 1


def fit(links, gnorm, own, up, down, left, right):
    vm = pl.BlockSpec(memory_space=pltpu.VMEM)
    return pl.pallas_call(
        fit_kernel,
        in_specs=[pl.BlockSpec(memory_space=pltpu.SMEM)] + [vm] * 6,
        out_specs=vm,
        out_shape=jax.ShapeDtypeStruct((COLS, NF, R), F32),
        scratch_shapes=[
            pltpu.VMEM((3, 4, R, K), F32),
            pltpu.VMEM((2 * R, K), F32),
            pltpu.VMEM((COLS, 424, K), F32),
            pltpu.VMEM((COLS, PADDED, WIDTH), F32),
            pltpu.VMEM((COLS, 128, 128), F32),
        ],
        name="fit",
    )(links, gnorm, own, up, down, left, right)


def shifts(axis, x, y):
    n = lax.axis_size(axis)
    return (
        lax.ppermute(x, axis, [(i, i + 1) for i in range(n - 1)]),
        lax.ppermute(y, axis, [(i + 1, i) for i in range(n - 1)]),
    )


def body(snapshots, basis, node_counts, adjacency):
    counts = node_counts[0]
    links = adjacency[0]
    proj, stats = local_pass(snapshots[0], basis[0], counts)
    near_row = links // 16
    near_col = links % 16
    local = (near_row - lax.axis_index(GX) + 1) * 4 + (near_col - lax.axis_index(GY) * COLS + 1)
    everyone = lax.all_to_all(jnp.broadcast_to(stats[None], (128, 1, 128)), GX_GY, 0, 0)
    states, gnorm = global_states(everyone.reshape(128, 128), proj)
    up, down = shifts(GX, states, states)
    right_edge = jnp.stack([up[1], states[1], down[1]])
    left_edge = jnp.stack([up[0], states[0], down[0]])
    left, right = shifts(GY, right_edge, left_edge)
    operator = fit(local.reshape(-1), gnorm, states, up, down, left, right)
    return (operator[None], states[None])


def solution(mesh):
    split = Mesh(mesh.devices.reshape(4, 4, 4, 2), ("gx_0", "gx_1", "gy_0", "gy_1"))
    placed = (P(GX, GY, None, None, None), P(GX, GY, None, None, None), P(GX, GY), P(GX, GY, None))
    return jax.shard_map(
        body,
        mesh=split,
        in_specs=placed,
        out_specs=(P(GX, GY, None, None), P(GX, GY, None, None)),
        check_vma=False,
    )
```

```python
import jax
import jax.numpy as jnp
from jax import lax
from jax.experimental import pallas as pl
from jax.experimental.pallas import tpu as pltpu
from jax.sharding import Mesh
from jax.sharding import PartitionSpec as P

GX = ("gx_0", "gx_1")
GY = ("gy_0", "gy_1")
GX_GY = ("gx_0", "gx_1", "gy_0", "gy_1")

R = 24
NVAR = 4
K = 512
SLOTS = 2048
COLS = 2
NB = 3
NF = 397
HALF = 0.5
F32 = jnp.float32
BF = jnp.bfloat16
HI = lax.Precision.HIGHEST


def iotas(shape):
    return lax.broadcasted_iota(jnp.int32, shape, 0), lax.broadcasted_iota(jnp.int32, shape, 1)


def fold_lanes(x):
    return (x[:, 0:128] + x[:, 128:256]) + (x[:, 256:384] + x[:, 384:512])


def local_kernel(counts, basis, snaps, proj0, proj1, stats, acc):
    s = pl.program_id(0)
    v = pl.program_id(1)
    count = counts[s]

    @pl.when((s == 0) & (v == 0))
    def _():
        acc[...] = jnp.zeros_like(acc)

    lane = lax.broadcasted_iota(jnp.int32, (R, SLOTS), 1)
    modes = jnp.where(lane < count, basis[0, 0], jnp.zeros((), BF))
    prod = jnp.dot(modes, snaps[0, 0], preferred_element_type=F32)
    step = 128
    row = lax.broadcasted_iota(jnp.int32, (step, 128), 0)
    part = jnp.zeros((8, 128), F32)
    for lo in range(0, SLOTS, step):
        x = snaps[0, 0, lo : lo + step, :].astype(F32)
        t = jnp.where(row < count - lo, fold_lanes(x * x), 0.0)
        part = part + jnp.sum(t.reshape(step // 8, 8, 128), axis=0)
    acc[v] += part

    @pl.when(s == 0)
    def _():
        proj0[v] = prod

    @pl.when(s == 1)
    def _():
        proj1[v] = prod

    for sub, proj in ((0, proj0), (1, proj1)):

        @pl.when((s == sub) & (v == NVAR - 1))
        def _():
            q = NVAR
            for a in range(NVAR):
                pa = proj[a]
                for b in range(a, NVAR):
                    t = fold_lanes(pa * proj[b])
                    acc[q] += t[0:8] + t[8:16] + t[16:24]
                    q += 1

    @pl.when((s == COLS - 1) & (v == NVAR - 1))
    def _():
        rows = jnp.sum(acc[...], axis=1)
        total = jnp.sum(rows, axis=1, keepdims=True)
        i, j = iotas((16, 128))
        flat = jnp.sum(jnp.where(i == j, total, 0.0), axis=0, keepdims=True)
        nodes = (counts[0] + counts[1]).astype(F32)
        _, lane1 = iotas((1, 128))
        stats[...] = jnp.broadcast_to(jnp.where(lane1 == 14, nodes, flat), (128, 128))


def local_pass(snapshots, basis, counts):
    return pl.pallas_call(
        local_kernel,
        grid_spec=pltpu.PrefetchScalarGridSpec(
            num_scalar_prefetch=1,
            grid=(COLS, NVAR),
            in_specs=[
                pl.BlockSpec((1, 1, R, SLOTS), lambda s, v, c: (s, v, 0, 0)),
                pl.BlockSpec((1, 1, SLOTS, K), lambda s, v, c: (s, v, 0, 0)),
            ],
            out_specs=[
                pl.BlockSpec((NVAR, R, K), lambda s, v, c: (0, 0, 0)),
                pl.BlockSpec((NVAR, R, K), lambda s, v, c: (0, 0, 0)),
                pl.BlockSpec((128, 128), lambda s, v, c: (0, 0)),
            ],
            scratch_shapes=[pltpu.VMEM((16, 8, 128), F32)],
        ),
        out_shape=[
            jax.ShapeDtypeStruct((NVAR, R, K), F32),
            jax.ShapeDtypeStruct((NVAR, R, K), F32),
            jax.ShapeDtypeStruct((128, 128), F32),
        ],
        compiler_params=pltpu.CompilerParams(dimension_semantics=("arbitrary", "arbitrary")),
        name="local",
    )(counts, basis, snapshots)


def states_kernel(everyone, left, proj0, proj1, right, own, patch, gnorm):
    total = jnp.sum(everyone[...], axis=0, keepdims=True)
    nodes = total[:, 14:15]
    inv = []
    for v in range(NVAR):
        scale = jnp.sqrt(total[:, v : v + 1] / (nodes * K) + 1e-06)
        inv.append(1.0 / scale)
    g = jnp.zeros((1, 1), F32)
    q = NVAR
    for a in range(NVAR):
        for b in range(a, NVAR):
            term = total[:, q : q + 1] * inv[a] * inv[b]
            g = g + (term if a == b else 2.0 * term)
            q += 1
    gnorm[...] = jnp.broadcast_to(g * (1.0 / (256 * R * K)), (1, 128))
    for c, proj in enumerate((left, proj0, proj1, right)):
        t = proj[0] * inv[0]
        for v in range(1, NVAR):
            t = t + proj[v] * inv[v]
        patch[c] = t
        if c in (1, 2):
            own[c - 1] = t


def global_states(everyone, left, proj0, proj1, right):
    return pl.pallas_call(
        states_kernel,
        out_shape=[
            jax.ShapeDtypeStruct((COLS, R, K), F32),
            jax.ShapeDtypeStruct((4, R, K), F32),
            jax.ShapeDtypeStruct((1, 128), F32),
        ],
        name="states",
    )(everyone, left, proj0, proj1, right)


OWN = 328
NQ = 288
MIXED = 312
FUT = OWN
NEAR = 72
LANES = 384


def lane_copy(x, at):
    return jnp.take_along_axis(x, jnp.full((8, 128), at, jnp.int32), axis=1)


def sub_copy(x, j):
    return jnp.broadcast_to(x[j : j + 1, :], (8, 128))


def split3(x):
    h = x.astype(BF)
    r = x - h.astype(F32)
    m = r.astype(BF)
    return h, m, (r - m.astype(F32)).astype(BF)


def dot(a, b):
    return jnp.dot(a, b, preferred_element_type=F32)


def mm(a, b):
    return jnp.dot(a, b, precision=HI, preferred_element_type=F32)


def tree(terms):
    while len(terms) > 1:
        terms = [terms[i] + terms[i + 1] for i in range(0, len(terms) - 1, 2)] + terms[len(terms) // 2 * 2 :]
    return terms[0]


def padded_dot(a, w, lo):
    ah, am, al = split3(a)
    n = w.shape[0]
    parts = [jnp.zeros((lo, 128), F32)] * (lo > 0) + [w] + [jnp.zeros((128 - lo - n, 128), F32)] * (lo + n < 128)
    wh, wm, wl = split3(jnp.concatenate(parts, axis=0) if len(parts) > 1 else w)
    pair = jnp.concatenate([wh, wm], axis=1)
    u = dot(jnp.concatenate([ah, am], axis=1), jnp.concatenate([pair, pair], axis=0))
    v = dot(jnp.concatenate([ah, al], axis=1), jnp.concatenate([wl, wh], axis=0))
    return u[:, :128] + (u[:, 128:] + v)


def invert(block, tiles, strip=4, look=2):
    sub, lane = iotas((8, 128))
    for s in range(0, tiles, strip):
        own = list(range(s, min(s + strip, tiles)))
        ahead = list(range(s + strip, min(s + strip + look, tiles)))
        for p in own:
            base = 8 * p
            inside = (lane >= base) & (lane < base + 8)
            unit = jnp.where(lane - base == sub, 1.0, 0.0)
            ws = []
            for m in range(COLS):
                tile = block[m, base : base + 8, :]
                col = [lane_copy(tile, base + k) for k in range(8)]
                x = jnp.where(inside, unit, tile)
                recips = jnp.zeros((8, 128), F32)
                for j in range(8):
                    r = 1.0 / sub_copy(col[j], j)
                    mult = jnp.where(sub == j, 0.0, col[j]) * r
                    recips = jnp.where(sub == j, r, recips)
                    for k in range(j + 1, 8):
                        col[k] = col[k] - mult * sub_copy(col[k], j)
                    x = x - mult * sub_copy(x, j)
                w = x * recips
                block[m, base : base + 8, :] = w
                ws.append([sub_copy(w, j) for j in range(8)])
            for t in [t for t in own + ahead if t > p] + [t for t in own if t < p]:
                for m in range(COLS):
                    a = block[m, 8 * t : 8 * t + 8, :]
                    delta = tree([lane_copy(a, base + j) * ws[m][j] for j in range(8)])
                    block[m, 8 * t : 8 * t + 8, :] = jnp.where(inside, 0.0, a) - delta
            yield
        lo, hi = 8 * s, 8 * (own[-1] + 1)
        ranges = [(a, b) for a, b in ((hi + 8 * len(ahead), 8 * tiles), (0, lo)) if a < b]
        if ranges:
            for m in range(COLS):
                rest = [block[m, a:b, :] for a, b in ranges]
                rest = jnp.concatenate(rest, axis=0) if len(rest) > 1 else rest[0]
                _, wide = iotas(rest.shape)
                kept = jnp.where((wide >= lo) & (wide < hi), 0.0, rest)
                new = kept - padded_dot(rest, block[m, lo:hi, :], lo)
                at = 0
                for a, b in ranges:
                    block[m, a:b, :] = new[at : at + b - a]
                    at += b - a


def spread(panels, count, work):
    work = list(work)
    done = 0
    for i, _ in enumerate(panels):
        want = (i + 1) * len(work) // count if i + 1 < count else len(work)
        while done < min(want, len(work)):
            work[done]()
            done += 1
    for f in work[done:]:
        f()


def own_features(feats, twice, m, state, keep):
    past = jnp.where(keep, state, 0.0)
    twice[m, 0:R] = past
    twice[m, R : 2 * R] = past
    for d in range(12):
        feats(R * d, past * twice[m, d : d + R])
    feats(NQ, past)
    row, lane = iotas((16, K))
    one = jnp.where((row == 12) & (lane < K - 1), 1.0, 0.0)
    feats(MIXED, jnp.where(row < 12, twice[m, 0:16] * twice[m, 12:28], one))
    feats(FUT, pltpu.roll(state, K - 1, 1))


def ridge(gnorm):
    g = gnorm[...]
    return K * (HALF * g), K * (HALF * g * g)


def past_mask():
    return lax.broadcasted_iota(jnp.int32, (R, K), 1) < K - 1


def nt(a, b):
    return lax.dot_general(a, b, (((1,), (1,)), ((), ())), preferred_element_type=F32)


def own_kernel(gnorm, own, out, twice, fh, fm, fl, h, block):
    keep = past_mask()
    for m in range(COLS):

        def put(at, x, m=m):
            a, b, c = split3(x)
            n = x.shape[0]
            fh[m, at : at + n], fm[m, at : at + n], fl[m, at : at + n] = a, b, c

        own_features(put, twice, m, own[m], keep)
    lin, quad = ridge(gnorm)
    sub, lane = iotas((8, 128))

    def gram(m, r0, r1, c0, c1):
        a = [f[m, r0:r1] for f in (fh, fm, fl)]
        b = [f[m, c0:c1] for f in (fh, fm, fl)]
        g = ((nt(a[1], b[1]) + nt(a[0], b[2])) + nt(a[2], b[0])) + (nt(a[0], b[1]) + nt(a[1], b[0]))
        return g + nt(a[0], b[0])

    def reg(row):
        if row < NQ or row == MIXED:
            return quad
        if row == MIXED + 8:
            return jnp.where(sub < 4, quad, jnp.where(sub == 4, lin, 1.0))
        return lin

    def ridged(x, row0):
        tiles = []
        for i in range(x.shape[0] // 8):
            tiles.append(x[8 * i : 8 * i + 8] + jnp.where(lane == sub + 8 * i, reg(row0 + 8 * i), 0.0))
        return jnp.concatenate(tiles, axis=0)

    for m in range(COLS):
        block[m] = ridged(gram(m, 0, 128, 0, 128), 0)

    def piece(m, kind):
        def go():
            if kind == 0:
                h[m, 0:128, 128:256] = gram(m, 0, 128, 128, 256)
            elif kind == 1:
                h[m, 128:OWN, 0:128] = gram(m, 128, OWN, 0, 128)
            elif kind == 2:
                h[m, 128:256, 128:256] = ridged(gram(m, 128, 256, 128, 256), 128)
            elif kind == 3:
                h[m, 256:OWN, 128:256] = gram(m, 256, OWN, 128, 256)
            else:
                h[m, :, 256:LANES] = jnp.zeros((OWN, 128), F32)
                h[m, 0:256, 256 : OWN + R] = gram(m, 0, 256, 256, OWN + R)
                h[m, 256:OWN, 256 : OWN + R] = gram(m, 256, OWN, 256, OWN + R)
                h[m, 256:OWN, 256:LANES] = ridged(h[m, 256:OWN, 256:LANES], 256)

        return go

    spread(invert(block, 16), 14, [piece(m, k) for k in range(5) for m in range(COLS)])
    inv0 = [block[m] for m in range(COLS)]
    for m in range(COLS):
        w = mm(inv0[m], h[m, 0:128, 128:256])
        block[m] = h[m, 128:256, 128:256] - mm(h[m, 128:256, 0:128], w)
        h[m, 0:128, 128:256] = w
        h[m, 0:128, 0:128] = inv0[m]

    def after0(m, kind):
        def go():
            if kind == 0:
                h[m, 0:128, 256:LANES] = mm(h[m, 0:128, 0:128], h[m, 0:128, 256:LANES])
            elif kind == 1:
                rows = slice(128, OWN)
                h[m, rows, 256:LANES] -= mm(h[m, rows, 0:128], h[m, 0:128, 256:LANES])
            elif kind == 2:
                rows = slice(256, OWN)
                h[m, rows, 128:256] -= mm(h[m, rows, 0:128], h[m, 0:128, 128:256])
            else:
                rows = slice(128, OWN)
                h[m, rows, 0:128] = -mm(h[m, rows, 0:128], h[m, 0:128, 0:128])

        return go

    spread(invert(block, 16), 14, [after0(m, k) for k in range(4) for m in range(COLS)])
    for m in range(COLS):
        h[m, 128:256, 128:256] = block[m]
        w = mm(block[m], h[m, 128:256, 256:LANES])
        block[m, 0:NEAR] = h[m, 256:OWN, 256:LANES] - mm(h[m, 256:OWN, 128:256], w)
        h[m, 128:256, 256:LANES] = w

    def after1(m, kind):
        def go():
            if kind == 0:
                h[m, 128:256, 0:128] = mm(h[m, 128:256, 128:256], h[m, 128:256, 0:128])
            elif kind == 1:
                h[m, 0:128, 256:LANES] -= mm(h[m, 0:128, 128:256], h[m, 128:256, 256:LANES])
            elif kind == 2:
                for rows in (slice(0, 128), slice(256, OWN)):
                    h[m, rows, 0:128] -= mm(h[m, rows, 128:256], h[m, 128:256, 0:128])
            else:
                for rows in (slice(0, 128), slice(256, OWN)):
                    h[m, rows, 128:256] = -mm(h[m, rows, 128:256], h[m, 128:256, 128:256])

        return go

    spread(invert(block, 9), 8, [after1(m, k) for k in range(4) for m in range(COLS)])
    _, wide = iotas((256, 128))
    for m in range(COLS):
        last = block[m, 0:NEAR]
        w = mm(last[:, 0:NEAR], h[m, 256:OWN, 0:256])
        part = h[m, 0:256, 256:LANES]
        out[m, 0:256, 0:256] = h[m, 0:256, 0:256] - mm(part[:, 0:NEAR], w)
        out[m, 0:256, 256:LANES] = jnp.where(wide < NEAR, 0.0, part) - mm(part[:, 0:NEAR], last)
        out[m, 256:OWN, 0:256] = w
        out[m, 256:OWN, 256:LANES] = last


def fit_own(gnorm, own):
    return pl.pallas_call(
        own_kernel,
        out_shape=jax.ShapeDtypeStruct((COLS, OWN, LANES), F32),
        scratch_shapes=[
            pltpu.VMEM((COLS, 2 * R, K), F32),
            pltpu.VMEM((COLS, OWN + R, K), BF),
            pltpu.VMEM((COLS, OWN + R, K), BF),
            pltpu.VMEM((COLS, OWN + R, K), BF),
            pltpu.VMEM((COLS, OWN, LANES), F32),
            pltpu.VMEM((COLS, 128, 128), F32),
        ],
        name="fit_own",
    )(gnorm, own)


def near_kernel(adjacency, gnorm, mid, up, down, solved, out, twice, fh, fm, fl, near, block, x, order):
    row0 = lax.axis_index("gx_0") * 4 + lax.axis_index("gx_1")
    col0 = (lax.axis_index("gy_0") * 2 + lax.axis_index("gy_1")) * COLS
    for c in range(4):
        near[c] = up[c]
        near[4 + c] = mid[c]
        near[8 + c] = down[c]
    keep = past_mask()
    lin, _ = ridge(gnorm)
    sub, lane = iotas((8, 128))
    for m in range(COLS):

        def put(at, v, m=m):
            n = v.shape[0]
            fh[m, at : at + n], fm[m, at : at + n], fl[m, at : at + n] = split3(v)

        own_features(put, twice, m, mid[1 + m], keep)
        rows = []
        for b in range(NB):
            link = adjacency[0, m, b]
            at = ((link >> 4) - row0 + 1) * 4 + ((link & 15) - col0 + 1)
            rows.append(jnp.where(keep, near[at], 0.0))
        nh, nm, nl = split3(jnp.concatenate(rows, axis=0))
        thirds = jnp.concatenate([nh, nm, nl], axis=0)
        p = nt(fh[m], thirds)
        q = nt(fm[m], thirds[0 : 2 * NEAR])
        g = (p[:, 2 * NEAR : 3 * NEAR] + q[:, NEAR : 2 * NEAR] + nt(fl[m], nh)) + (p[:, NEAR : 2 * NEAR] + q[:, 0:NEAR])
        cross = g + p[:, 0:NEAR]
        p = nt(nh, thirds)
        q = nt(nm, thirds[0 : 2 * NEAR])
        g = (p[:, 2 * NEAR : 3 * NEAR] + q[:, NEAR : 2 * NEAR] + nt(nl, nh)) + (p[:, NEAR : 2 * NEAR] + q[:, 0:NEAR])
        square = g + p[:, 0:NEAR]
        wide = jnp.concatenate([cross, jnp.zeros((LANES - OWN - R, NEAR), F32)], axis=0)
        wide = jnp.concatenate([wide, jnp.zeros((LANES, 128 - NEAR), F32)], axis=1)
        turned = wide.T[0:NEAR]
        z = mm(solved[m, :, 0:256], cross[0:256]) + mm(solved[m, :, 256:OWN], cross[256:OWN])
        tail = solved[m, :, 256:LANES]
        _, lane_o = iotas((OWN, 128))
        z = jnp.concatenate([z, jnp.zeros((OWN, 128 - NEAR), F32)], axis=1)
        both = jnp.where(lane_o < NEAR, z, tail)
        x[m, 0:OWN] = both
        _, lane_n = iotas((NEAR, 128))
        square = jnp.concatenate([square, jnp.zeros((NEAR, 128 - NEAR), F32)], axis=1)
        start = jnp.where(lane_n < NEAR, square, turned[:, 256:LANES])
        start = jnp.where(lane_n < NEAR + R, start, 0.0)
        for i in range(NEAR // 8):
            rows8 = slice(8 * i, 8 * i + 8)
            block[m, rows8] = start[rows8] + jnp.where(lane == sub + 8 * i, lin, 0.0)
        block[m, 0:NEAR] = block[m, 0:NEAR] - mm(turned[:, 0:OWN], both)
    for _ in invert(block, 9):
        pass
    for m in range(COLS):
        last = block[m, 0:NEAR]
        both = x[m, 0:OWN]
        x[m, 0:OWN] = both - mm(both[:, 0:NEAR], last)
        x[m, OWN : OWN + NEAR] = last
        order[m, 0:1] = x[m, MIXED + 12 : MIXED + 13]
        order[m, 1:25] = x[m, NQ : NQ + R]
        order[m, 25:97] = last
        dst = 97
        for a in range(R):
            for b in range(a, R):
                d = b - a
                if d == 12:
                    src = MIXED + a
                elif d < 12:
                    src = R * d + a
                else:
                    src = R * (R - d) + b
                order[m, dst : dst + 1] = x[m, src : src + 1]
                dst += 1
        flat = order[m].T
        out[m] = flat[NEAR : NEAR + R, 0:NF]


def fit_near(adjacency, gnorm, mid, up, down, solved):
    vm = pl.BlockSpec(memory_space=pltpu.VMEM)
    return pl.pallas_call(
        near_kernel,
        in_specs=[pl.BlockSpec(memory_space=pltpu.SMEM)] + [vm] * 5,
        out_specs=vm,
        out_shape=jax.ShapeDtypeStruct((COLS, R, NF), F32),
        scratch_shapes=[
            pltpu.VMEM((COLS, 2 * R, K), F32),
            pltpu.VMEM((COLS, OWN + R, K), BF),
            pltpu.VMEM((COLS, OWN + R, K), BF),
            pltpu.VMEM((COLS, OWN + R, K), BF),
            pltpu.VMEM((12, R, K), F32),
            pltpu.VMEM((COLS, 128, 128), F32),
            pltpu.VMEM((COLS, OWN + NEAR, 128), F32),
            pltpu.VMEM((COLS, 512, 128), F32),
        ],
        name="fit_near",
    )(adjacency, gnorm, mid, up, down, solved)


def shifts(axis, x, y):
    n = lax.axis_size(axis)
    return (
        lax.ppermute(x, axis, [(i, i + 1) for i in range(n - 1)]),
        lax.ppermute(y, axis, [(i + 1, i) for i in range(n - 1)]),
    )


def body(snapshots, basis, node_counts, adjacency):
    proj0, proj1, stats = local_pass(snapshots[0], basis[0], node_counts[0])
    everyone = lax.all_to_all(stats, GX_GY, 0, 0, tiled=True)
    left, right = shifts(GY, proj1, proj0)
    own, mid, gnorm = global_states(everyone, left, proj0, proj1, right)
    up, down = shifts(GX, mid, mid)
    solved = fit_own(gnorm, own)
    operator = fit_near(adjacency, gnorm, mid, up, down, solved)
    return (jnp.swapaxes(operator, 1, 2)[None], own[None])


def solution(mesh):
    split = Mesh(mesh.devices.reshape(4, 4, 4, 2), ("gx_0", "gx_1", "gy_0", "gy_1"))
    placed = (P(GX, GY, None, None, None), P(GX, GY, None, None, None), P(GX, GY), P(GX, GY, None))
    return jax.shard_map(
        body,
        mesh=split,
        in_specs=placed,
        out_specs=(P(GX, GY, None, None), P(GX, GY, None, None)),
        check_vma=False,
    )
```

```python
import jax
import jax.numpy as jnp
from jax import lax
from jax.experimental import pallas as pl
from jax.experimental.pallas import tpu as pltpu
from jax.sharding import Mesh
from jax.sharding import PartitionSpec as P

GX = ("gx_0", "gx_1")
GY = ("gy_0", "gy_1")
GX_GY = ("gx_0", "gx_1", "gy_0", "gy_1")

R = 24
NVAR = 4
K = 512
SLOTS = 2048
COLS = 2
NB = 3
NF = 397
HALF = 0.5
F32 = jnp.float32
BF = jnp.bfloat16
HI = lax.Precision.HIGHEST


def iotas(shape):
    return lax.broadcasted_iota(jnp.int32, shape, 0), lax.broadcasted_iota(jnp.int32, shape, 1)


DEPTH = 3
CUTS = 1
BLOCK = 256


def fold_lanes(x):
    return (x[:, 0:128] + x[:, 128:256]) + (x[:, 256:384] + x[:, 384:512])


def local_kernel(counts, basis, snaps, proj0, proj1, stats, modes, data, proj, acc, basis_sem, sems):
    steps = COLS * NVAR
    rows = SLOTS // CUTS

    def copy(i, c):
        part = pl.ds(c * rows, rows)
        return pltpu.make_async_copy(snaps.at[i // NVAR, i % NVAR, part], data.at[i, part], sems.at[i, c])

    def modes_copy(i):
        return pltpu.make_async_copy(basis.at[i // NVAR, i % NVAR], modes.at[i], basis_sem.at[i])

    for i in range(DEPTH):
        modes_copy(i).start()
        for c in range(CUTS):
            copy(i, c).start()
    acc[...] = jnp.zeros_like(acc)

    def step(i, carry):
        count = counts[0, i // NVAR]
        v = i % NVAR

        @pl.when(i + DEPTH < steps)
        def _():
            modes_copy(i + DEPTH).start()
            for c in range(CUTS):
                copy(i + DEPTH, c).start()

        modes_copy(i).wait()
        for c in range(CUTS):
            copy(i, c).wait()
        lane = lax.broadcasted_iota(jnp.int32, (R, BLOCK), 1)
        row = lax.broadcasted_iota(jnp.int32, (BLOCK, 128), 0)
        parts = []
        prods = []
        for lo in range(0, SLOTS, BLOCK):
            kept = jnp.where(lane < count - lo, modes[i, :, lo : lo + BLOCK], jnp.zeros((), BF))
            prods.append(jnp.dot(kept, data[i, lo : lo + BLOCK], preferred_element_type=F32))
            x = data[i, lo : lo + BLOCK, :].astype(F32)
            t = jnp.where(row < count - lo, fold_lanes(x * x), 0.0)
            parts.append(jnp.sum(t.reshape(BLOCK // 8, 8, 128), axis=0))
        proj[i] = sum(prods)
        part = sum(parts)
        acc[v] += part
        return carry

    lax.fori_loop(0, steps, step, 0)
    q = NVAR
    for a in range(NVAR):
        for b in range(a, NVAR):
            t = fold_lanes(proj[a] * proj[b]) + fold_lanes(proj[NVAR + a] * proj[NVAR + b])
            acc[q] = t[0:8] + t[8:16] + t[16:24]
            q += 1
    for v in range(NVAR):
        proj0[v] = proj[v]
        proj1[v] = proj[NVAR + v]
    total = jnp.sum(jnp.sum(acc[...], axis=1), axis=1, keepdims=True)
    i, j = iotas((16, 128))
    flat = jnp.sum(jnp.where(i == j, total, 0.0), axis=0, keepdims=True)
    nodes = (counts[0, 0] + counts[0, 1]).astype(F32)
    _, lane1 = iotas((1, 128))
    stats[...] = jnp.broadcast_to(jnp.where(lane1 == 14, nodes, flat), (128, 128))


def local_pass(snapshots, basis, counts):
    vm = pl.BlockSpec(memory_space=pltpu.VMEM)
    hbm = pl.BlockSpec(memory_space=pl.ANY)
    return pl.pallas_call(
        local_kernel,
        in_specs=[pl.BlockSpec(memory_space=pltpu.SMEM), hbm, hbm],
        out_specs=[vm, vm, vm],
        out_shape=[
            jax.ShapeDtypeStruct((NVAR, R, K), F32),
            jax.ShapeDtypeStruct((NVAR, R, K), F32),
            jax.ShapeDtypeStruct((128, 128), F32),
        ],
        scratch_shapes=[
            pltpu.VMEM((COLS * NVAR, R, SLOTS), BF),
            pltpu.VMEM((COLS * NVAR, SLOTS, K), BF),
            pltpu.VMEM((COLS * NVAR, R, K), F32),
            pltpu.VMEM((16, 8, 128), F32),
            pltpu.SemaphoreType.DMA((COLS * NVAR,)),
            pltpu.SemaphoreType.DMA((COLS * NVAR, CUTS)),
        ],
        name="local",
    )(counts, basis, snapshots)


OWN = 328
NQ = 288
MIXED = 312
FUT = OWN
NEAR = 72
LANES = 384


def lane_copy(x, at):
    return jnp.take_along_axis(x, jnp.full((8, 128), at, jnp.int32), axis=1)


def sub_copy(x, j):
    return jnp.broadcast_to(x[j : j + 1, :], (8, 128))


def split3(x):
    h = x.astype(BF)
    r = x - h.astype(F32)
    m = r.astype(BF)
    return h, m, (r - m.astype(F32)).astype(BF)


def dot(a, b):
    return jnp.dot(a, b, preferred_element_type=F32)


def mm(a, b):
    return jnp.dot(a, b, precision=HI, preferred_element_type=F32)


def tree(terms):
    while len(terms) > 1:
        terms = [terms[i] + terms[i + 1] for i in range(0, len(terms) - 1, 2)] + terms[len(terms) // 2 * 2 :]
    return terms[0]


def padded_dot(a, w, lo):
    ah, am, al = split3(a)
    n = w.shape[0]
    parts = [jnp.zeros((lo, 128), F32)] * (lo > 0) + [w] + [jnp.zeros((128 - lo - n, 128), F32)] * (lo + n < 128)
    wh, wm, wl = split3(jnp.concatenate(parts, axis=0) if len(parts) > 1 else w)
    pair = jnp.concatenate([wh, wm], axis=1)
    u = dot(jnp.concatenate([ah, am], axis=1), jnp.concatenate([pair, pair], axis=0))
    v = dot(jnp.concatenate([ah, al], axis=1), jnp.concatenate([wl, wh], axis=0))
    return u[:, :128] + (u[:, 128:] + v)


def invert(block, tiles, strip=4, look=2):
    sub, lane = iotas((8, 128))
    for s in range(0, tiles, strip):
        own = list(range(s, min(s + strip, tiles)))
        ahead = list(range(s + strip, min(s + strip + look, tiles)))
        for p in own:
            base = 8 * p
            inside = (lane >= base) & (lane < base + 8)
            unit = jnp.where(lane - base == sub, 1.0, 0.0)
            ws = []
            for m in range(COLS):
                tile = block[m, base : base + 8, :]
                col = [lane_copy(tile, base + k) for k in range(8)]
                x = jnp.where(inside, unit, tile)
                recips = jnp.zeros((8, 128), F32)
                for j in range(8):
                    r = 1.0 / sub_copy(col[j], j)
                    mult = jnp.where(sub == j, 0.0, col[j]) * r
                    recips = jnp.where(sub == j, r, recips)
                    for k in range(j + 1, 8):
                        col[k] = col[k] - mult * sub_copy(col[k], j)
                    x = x - mult * sub_copy(x, j)
                w = x * recips
                block[m, base : base + 8, :] = w
                ws.append([sub_copy(w, j) for j in range(8)])
            for t in [t for t in own + ahead if t > p] + [t for t in own if t < p]:
                for m in range(COLS):
                    a = block[m, 8 * t : 8 * t + 8, :]
                    delta = tree([lane_copy(a, base + j) * ws[m][j] for j in range(8)])
                    block[m, 8 * t : 8 * t + 8, :] = jnp.where(inside, 0.0, a) - delta
            yield
        lo, hi = 8 * s, 8 * (own[-1] + 1)
        ranges = [(a, b) for a, b in ((hi + 8 * len(ahead), 8 * tiles), (0, lo)) if a < b]
        if ranges:
            for m in range(COLS):
                rest = [block[m, a:b, :] for a, b in ranges]
                rest = jnp.concatenate(rest, axis=0) if len(rest) > 1 else rest[0]
                _, wide = iotas(rest.shape)
                kept = jnp.where((wide >= lo) & (wide < hi), 0.0, rest)
                new = kept - padded_dot(rest, block[m, lo:hi, :], lo)
                at = 0
                for a, b in ranges:
                    block[m, a:b, :] = new[at : at + b - a]
                    at += b - a


def spread(panels, count, work):
    work = list(work)
    done = 0
    for i, _ in enumerate(panels):
        want = (i + 1) * len(work) // count if i + 1 < count else len(work)
        while done < min(want, len(work)):
            work[done]()
            done += 1
    for f in work[done:]:
        f()


def own_features(feats, twice, m, state, keep):
    past = jnp.where(keep, state, 0.0)
    twice[m, 0:R] = past
    twice[m, R : 2 * R] = past
    for d in range(12):
        feats(R * d, past * twice[m, d : d + R])
    feats(NQ, past)
    row, lane = iotas((16, K))
    one = jnp.where((row == 12) & (lane < K - 1), 1.0, 0.0)
    feats(MIXED, jnp.where(row < 12, twice[m, 0:16] * twice[m, 12:28], one))
    feats(FUT, pltpu.roll(state, K - 1, 1))


def global_scales(everyone):
    total = jnp.sum(everyone[...], axis=0, keepdims=True)
    nodes = total[:, 14:15]
    inv = []
    for v in range(NVAR):
        inv.append(1.0 / jnp.sqrt(total[:, v : v + 1] / (nodes * K) + 1e-06))
    g = jnp.zeros((1, 1), F32)
    q = NVAR
    for a in range(NVAR):
        for b in range(a, NVAR):
            term = total[:, q : q + 1] * inv[a] * inv[b]
            g = g + (term if a == b else 2.0 * term)
            q += 1
    return [jnp.broadcast_to(x, (1, 128)) for x in inv + [g * (1.0 / (256 * R * K))]]


def scaled_sum(proj, inv):
    t = proj[0] * inv[0]
    for v in range(1, NVAR):
        t = t + proj[v] * inv[v]
    return t


def ridge(g):
    return K * (HALF * g), K * (HALF * g * g)


def past_mask():
    return lax.broadcasted_iota(jnp.int32, (R, K), 1) < K - 1


def nt(a, b):
    return lax.dot_general(a, b, (((1,), (1,)), ((), ())), preferred_element_type=F32)


def own_kernel(everyone, proj0, proj1, out, own, scales, twice, fh, fm, fl, h, block):
    keep = past_mask()
    found = global_scales(everyone)
    scales[...] = jnp.concatenate(found + [jnp.zeros((3, 128), F32)], axis=0)
    for m, proj in enumerate((proj0, proj1)):
        own[m] = scaled_sum(proj, [x[:, 0:1] for x in found])
    for m in range(COLS):

        def put(at, x, m=m):
            a, b, c = split3(x)
            n = x.shape[0]
            fh[m, at : at + n], fm[m, at : at + n], fl[m, at : at + n] = a, b, c

        own_features(put, twice, m, own[m], keep)
    lin, quad = ridge(found[NVAR])
    sub, lane = iotas((8, 128))

    def gram(m, r0, r1, c0, c1):
        a = [f[m, r0:r1] for f in (fh, fm, fl)]
        b = [f[m, c0:c1] for f in (fh, fm, fl)]
        g = ((nt(a[1], b[1]) + nt(a[0], b[2])) + nt(a[2], b[0])) + (nt(a[0], b[1]) + nt(a[1], b[0]))
        return g + nt(a[0], b[0])

    def reg(row):
        if row < NQ or row == MIXED:
            return quad
        if row == MIXED + 8:
            return jnp.where(sub < 4, quad, jnp.where(sub == 4, lin, 1.0))
        return lin

    def ridged(x, row0):
        tiles = []
        for i in range(x.shape[0] // 8):
            tiles.append(x[8 * i : 8 * i + 8] + jnp.where(lane == sub + 8 * i, reg(row0 + 8 * i), 0.0))
        return jnp.concatenate(tiles, axis=0)

    for m in range(COLS):
        block[m] = ridged(gram(m, 0, 128, 0, 128), 0)

    def piece(m, kind):
        def go():
            if kind == 0:
                h[m, 0:128, 128:256] = gram(m, 0, 128, 128, 256)
            elif kind == 1:
                h[m, 128:OWN, 0:128] = gram(m, 128, OWN, 0, 128)
            elif kind == 2:
                h[m, 128:256, 128:256] = ridged(gram(m, 128, 256, 128, 256), 128)
            elif kind == 3:
                h[m, 256:OWN, 128:256] = gram(m, 256, OWN, 128, 256)
            else:
                h[m, :, 256:LANES] = jnp.zeros((OWN, 128), F32)
                h[m, 0:256, 256 : OWN + R] = gram(m, 0, 256, 256, OWN + R)
                h[m, 256:OWN, 256 : OWN + R] = gram(m, 256, OWN, 256, OWN + R)
                h[m, 256:OWN, 256:LANES] = ridged(h[m, 256:OWN, 256:LANES], 256)

        return go

    spread(invert(block, 16), 14, [piece(m, k) for k in range(5) for m in range(COLS)])
    inv0 = [block[m] for m in range(COLS)]
    for m in range(COLS):
        w = mm(inv0[m], h[m, 0:128, 128:256])
        block[m] = h[m, 128:256, 128:256] - mm(h[m, 128:256, 0:128], w)
        h[m, 0:128, 128:256] = w
        h[m, 0:128, 0:128] = inv0[m]

    def after0(m, kind):
        def go():
            if kind == 0:
                h[m, 0:128, 256:LANES] = mm(h[m, 0:128, 0:128], h[m, 0:128, 256:LANES])
            elif kind == 1:
                rows = slice(128, OWN)
                h[m, rows, 256:LANES] -= mm(h[m, rows, 0:128], h[m, 0:128, 256:LANES])
            elif kind == 2:
                rows = slice(256, OWN)
                h[m, rows, 128:256] -= mm(h[m, rows, 0:128], h[m, 0:128, 128:256])
            else:
                rows = slice(128, OWN)
                h[m, rows, 0:128] = -mm(h[m, rows, 0:128], h[m, 0:128, 0:128])

        return go

    spread(invert(block, 16), 14, [after0(m, k) for k in range(4) for m in range(COLS)])
    for m in range(COLS):
        h[m, 128:256, 128:256] = block[m]
        w = mm(block[m], h[m, 128:256, 256:LANES])
        block[m, 0:NEAR] = h[m, 256:OWN, 256:LANES] - mm(h[m, 256:OWN, 128:256], w)
        h[m, 128:256, 256:LANES] = w

    def after1(m, kind):
        def go():
            if kind == 0:
                h[m, 128:256, 0:128] = mm(h[m, 128:256, 128:256], h[m, 128:256, 0:128])
            elif kind == 1:
                h[m, 0:128, 256:LANES] -= mm(h[m, 0:128, 128:256], h[m, 128:256, 256:LANES])
            elif kind == 2:
                for rows in (slice(0, 128), slice(256, OWN)):
                    h[m, rows, 0:128] -= mm(h[m, rows, 128:256], h[m, 128:256, 0:128])
            else:
                for rows in (slice(0, 128), slice(256, OWN)):
                    h[m, rows, 128:256] = -mm(h[m, rows, 128:256], h[m, 128:256, 128:256])

        return go

    spread(invert(block, 9), 8, [after1(m, k) for k in range(4) for m in range(COLS)])
    _, wide = iotas((256, 128))
    for m in range(COLS):
        last = block[m, 0:NEAR]
        w = mm(last[:, 0:NEAR], h[m, 256:OWN, 0:256])
        part = h[m, 0:256, 256:LANES]
        out[m, 0:256, 0:256] = h[m, 0:256, 0:256] - mm(part[:, 0:NEAR], w)
        out[m, 0:256, 256:LANES] = jnp.where(wide < NEAR, 0.0, part) - mm(part[:, 0:NEAR], last)
        out[m, 256:OWN, 0:256] = w
        out[m, 256:OWN, 256:LANES] = last


def fit_own(everyone, proj0, proj1):
    return pl.pallas_call(
        own_kernel,
        out_shape=[
            jax.ShapeDtypeStruct((COLS, OWN, LANES), F32),
            jax.ShapeDtypeStruct((COLS, R, K), F32),
            jax.ShapeDtypeStruct((8, 128), F32),
        ],
        scratch_shapes=[
            pltpu.VMEM((COLS, 2 * R, K), F32),
            pltpu.VMEM((COLS, OWN + R, K), BF),
            pltpu.VMEM((COLS, OWN + R, K), BF),
            pltpu.VMEM((COLS, OWN + R, K), BF),
            pltpu.VMEM((COLS, OWN, LANES), F32),
            pltpu.VMEM((COLS, 128, 128), F32),
        ],
        name="fit_own",
    )(everyone, proj0, proj1)


def near_kernel(adjacency, scales, own, mid, up, down, solved, out, twice, fh, fm, fl, near, block, x, order, sems):
    row0 = lax.axis_index("gx_0") * 4 + lax.axis_index("gx_1")
    col0 = (lax.axis_index("gy_0") * 2 + lax.axis_index("gy_1")) * COLS
    for m in range(COLS):
        for b in range(NB):
            link = adjacency[0, m, b]
            row = (link >> 4) - row0 + 1
            col = (link & 15) - col0 + 1
            slot = m * NB + b
            for r, source in enumerate((up, mid, down)):

                @pl.when(row == r)
                def _():
                    pltpu.make_async_copy(source.at[col], near.at[slot], sems.at[slot]).start()

    keep = past_mask()
    lin, _ = ridge(scales[NVAR : NVAR + 1, :])
    inv = [scales[v : v + 1, 0:1] for v in range(NVAR)]
    sub, lane = iotas((8, 128))
    for m in range(COLS):

        def put(at, v, m=m):
            n = v.shape[0]
            fh[m, at : at + n], fm[m, at : at + n], fl[m, at : at + n] = split3(v)

        own_features(put, twice, m, own[m], keep)
    for m in range(COLS):
        rows = []
        for b in range(NB):
            slot = m * NB + b
            pltpu.make_async_copy(mid.at[0], near.at[slot], sems.at[slot]).wait()
            rows.append(jnp.where(keep, scaled_sum(near.at[slot], inv), 0.0))
        nh, nm, nl = split3(jnp.concatenate(rows, axis=0))
        thirds = jnp.concatenate([nh, nm, nl], axis=0)
        p = nt(fh[m], thirds)
        q = nt(fm[m], thirds[0 : 2 * NEAR])
        g = (p[:, 2 * NEAR : 3 * NEAR] + q[:, NEAR : 2 * NEAR] + nt(fl[m], nh)) + (p[:, NEAR : 2 * NEAR] + q[:, 0:NEAR])
        cross = g + p[:, 0:NEAR]
        p = nt(nh, thirds)
        q = nt(nm, thirds[0 : 2 * NEAR])
        g = (p[:, 2 * NEAR : 3 * NEAR] + q[:, NEAR : 2 * NEAR] + nt(nl, nh)) + (p[:, NEAR : 2 * NEAR] + q[:, 0:NEAR])
        square = g + p[:, 0:NEAR]
        wide = jnp.concatenate([cross, jnp.zeros((LANES - OWN - R, NEAR), F32)], axis=0)
        wide = jnp.concatenate([wide, jnp.zeros((LANES, 128 - NEAR), F32)], axis=1)
        turned = wide.T[0:NEAR]
        z = mm(solved[m, :, 0:256], cross[0:256]) + mm(solved[m, :, 256:OWN], cross[256:OWN])
        tail = solved[m, :, 256:LANES]
        _, lane_o = iotas((OWN, 128))
        z = jnp.concatenate([z, jnp.zeros((OWN, 128 - NEAR), F32)], axis=1)
        both = jnp.where(lane_o < NEAR, z, tail)
        x[m, 0:OWN] = both
        _, lane_n = iotas((NEAR, 128))
        square = jnp.concatenate([square, jnp.zeros((NEAR, 128 - NEAR), F32)], axis=1)
        start = jnp.where(lane_n < NEAR, square, turned[:, 256:LANES])
        start = jnp.where(lane_n < NEAR + R, start, 0.0)
        for i in range(NEAR // 8):
            rows8 = slice(8 * i, 8 * i + 8)
            block[m, rows8] = start[rows8] + jnp.where(lane == sub + 8 * i, lin, 0.0)
        block[m, 0:NEAR] = block[m, 0:NEAR] - mm(turned[:, 0:OWN], both)
    for _ in invert(block, 9):
        pass
    for m in range(COLS):
        last = block[m, 0:NEAR]
        both = x[m, 0:OWN]
        x[m, 0:OWN] = both - mm(both[:, 0:NEAR], last)
        x[m, OWN : OWN + NEAR] = last
        order[m, 0:1] = x[m, MIXED + 12 : MIXED + 13]
        order[m, 1:25] = x[m, NQ : NQ + R]
        order[m, 25:97] = last
        dst = 97
        for a in range(R):
            for b in range(a, R):
                d = b - a
                if d == 12:
                    src = MIXED + a
                elif d < 12:
                    src = R * d + a
                else:
                    src = R * (R - d) + b
                order[m, dst : dst + 1] = x[m, src : src + 1]
                dst += 1
        flat = order[m].T
        out[m] = flat[NEAR : NEAR + R, 0:NF]


def fit_near(adjacency, scales, own, mid, up, down, solved):
    vm = pl.BlockSpec(memory_space=pltpu.VMEM)
    far = pl.BlockSpec(memory_space=pl.ANY)
    return pl.pallas_call(
        near_kernel,
        in_specs=[pl.BlockSpec(memory_space=pltpu.SMEM), vm, vm, far, far, far, vm],
        out_specs=vm,
        out_shape=jax.ShapeDtypeStruct((COLS, R, NF), F32),
        scratch_shapes=[
            pltpu.VMEM((COLS, 2 * R, K), F32),
            pltpu.VMEM((COLS, OWN + R, K), BF),
            pltpu.VMEM((COLS, OWN + R, K), BF),
            pltpu.VMEM((COLS, OWN + R, K), BF),
            pltpu.VMEM((COLS * NB, NVAR, R, K), F32),
            pltpu.VMEM((COLS, 128, 128), F32),
            pltpu.VMEM((COLS, OWN + NEAR, 128), F32),
            pltpu.VMEM((COLS, 512, 128), F32),
            pltpu.SemaphoreType.DMA((COLS * NB,)),
        ],
        name="fit_near",
    )(adjacency, scales, own, mid, up, down, solved)


def shifts(axis, x, y):
    n = lax.axis_size(axis)
    return (
        lax.ppermute(x, axis, [(i, i + 1) for i in range(n - 1)]),
        lax.ppermute(y, axis, [(i + 1, i) for i in range(n - 1)]),
    )


def body(snapshots, basis, node_counts, adjacency):
    proj0, proj1, stats = local_pass(snapshots[0], basis[0], node_counts)
    everyone = lax.all_to_all(stats, GX_GY, 0, 0, tiled=True)
    left, right = shifts(GY, proj1, proj0)
    mid = jnp.stack([left, proj0, proj1, right])
    up, down = shifts(GX, mid, mid)
    solved, own, scales = fit_own(everyone, proj0, proj1)
    operator = fit_near(adjacency, scales, own, mid, up, down, solved)
    return (jnp.swapaxes(operator, 1, 2)[None], own[None])


def solution(mesh):
    split = Mesh(mesh.devices.reshape(4, 4, 4, 2), ("gx_0", "gx_1", "gy_0", "gy_1"))
    placed = (P(GX, GY, None, None, None), P(GX, GY, None, None, None), P(GX, GY), P(GX, GY, None))
    return jax.shard_map(
        body,
        mesh=split,
        in_specs=placed,
        out_specs=(P(GX, GY, None, None), P(GX, GY, None, None)),
        check_vma=False,
    )
```

```python
import jax
import jax.numpy as jnp
from jax import lax
from jax.experimental import pallas as pl
from jax.experimental.pallas import tpu as pltpu
from jax.sharding import Mesh
from jax.sharding import PartitionSpec as P

GX = ("gx_0", "gx_1")
GY = ("gy_0", "gy_1")
GX_GY = ("gx_0", "gx_1", "gy_0", "gy_1")

R = 24
NVAR = 4
K = 512
SLOTS = 2048
COLS = 2
NB = 3
NF = 397
HALF = 0.5
F32 = jnp.float32
BF = jnp.bfloat16
HI = lax.Precision.HIGHEST


def iotas(shape):
    return lax.broadcasted_iota(jnp.int32, shape, 0), lax.broadcasted_iota(jnp.int32, shape, 1)


DEPTH = 3
CUTS = 1
BLOCK = 256


def fold_lanes(x):
    return (x[:, 0:128] + x[:, 128:256]) + (x[:, 256:384] + x[:, 384:512])


def local_kernel(counts, basis, snaps, proj0, proj1, stats, modes, data, proj, acc, basis_sem, sems):
    steps = COLS * NVAR
    rows = SLOTS // CUTS

    def copy(i, c):
        part = pl.ds(c * rows, rows)
        return pltpu.make_async_copy(snaps.at[i // NVAR, i % NVAR, part], data.at[i, part], sems.at[i, c])

    def modes_copy(i):
        return pltpu.make_async_copy(basis.at[i // NVAR, i % NVAR], modes.at[i], basis_sem.at[i])

    for i in range(DEPTH):
        modes_copy(i).start()
        for c in range(CUTS):
            copy(i, c).start()
    acc[...] = jnp.zeros_like(acc)

    def step(i, carry):
        count = counts[0, i // NVAR]
        v = i % NVAR

        @pl.when(i + DEPTH < steps)
        def _():
            modes_copy(i + DEPTH).start()
            for c in range(CUTS):
                copy(i + DEPTH, c).start()

        modes_copy(i).wait()
        for c in range(CUTS):
            copy(i, c).wait()
        lane = lax.broadcasted_iota(jnp.int32, (R, BLOCK), 1)
        row = lax.broadcasted_iota(jnp.int32, (BLOCK, 128), 0)
        parts = []
        prods = []
        for lo in range(0, SLOTS, BLOCK):
            kept = jnp.where(lane < count - lo, modes[i, :, lo : lo + BLOCK], jnp.zeros((), BF))
            prods.append(jnp.dot(kept, data[i, lo : lo + BLOCK], preferred_element_type=F32))
            x = data[i, lo : lo + BLOCK, :].astype(F32)
            t = jnp.where(row < count - lo, fold_lanes(x * x), 0.0)
            parts.append(jnp.sum(t.reshape(BLOCK // 8, 8, 128), axis=0))
        proj[i] = sum(prods)
        part = sum(parts)
        acc[v] += part
        return carry

    lax.fori_loop(0, steps, step, 0)
    q = NVAR
    for a in range(NVAR):
        for b in range(a, NVAR):
            t = fold_lanes(proj[a] * proj[b]) + fold_lanes(proj[NVAR + a] * proj[NVAR + b])
            acc[q] = t[0:8] + t[8:16] + t[16:24]
            q += 1
    for v in range(NVAR):
        proj0[v] = proj[v]
        proj1[v] = proj[NVAR + v]
    total = jnp.sum(jnp.sum(acc[...], axis=1), axis=1, keepdims=True)
    i, j = iotas((16, 128))
    flat = jnp.sum(jnp.where(i == j, total, 0.0), axis=0, keepdims=True)
    nodes = (counts[0, 0] + counts[0, 1]).astype(F32)
    _, lane1 = iotas((1, 128))
    stats[...] = jnp.broadcast_to(jnp.where(lane1 == 14, nodes, flat), (128, 128))


ROOM = 36 << 20


def on_chip(*xs):
    return [pltpu.with_memory_space_constraint(x, pltpu.VMEM) for x in xs]


def local_pass(snapshots, basis, counts):
    vm = pl.BlockSpec(memory_space=pltpu.VMEM)
    hbm = pl.BlockSpec(memory_space=pl.ANY)
    return pl.pallas_call(
        local_kernel,
        in_specs=[pl.BlockSpec(memory_space=pltpu.SMEM), hbm, hbm],
        out_specs=[vm, vm, vm],
        out_shape=[
            pltpu.VMEM((NVAR, R, K), F32),
            pltpu.VMEM((NVAR, R, K), F32),
            pltpu.VMEM((128, 128), F32),
        ],
        scratch_shapes=[
            pltpu.VMEM((COLS * NVAR, R, SLOTS), BF),
            pltpu.VMEM((COLS * NVAR, SLOTS, K), BF),
            pltpu.VMEM((COLS * NVAR, R, K), F32),
            pltpu.VMEM((16, 8, 128), F32),
            pltpu.SemaphoreType.DMA((COLS * NVAR,)),
            pltpu.SemaphoreType.DMA((COLS * NVAR, CUTS)),
        ],
        compiler_params=pltpu.CompilerParams(vmem_limit_bytes=ROOM),
        name="local",
    )(*[pltpu.with_memory_space_constraint(x, pltpu.HBM) for x in (counts, basis, snapshots)])


OWN = 328
NQ = 288
MIXED = 312
FUT = OWN
NEAR = 72
LANES = 384


def lane_copy(x, at):
    return jnp.take_along_axis(x, jnp.full((8, 128), at, jnp.int32), axis=1)


def sub_copy(x, j):
    return jnp.broadcast_to(x[j : j + 1, :], (8, 128))


def split3(x):
    h = x.astype(BF)
    r = x - h.astype(F32)
    m = r.astype(BF)
    return h, m, (r - m.astype(F32)).astype(BF)


def dot(a, b):
    return jnp.dot(a, b, preferred_element_type=F32)


def mm(a, b):
    return jnp.dot(a, b, precision=HI, preferred_element_type=F32)


def tree(terms):
    while len(terms) > 1:
        terms = [terms[i] + terms[i + 1] for i in range(0, len(terms) - 1, 2)] + terms[len(terms) // 2 * 2 :]
    return terms[0]


def padded_dot(a, w, lo):
    ah, am, al = split3(a)
    n = w.shape[0]
    parts = [jnp.zeros((lo, 128), F32)] * (lo > 0) + [w] + [jnp.zeros((128 - lo - n, 128), F32)] * (lo + n < 128)
    wh, wm, wl = split3(jnp.concatenate(parts, axis=0) if len(parts) > 1 else w)
    pair = jnp.concatenate([wh, wm], axis=1)
    u = dot(jnp.concatenate([ah, am], axis=1), jnp.concatenate([pair, pair], axis=0))
    v = dot(jnp.concatenate([ah, al], axis=1), jnp.concatenate([wl, wh], axis=0))
    return u[:, :128] + (u[:, 128:] + v)


def invert(block, tiles, strip=4, look=2):
    sub, lane = iotas((8, 128))
    for s in range(0, tiles, strip):
        own = list(range(s, min(s + strip, tiles)))
        ahead = list(range(s + strip, min(s + strip + look, tiles)))
        for p in own:
            base = 8 * p
            inside = (lane >= base) & (lane < base + 8)
            unit = jnp.where(lane - base == sub, 1.0, 0.0)
            ws = []
            for m in range(COLS):
                tile = block[m, base : base + 8, :]
                col = [lane_copy(tile, base + k) for k in range(8)]
                x = jnp.where(inside, unit, tile)
                recips = jnp.zeros((8, 128), F32)
                for j in range(8):
                    r = 1.0 / sub_copy(col[j], j)
                    mult = jnp.where(sub == j, 0.0, col[j]) * r
                    recips = jnp.where(sub == j, r, recips)
                    for k in range(j + 1, 8):
                        col[k] = col[k] - mult * sub_copy(col[k], j)
                    x = x - mult * sub_copy(x, j)
                w = x * recips
                block[m, base : base + 8, :] = w
                ws.append([sub_copy(w, j) for j in range(8)])
            for t in [t for t in own + ahead if t > p] + [t for t in own if t < p]:
                for m in range(COLS):
                    a = block[m, 8 * t : 8 * t + 8, :]
                    delta = tree([lane_copy(a, base + j) * ws[m][j] for j in range(8)])
                    block[m, 8 * t : 8 * t + 8, :] = jnp.where(inside, 0.0, a) - delta
            yield
        lo, hi = 8 * s, 8 * (own[-1] + 1)
        ranges = [(a, b) for a, b in ((hi + 8 * len(ahead), 8 * tiles), (0, lo)) if a < b]
        if ranges:
            for m in range(COLS):
                rest = [block[m, a:b, :] for a, b in ranges]
                rest = jnp.concatenate(rest, axis=0) if len(rest) > 1 else rest[0]
                _, wide = iotas(rest.shape)
                kept = jnp.where((wide >= lo) & (wide < hi), 0.0, rest)
                new = kept - padded_dot(rest, block[m, lo:hi, :], lo)
                at = 0
                for a, b in ranges:
                    block[m, a:b, :] = new[at : at + b - a]
                    at += b - a


def spread(panels, count, work):
    work = list(work)
    done = 0
    for i, _ in enumerate(panels):
        want = (i + 1) * len(work) // count if i + 1 < count else len(work)
        while done < min(want, len(work)):
            work[done]()
            done += 1
    for f in work[done:]:
        f()


def own_features(feats, twice, m, state, keep):
    past = jnp.where(keep, state, 0.0)
    twice[m, 0:R] = past
    twice[m, R : 2 * R] = past
    for d in range(12):
        feats(R * d, past * twice[m, d : d + R])
    feats(NQ, past)
    row, lane = iotas((16, K))
    one = jnp.where((row == 12) & (lane < K - 1), 1.0, 0.0)
    feats(MIXED, jnp.where(row < 12, twice[m, 0:16] * twice[m, 12:28], one))
    feats(FUT, pltpu.roll(state, K - 1, 1))


def global_scales(everyone):
    total = jnp.sum(everyone[...], axis=0, keepdims=True)
    nodes = total[:, 14:15]
    inv = []
    for v in range(NVAR):
        inv.append(1.0 / jnp.sqrt(total[:, v : v + 1] / (nodes * K) + 1e-06))
    g = jnp.zeros((1, 1), F32)
    q = NVAR
    for a in range(NVAR):
        for b in range(a, NVAR):
            term = total[:, q : q + 1] * inv[a] * inv[b]
            g = g + (term if a == b else 2.0 * term)
            q += 1
    return [jnp.broadcast_to(x, (1, 128)) for x in inv + [g * (1.0 / (256 * R * K))]]


def scaled_sum(proj, inv):
    t = proj[0] * inv[0]
    for v in range(1, NVAR):
        t = t + proj[v] * inv[v]
    return t


def ridge(g):
    return K * (HALF * g), K * (HALF * g * g)


def past_mask():
    return lax.broadcasted_iota(jnp.int32, (R, K), 1) < K - 1


def nt(a, b):
    return lax.dot_general(a, b, (((1,), (1,)), ((), ())), preferred_element_type=F32)


def own_kernel(everyone, proj0, proj1, out, own, scales, twice, fh, fm, fl, h, block):
    keep = past_mask()
    found = global_scales(everyone)
    scales[...] = jnp.concatenate(found + [jnp.zeros((3, 128), F32)], axis=0)
    for m, proj in enumerate((proj0, proj1)):
        own[m] = scaled_sum(proj, [x[:, 0:1] for x in found])
    for m in range(COLS):

        def put(at, x, m=m):
            a, b, c = split3(x)
            n = x.shape[0]
            fh[m, at : at + n], fm[m, at : at + n], fl[m, at : at + n] = a, b, c

        own_features(put, twice, m, own[m], keep)
    lin, quad = ridge(found[NVAR])
    sub, lane = iotas((8, 128))

    def gram(m, r0, r1, c0, c1):
        a = [f[m, r0:r1] for f in (fh, fm, fl)]
        b = [f[m, c0:c1] for f in (fh, fm, fl)]
        g = ((nt(a[1], b[1]) + nt(a[0], b[2])) + nt(a[2], b[0])) + (nt(a[0], b[1]) + nt(a[1], b[0]))
        return g + nt(a[0], b[0])

    def reg(row):
        if row < NQ or row == MIXED:
            return quad
        if row == MIXED + 8:
            return jnp.where(sub < 4, quad, jnp.where(sub == 4, lin, 1.0))
        return lin

    def ridged(x, row0):
        tiles = []
        for i in range(x.shape[0] // 8):
            tiles.append(x[8 * i : 8 * i + 8] + jnp.where(lane == sub + 8 * i, reg(row0 + 8 * i), 0.0))
        return jnp.concatenate(tiles, axis=0)

    for m in range(COLS):
        block[m] = ridged(gram(m, 0, 128, 0, 128), 0)

    def piece(m, kind):
        def go():
            if kind == 0:
                h[m, 0:128, 128:256] = gram(m, 0, 128, 128, 256)
            elif kind == 1:
                h[m, 128:OWN, 0:128] = gram(m, 128, OWN, 0, 128)
            elif kind == 2:
                h[m, 128:256, 128:256] = ridged(gram(m, 128, 256, 128, 256), 128)
            elif kind == 3:
                h[m, 256:OWN, 128:256] = gram(m, 256, OWN, 128, 256)
            else:
                h[m, :, 256:LANES] = jnp.zeros((OWN, 128), F32)
                h[m, 0:256, 256 : OWN + R] = gram(m, 0, 256, 256, OWN + R)
                h[m, 256:OWN, 256 : OWN + R] = gram(m, 256, OWN, 256, OWN + R)
                h[m, 256:OWN, 256:LANES] = ridged(h[m, 256:OWN, 256:LANES], 256)

        return go

    spread(invert(block, 16), 14, [piece(m, k) for k in range(5) for m in range(COLS)])
    inv0 = [block[m] for m in range(COLS)]
    for m in range(COLS):
        w = mm(inv0[m], h[m, 0:128, 128:256])
        block[m] = h[m, 128:256, 128:256] - mm(h[m, 128:256, 0:128], w)
        h[m, 0:128, 128:256] = w
        h[m, 0:128, 0:128] = inv0[m]

    def after0(m, kind):
        def go():
            if kind == 0:
                h[m, 0:128, 256:LANES] = mm(h[m, 0:128, 0:128], h[m, 0:128, 256:LANES])
            elif kind == 1:
                rows = slice(128, OWN)
                h[m, rows, 256:LANES] -= mm(h[m, rows, 0:128], h[m, 0:128, 256:LANES])
            elif kind == 2:
                rows = slice(256, OWN)
                h[m, rows, 128:256] -= mm(h[m, rows, 0:128], h[m, 0:128, 128:256])
            else:
                rows = slice(128, OWN)
                h[m, rows, 0:128] = -mm(h[m, rows, 0:128], h[m, 0:128, 0:128])

        return go

    spread(invert(block, 16), 14, [after0(m, k) for k in range(4) for m in range(COLS)])
    for m in range(COLS):
        h[m, 128:256, 128:256] = block[m]
        w = mm(block[m], h[m, 128:256, 256:LANES])
        block[m, 0:NEAR] = h[m, 256:OWN, 256:LANES] - mm(h[m, 256:OWN, 128:256], w)
        h[m, 128:256, 256:LANES] = w

    def after1(m, kind):
        def go():
            if kind == 0:
                h[m, 128:256, 0:128] = mm(h[m, 128:256, 128:256], h[m, 128:256, 0:128])
            elif kind == 1:
                h[m, 0:128, 256:LANES] -= mm(h[m, 0:128, 128:256], h[m, 128:256, 256:LANES])
            elif kind == 2:
                for rows in (slice(0, 128), slice(256, OWN)):
                    h[m, rows, 0:128] -= mm(h[m, rows, 128:256], h[m, 128:256, 0:128])
            else:
                for rows in (slice(0, 128), slice(256, OWN)):
                    h[m, rows, 128:256] = -mm(h[m, rows, 128:256], h[m, 128:256, 128:256])

        return go

    spread(invert(block, 9), 8, [after1(m, k) for k in range(4) for m in range(COLS)])
    _, wide = iotas((256, 128))
    for m in range(COLS):
        last = block[m, 0:NEAR]
        w = mm(last[:, 0:NEAR], h[m, 256:OWN, 0:256])
        part = h[m, 0:256, 256:LANES]
        out[m, 0:256, 0:256] = h[m, 0:256, 0:256] - mm(part[:, 0:NEAR], w)
        out[m, 0:256, 256:LANES] = jnp.where(wide < NEAR, 0.0, part) - mm(part[:, 0:NEAR], last)
        out[m, 256:OWN, 0:256] = w
        out[m, 256:OWN, 256:LANES] = last


def fit_own(everyone, proj0, proj1):
    return pl.pallas_call(
        own_kernel,
        out_shape=[
            pltpu.VMEM((COLS, OWN, LANES), F32),
            pltpu.VMEM((COLS, R, K), F32),
            pltpu.VMEM((8, 128), F32),
        ],
        scratch_shapes=[
            pltpu.VMEM((COLS, 2 * R, K), F32),
            pltpu.VMEM((COLS, OWN + R, K), BF),
            pltpu.VMEM((COLS, OWN + R, K), BF),
            pltpu.VMEM((COLS, OWN + R, K), BF),
            pltpu.VMEM((COLS, OWN, LANES), F32),
            pltpu.VMEM((COLS, 128, 128), F32),
        ],
        compiler_params=pltpu.CompilerParams(vmem_limit_bytes=ROOM),
        name="fit_own",
    )(*on_chip(everyone, proj0, proj1))


def near_kernel(adjacency, scales, own, mid, up, down, solved, out, twice, fh, fm, fl, near, block, x, order, sems):
    row0 = lax.axis_index("gx_0") * 4 + lax.axis_index("gx_1")
    col0 = (lax.axis_index("gy_0") * 2 + lax.axis_index("gy_1")) * COLS
    for m in range(COLS):
        for b in range(NB):
            link = adjacency[0, m, b]
            row = (link >> 4) - row0 + 1
            col = (link & 15) - col0 + 1
            slot = m * NB + b
            for r, source in enumerate((up, mid, down)):

                @pl.when(row == r)
                def _():
                    pltpu.make_async_copy(source.at[col], near.at[slot], sems.at[slot]).start()

    keep = past_mask()
    lin, _ = ridge(scales[NVAR : NVAR + 1, :])
    inv = [scales[v : v + 1, 0:1] for v in range(NVAR)]
    sub, lane = iotas((8, 128))
    for m in range(COLS):

        def put(at, v, m=m):
            n = v.shape[0]
            fh[m, at : at + n], fm[m, at : at + n], fl[m, at : at + n] = split3(v)

        own_features(put, twice, m, own[m], keep)
    for m in range(COLS):
        rows = []
        for b in range(NB):
            slot = m * NB + b
            pltpu.make_async_copy(mid.at[0], near.at[slot], sems.at[slot]).wait()
            rows.append(jnp.where(keep, scaled_sum(near.at[slot], inv), 0.0))
        nh, nm, nl = split3(jnp.concatenate(rows, axis=0))
        thirds = jnp.concatenate([nh, nm, nl], axis=0)
        p = nt(fh[m], thirds)
        q = nt(fm[m], thirds[0 : 2 * NEAR])
        g = (p[:, 2 * NEAR : 3 * NEAR] + q[:, NEAR : 2 * NEAR] + nt(fl[m], nh)) + (p[:, NEAR : 2 * NEAR] + q[:, 0:NEAR])
        cross = g + p[:, 0:NEAR]
        p = nt(nh, thirds)
        q = nt(nm, thirds[0 : 2 * NEAR])
        g = (p[:, 2 * NEAR : 3 * NEAR] + q[:, NEAR : 2 * NEAR] + nt(nl, nh)) + (p[:, NEAR : 2 * NEAR] + q[:, 0:NEAR])
        square = g + p[:, 0:NEAR]
        wide = jnp.concatenate([cross, jnp.zeros((LANES - OWN - R, NEAR), F32)], axis=0)
        wide = jnp.concatenate([wide, jnp.zeros((LANES, 128 - NEAR), F32)], axis=1)
        turned = wide.T[0:NEAR]
        z = mm(solved[m, :, 0:256], cross[0:256]) + mm(solved[m, :, 256:OWN], cross[256:OWN])
        tail = solved[m, :, 256:LANES]
        _, lane_o = iotas((OWN, 128))
        z = jnp.concatenate([z, jnp.zeros((OWN, 128 - NEAR), F32)], axis=1)
        both = jnp.where(lane_o < NEAR, z, tail)
        x[m, 0:OWN] = both
        _, lane_n = iotas((NEAR, 128))
        square = jnp.concatenate([square, jnp.zeros((NEAR, 128 - NEAR), F32)], axis=1)
        start = jnp.where(lane_n < NEAR, square, turned[:, 256:LANES])
        start = jnp.where(lane_n < NEAR + R, start, 0.0)
        for i in range(NEAR // 8):
            rows8 = slice(8 * i, 8 * i + 8)
            block[m, rows8] = start[rows8] + jnp.where(lane == sub + 8 * i, lin, 0.0)
        block[m, 0:NEAR] = block[m, 0:NEAR] - mm(turned[:, 0:OWN], both)
    for _ in invert(block, 9):
        pass
    for m in range(COLS):
        last = block[m, 0:NEAR]
        both = x[m, 0:OWN]
        x[m, 0:OWN] = both - mm(both[:, 0:NEAR], last)
        x[m, OWN : OWN + NEAR] = last
        order[m, 0:1] = x[m, MIXED + 12 : MIXED + 13]
        order[m, 1:25] = x[m, NQ : NQ + R]
        order[m, 25:97] = last
        dst = 97
        for a in range(R):
            for b in range(a, R):
                d = b - a
                if d == 12:
                    src = MIXED + a
                elif d < 12:
                    src = R * d + a
                else:
                    src = R * (R - d) + b
                order[m, dst : dst + 1] = x[m, src : src + 1]
                dst += 1
        flat = order[m].T
        out[m] = flat[NEAR : NEAR + R, 0:NF]


def fit_near(adjacency, scales, own, mid, up, down, solved):
    vm = pl.BlockSpec(memory_space=pltpu.VMEM)
    far = pl.BlockSpec(memory_space=pl.ANY)
    return pl.pallas_call(
        near_kernel,
        in_specs=[pl.BlockSpec(memory_space=pltpu.SMEM), vm, vm, far, far, far, vm],
        out_specs=vm,
        out_shape=jax.ShapeDtypeStruct((COLS, R, NF), F32),
        scratch_shapes=[
            pltpu.VMEM((COLS, 2 * R, K), F32),
            pltpu.VMEM((COLS, OWN + R, K), BF),
            pltpu.VMEM((COLS, OWN + R, K), BF),
            pltpu.VMEM((COLS, OWN + R, K), BF),
            pltpu.VMEM((COLS * NB, NVAR, R, K), F32),
            pltpu.VMEM((COLS, 128, 128), F32),
            pltpu.VMEM((COLS, OWN + NEAR, 128), F32),
            pltpu.VMEM((COLS, 512, 128), F32),
            pltpu.SemaphoreType.DMA((COLS * NB,)),
        ],
        compiler_params=pltpu.CompilerParams(vmem_limit_bytes=ROOM),
        name="fit_near",
    )(pltpu.with_memory_space_constraint(adjacency, pltpu.HBM), *on_chip(scales, own, mid, up, down, solved))


def shifts(axis, x, y):
    n = lax.axis_size(axis)
    return (
        lax.ppermute(x, axis, [(i, i + 1) for i in range(n - 1)]),
        lax.ppermute(y, axis, [(i + 1, i) for i in range(n - 1)]),
    )


def body(snapshots, basis, node_counts, adjacency):
    proj0, proj1, stats = local_pass(snapshots[0], basis[0], node_counts)
    everyone = lax.all_to_all(stats, GX_GY, 0, 0, tiled=True)
    left, right = shifts(GY, proj1, proj0)
    mid = jnp.stack([left, proj0, proj1, right])
    up, down = shifts(GX, mid, mid)
    solved, own, scales = fit_own(everyone, proj0, proj1)
    operator = fit_near(adjacency, scales, own, mid, up, down, solved)
    return (jnp.swapaxes(operator, 1, 2)[None], own[None])


def solution(mesh):
    split = Mesh(mesh.devices.reshape(4, 4, 4, 2), ("gx_0", "gx_1", "gy_0", "gy_1"))
    placed = (P(GX, GY, None, None, None), P(GX, GY, None, None, None), P(GX, GY), P(GX, GY, None))
    return jax.shard_map(
        body,
        mesh=split,
        in_specs=placed,
        out_specs=(P(GX, GY, None, None), P(GX, GY, None, None)),
        check_vma=False,
    )
```

```python
import jax
import jax.numpy as jnp
from jax import lax
from jax.experimental import pallas as pl
from jax.experimental.pallas import tpu as pltpu
from jax.sharding import Mesh
from jax.sharding import PartitionSpec as P

GX = ("gx_0", "gx_1")
GY = ("gy_0", "gy_1")
GX_GY = ("gx_0", "gx_1", "gy_0", "gy_1")

R = 24
NVAR = 4
K = 512
SLOTS = 2048
COLS = 2
NB = 3
NF = 397
HALF = 0.5
F32 = jnp.float32
BF = jnp.bfloat16


def iotas(shape):
    return lax.broadcasted_iota(jnp.int32, shape, 0), lax.broadcasted_iota(jnp.int32, shape, 1)


DEPTH = 3
CUTS = 1
BLOCK = 256


def fold_lanes(x):
    return (x[:, 0:128] + x[:, 128:256]) + (x[:, 256:384] + x[:, 384:512])


def local_kernel(counts, basis, snaps, proj0, proj1, stats, modes, data, proj, acc, basis_sem, sems):
    steps = COLS * NVAR
    rows = SLOTS // CUTS

    def copy(i, c):
        part = pl.ds(c * rows, rows)
        return pltpu.make_async_copy(snaps.at[i // NVAR, i % NVAR, part], data.at[i, part], sems.at[i, c])

    def modes_copy(i):
        return pltpu.make_async_copy(basis.at[i // NVAR, i % NVAR], modes.at[i], basis_sem.at[i])

    for i in range(DEPTH):
        modes_copy(i).start()
        for c in range(CUTS):
            copy(i, c).start()
    acc[...] = jnp.zeros_like(acc)

    def step(i, carry):
        count = counts[0, i // NVAR]
        v = i % NVAR

        @pl.when(i + DEPTH < steps)
        def _():
            modes_copy(i + DEPTH).start()
            for c in range(CUTS):
                copy(i + DEPTH, c).start()

        modes_copy(i).wait()
        for c in range(CUTS):
            copy(i, c).wait()
        lane = lax.broadcasted_iota(jnp.int32, (R, BLOCK), 1)
        row = lax.broadcasted_iota(jnp.int32, (BLOCK, 128), 0)
        parts = []
        prods = []
        for lo in range(0, SLOTS, BLOCK):
            kept = jnp.where(lane < count - lo, modes[i, :, lo : lo + BLOCK], jnp.zeros((), BF))
            prods.append(jnp.dot(kept, data[i, lo : lo + BLOCK], preferred_element_type=F32))
            x = data[i, lo : lo + BLOCK, :].astype(F32)
            t = jnp.where(row < count - lo, fold_lanes(x * x), 0.0)
            parts.append(jnp.sum(t.reshape(BLOCK // 8, 8, 128), axis=0))
        proj[i] = sum(prods)
        part = sum(parts)
        acc[v] += part
        return carry

    lax.fori_loop(0, steps, step, 0)
    q = NVAR
    for a in range(NVAR):
        for b in range(a, NVAR):
            t = fold_lanes(proj[a] * proj[b]) + fold_lanes(proj[NVAR + a] * proj[NVAR + b])
            acc[q] = t[0:8] + t[8:16] + t[16:24]
            q += 1
    for v in range(NVAR):
        proj0[v] = proj[v]
        proj1[v] = proj[NVAR + v]
    total = jnp.sum(jnp.sum(acc[...], axis=1), axis=1, keepdims=True)
    i, j = iotas((16, 128))
    flat = jnp.sum(jnp.where(i == j, total, 0.0), axis=0, keepdims=True)
    nodes = (counts[0, 0] + counts[0, 1]).astype(F32)
    _, lane1 = iotas((1, 128))
    stats[...] = jnp.broadcast_to(jnp.where(lane1 == 14, nodes, flat), (128, 128))


ROOM = 36 << 20


def on_chip(*xs):
    return [pltpu.with_memory_space_constraint(x, pltpu.VMEM) for x in xs]


def local_pass(snapshots, basis, counts):
    vm = pl.BlockSpec(memory_space=pltpu.VMEM)
    hbm = pl.BlockSpec(memory_space=pl.ANY)
    return pl.pallas_call(
        local_kernel,
        in_specs=[pl.BlockSpec(memory_space=pltpu.SMEM), hbm, hbm],
        out_specs=[vm, vm, vm],
        out_shape=[
            pltpu.VMEM((NVAR, R, K), F32),
            pltpu.VMEM((NVAR, R, K), F32),
            pltpu.VMEM((128, 128), F32),
        ],
        scratch_shapes=[
            pltpu.VMEM((COLS * NVAR, R, SLOTS), BF),
            pltpu.VMEM((COLS * NVAR, SLOTS, K), BF),
            pltpu.VMEM((COLS * NVAR, R, K), F32),
            pltpu.VMEM((16, 8, 128), F32),
            pltpu.SemaphoreType.DMA((COLS * NVAR,)),
            pltpu.SemaphoreType.DMA((COLS * NVAR, CUTS)),
        ],
        compiler_params=pltpu.CompilerParams(vmem_limit_bytes=ROOM),
        name="local",
    )(*[pltpu.with_memory_space_constraint(x, pltpu.HBM) for x in (counts, basis, snapshots)])


OWN = 328
NQ = 288
MIXED = 312
FUT = OWN
NEAR = 72
LANES = 384


def lane_copy(x, at):
    return jnp.take_along_axis(x, jnp.full((8, 128), at, jnp.int32), axis=1)


def sub_copy(x, j):
    return jnp.broadcast_to(x[j : j + 1, :], (8, 128))


def split3(x):
    h = x.astype(BF)
    r = x - h.astype(F32)
    m = r.astype(BF)
    return h, m, (r - m.astype(F32)).astype(BF)


def dot(a, b):
    return jnp.dot(a, b, preferred_element_type=F32)


def mm(a, b):
    ah, am, al = split3(a)
    bh, bm, bl = split3(b)
    n = b.shape[1]
    w = jnp.concatenate([bh, bm], axis=1)
    p = dot(jnp.concatenate([ah, am], axis=1), jnp.concatenate([w, w], axis=0))
    q = dot(jnp.concatenate([ah, al], axis=1), jnp.concatenate([bl, bh], axis=0))
    return p[:, :n] + (p[:, n:] + q)


def mm_thirds(a, b):
    bh, bm, bl = split3(b)
    n = b.shape[1]
    w = jnp.concatenate([bh, bm], axis=1)
    p = dot(a[0], w)
    q = dot(a[1], w)
    r = dot(a[0], bl) + dot(a[2], bh)
    return p[:, :n] + ((p[:, n:] + q[:, :n]) + (q[:, n:] + r))


def first_lanes(x):
    return jnp.where(iotas(x.shape)[1] < NEAR, x, 0.0)


def to_rows(x, rows):
    return jnp.concatenate([x, jnp.zeros((rows - x.shape[0], x.shape[1]), F32)], axis=0)


def tree(terms):
    while len(terms) > 1:
        terms = [terms[i] + terms[i + 1] for i in range(0, len(terms) - 1, 2)] + terms[len(terms) // 2 * 2 :]
    return terms[0]


def padded_dot(a, w, lo):
    ah, am, al = split3(a)
    n = w.shape[0]
    parts = [jnp.zeros((lo, 128), F32)] * (lo > 0) + [w] + [jnp.zeros((128 - lo - n, 128), F32)] * (lo + n < 128)
    wh, wm, wl = split3(jnp.concatenate(parts, axis=0) if len(parts) > 1 else w)
    pair = jnp.concatenate([wh, wm], axis=1)
    u = dot(jnp.concatenate([ah, am], axis=1), jnp.concatenate([pair, pair], axis=0))
    v = dot(jnp.concatenate([ah, al], axis=1), jnp.concatenate([wl, wh], axis=0))
    return u[:, :128] + (u[:, 128:] + v)


def pivots(col, riders, sub):
    recips = jnp.zeros((8, 128), F32)
    diag = sub_copy(col[0], 0)
    for j in range(8):
        r = 1.0 / diag
        bare = jnp.where(sub == j, 0.0, col[j])
        recips = jnp.where(sub == j, r, recips)
        heads = {k: sub_copy(col[k], j) for k in range(j + 1, 8)}
        if j < 7:
            diag = sub_copy(col[j + 1], j + 1) - (sub_copy(col[j], j + 1) * heads[j + 1]) * r
        mult = bare * r
        for k in range(j + 1, 8):
            col[k] = col[k] - mult * heads[k]
        riders = [x - mult * sub_copy(x, j) for x in riders]
    return [x * recips for x in riders]


def invert(block, tiles, strip=4, look=1):
    sub, lane = iotas((8, 128))
    for s in range(0, tiles, strip):
        own = list(range(s, min(s + strip, tiles)))
        ahead = list(range(s + strip, min(s + strip + look, tiles)))
        for p in own:
            base = 8 * p
            inside = (lane >= base) & (lane < base + 8)
            unit = jnp.where(lane - base == sub, 1.0, 0.0)
            ws = []
            for m in range(COLS):
                tile = block[m, base : base + 8, :]
                col = [lane_copy(tile, base + k) for k in range(8)]
                w = pivots(col, [jnp.where(inside, unit, tile)], sub)[0]
                block[m, base : base + 8, :] = w
                ws.append([sub_copy(w, j) for j in range(8)])
            for t in [t for t in own + ahead if t > p] + [t for t in own if t < p]:
                for m in range(COLS):
                    a = block[m, 8 * t : 8 * t + 8, :]
                    delta = tree([lane_copy(a, base + j) * ws[m][j] for j in range(8)])
                    block[m, 8 * t : 8 * t + 8, :] = jnp.where(inside, 0.0, a) - delta
            yield
        lo, hi = 8 * s, 8 * (own[-1] + 1)
        ranges = [(a, b) for a, b in ((hi + 8 * len(ahead), 8 * tiles), (0, lo)) if a < b]
        if ranges:
            for m in range(COLS):
                rest = [block[m, a:b, :] for a, b in ranges]
                rest = jnp.concatenate(rest, axis=0) if len(rest) > 1 else rest[0]
                _, wide_l = iotas(rest.shape)
                kept = jnp.where((wide_l >= lo) & (wide_l < hi), 0.0, rest)
                new = kept - padded_dot(rest, block[m, lo:hi, :], lo)
                at = 0
                for a, b in ranges:
                    block[m, a:b, :] = new[at : at + b - a]
                    at += b - a


def spread(panels, count, work):
    work = list(work)
    done = 0
    for i, _ in enumerate(panels):
        want = (i + 1) * len(work) // count if i + 1 < count else len(work)
        while done < min(want, len(work)):
            work[done]()
            done += 1
    for f in work[done:]:
        f()


def states_kernel(everyone, left, proj0, proj1, right, mid, gnorm):
    found = global_scales(everyone)
    gnorm[...] = jnp.broadcast_to(found[NVAR], (8, 128))
    inv = [x[:, 0:1] for x in found]
    for c, proj in enumerate((left, proj0, proj1, right)):
        mid[c] = scaled_sum(proj, inv)


def global_states(everyone, left, proj0, proj1, right):
    return pl.pallas_call(
        states_kernel,
        out_shape=[pltpu.VMEM((4, R, K), F32), pltpu.VMEM((8, 128), F32)],
        compiler_params=pltpu.CompilerParams(vmem_limit_bytes=ROOM),
        name="states",
    )(*on_chip(everyone, left, proj0, proj1, right))


def own_features(feats, twice, m, state, keep):
    past = jnp.where(keep, state, 0.0)
    twice[m, 0:R] = past
    twice[m, R : 2 * R] = past
    for d in range(12):
        feats(R * d, past * twice[m, d : d + R])
    feats(NQ, past)
    row, lane = iotas((16, K))
    one = jnp.where((row == 12) & (lane < K - 1), 1.0, 0.0)
    feats(MIXED, jnp.where(row < 12, twice[m, 0:16] * twice[m, 12:28], one))
    feats(FUT, pltpu.roll(state, K - 1, 1))


def global_scales(everyone):
    total = jnp.sum(everyone[...], axis=0, keepdims=True)
    nodes = total[:, 14:15]
    inv = []
    for v in range(NVAR):
        inv.append(1.0 / jnp.sqrt(total[:, v : v + 1] / (nodes * K) + 1e-06))
    g = jnp.zeros((1, 1), F32)
    q = NVAR
    for a in range(NVAR):
        for b in range(a, NVAR):
            term = total[:, q : q + 1] * inv[a] * inv[b]
            g = g + (term if a == b else 2.0 * term)
            q += 1
    return [jnp.broadcast_to(x, (1, 128)) for x in inv + [g * (1.0 / (256 * R * K))]]


def scaled_sum(proj, inv):
    t = proj[0] * inv[0]
    for v in range(1, NVAR):
        t = t + proj[v] * inv[v]
    return t


def ridge(g):
    return K * (HALF * g), K * (HALF * g * g)


def past_mask():
    return lax.broadcasted_iota(jnp.int32, (R, K), 1) < K - 1


def nt(a, b):
    return lax.dot_general(a, b, (((1,), (1,)), ((), ())), preferred_element_type=F32)


def own_kernel(gnorm, mid, fh, fm, fl, ah, am, al, tail, twice, h, block):
    keep = past_mask()
    for m in range(COLS):

        def put(at, x, m=m):
            n = x.shape[0]
            fh[m, at : at + n], fm[m, at : at + n], fl[m, at : at + n] = split3(x)

        own_features(put, twice, m, mid[1 + m], keep)
    lin, quad = ridge(gnorm[0:1])
    sub, lane = iotas((8, 128))

    def gram(m, r0, r1, c0, c1):
        a = [f[m, r0:r1] for f in (fh, fm, fl)]
        b = [f[m, c0:c1] for f in (fh, fm, fl)]
        g = ((nt(a[1], b[1]) + nt(a[0], b[2])) + nt(a[2], b[0])) + (nt(a[0], b[1]) + nt(a[1], b[0]))
        return g + nt(a[0], b[0])

    def reg(row):
        if row < NQ or row == MIXED:
            return quad
        if row == MIXED + 8:
            return jnp.where(sub < 4, quad, jnp.where(sub == 4, lin, 1.0))
        return lin

    def ridged(x, row0):
        tiles = []
        for i in range(x.shape[0] // 8):
            tiles.append(x[8 * i : 8 * i + 8] + jnp.where(lane == sub + 8 * i, reg(row0 + 8 * i), 0.0))
        return jnp.concatenate(tiles, axis=0)

    for m in range(COLS):
        block[m] = ridged(gram(m, 0, 128, 0, 128), 0)

    def piece(m, kind):
        def go():
            if kind == 0:
                h[m, 0:128, 128:256] = gram(m, 0, 128, 128, 256)
            elif kind == 1:
                h[m, 128:OWN, 0:128] = gram(m, 128, OWN, 0, 128)
            elif kind == 2:
                h[m, 128:256, 128:256] = ridged(gram(m, 128, 256, 128, 256), 128)
            elif kind == 3:
                h[m, 256:OWN, 128:256] = gram(m, 256, OWN, 128, 256)
            else:
                h[m, :, 256:LANES] = jnp.zeros((OWN, 128), F32)
                h[m, 0:256, 256 : OWN + R] = gram(m, 0, 256, 256, OWN + R)
                h[m, 256:OWN, 256 : OWN + R] = gram(m, 256, OWN, 256, OWN + R)
                h[m, 256:OWN, 256:LANES] = ridged(h[m, 256:OWN, 256:LANES], 256)

        return go

    spread(invert(block, 16), 14, [piece(m, k) for k in range(5) for m in range(COLS)])
    inv0 = [block[m] for m in range(COLS)]
    for m in range(COLS):
        w = mm(inv0[m], h[m, 0:128, 128:256])
        block[m] = h[m, 128:256, 128:256] - mm(h[m, 128:256, 0:128], w)
        h[m, 0:128, 128:256] = w
        h[m, 0:128, 0:128] = inv0[m]

    def after0(m, kind):
        def go():
            if kind == 0:
                h[m, 0:128, 256:LANES] = mm(h[m, 0:128, 0:128], h[m, 0:128, 256:LANES])
            elif kind == 1:
                rows = slice(128, OWN)
                h[m, rows, 256:LANES] -= mm(h[m, rows, 0:128], h[m, 0:128, 256:LANES])
            elif kind == 2:
                rows = slice(256, OWN)
                h[m, rows, 128:256] -= mm(h[m, rows, 0:128], h[m, 0:128, 128:256])
            else:
                rows = slice(128, OWN)
                h[m, rows, 0:128] = -mm(h[m, rows, 0:128], h[m, 0:128, 0:128])

        return go

    spread(invert(block, 16), 14, [after0(m, k) for k in range(4) for m in range(COLS)])
    for m in range(COLS):
        h[m, 128:256, 128:256] = block[m]
        w = mm(block[m], h[m, 128:256, 256:LANES])
        block[m, 0:NEAR] = h[m, 256:OWN, 256:LANES] - mm(h[m, 256:OWN, 128:256], w)
        h[m, 128:256, 256:LANES] = w

    def after1(m, kind):
        def go():
            if kind == 0:
                h[m, 128:256, 0:128] = mm(h[m, 128:256, 128:256], h[m, 128:256, 0:128])
            elif kind == 1:
                h[m, 0:128, 256:LANES] -= mm(h[m, 0:128, 128:256], h[m, 128:256, 256:LANES])
            elif kind == 2:
                for rows in (slice(0, 128), slice(256, OWN)):
                    h[m, rows, 0:128] -= mm(h[m, rows, 128:256], h[m, 128:256, 0:128])
            else:
                for rows in (slice(0, 128), slice(256, OWN)):
                    h[m, rows, 128:256] = -mm(h[m, rows, 128:256], h[m, 128:256, 128:256])

        return go

    spread(invert(block, 9), 8, [after1(m, k) for k in range(4) for m in range(COLS)])
    _, _ = iotas((256, 128))
    for m in range(COLS):

        def put(rows, lanes, x, m=m):
            ah[m, rows, lanes], am[m, rows, lanes], al[m, rows, lanes] = split3(x)

        last = block[m, 0:NEAR]
        w = mm(first_lanes(last), to_rows(h[m, 256:OWN, 0:256], 128))
        part = h[m, 0:256, 256:LANES]
        lead = first_lanes(part)
        top, low = slice(0, 256), slice(256, OWN)
        left, right = slice(0, 256), slice(256, LANES)
        put(top, left, h[m, 0:256, 0:256] - mm(lead, to_rows(w, 128)))
        end = (part - lead) - mm(lead, to_rows(last, 128))
        put(top, right, end)
        tail[m, top] = end
        put(low, left, w)
        put(low, right, last)
        tail[m, low] = last


def fit_own(gnorm, mid):
    thirds = [pltpu.VMEM((COLS, OWN + R, K), BF)] * 3 + [pltpu.VMEM((COLS, OWN, LANES), BF)] * 3
    return pl.pallas_call(
        own_kernel,
        out_shape=thirds + [pltpu.VMEM((COLS, OWN, 128), F32)],
        scratch_shapes=[
            pltpu.VMEM((COLS, 2 * R, K), F32),
            pltpu.VMEM((COLS, OWN, LANES), F32),
            pltpu.VMEM((COLS, 128, 128), F32),
        ],
        compiler_params=pltpu.CompilerParams(vmem_limit_bytes=ROOM),
        name="fit_own",
    )(*on_chip(gnorm, mid))


def near_kernel(
    adjacency, gnorm, mid, up, down, fh, fm, fl, ah, am, al, tail, out, own, links, patch, block, x, order, sem
):
    fetch = pltpu.make_async_copy(adjacency, links, sem)
    fetch.start()
    row0 = lax.axis_index("gx_0") * 4 + lax.axis_index("gx_1")
    col0 = (lax.axis_index("gy_0") * 2 + lax.axis_index("gy_1")) * COLS
    keep = past_mask()
    lin, _ = ridge(gnorm[0:1])
    sub, lane = iotas((8, 128))
    for c in range(4):
        for r, source in enumerate((up, mid, down)):
            patch[4 * r + c] = jnp.where(keep, source[c], 0.0)
    own[0] = mid[1]
    own[1] = mid[2]
    gap = jnp.zeros((128 - NEAR, K), F32)
    fetch.wait()
    for m in range(COLS):
        rows = []
        for b in range(NB):
            link = links[0, m, b]
            rows.append(patch[((link >> 4) - row0 + 1) * 4 + ((link & 15) - col0 + 1)])
        nh, nm, nl = split3(jnp.concatenate(rows + [gap], axis=0))
        pair = jnp.concatenate([nh, nm], axis=0)
        a = [jnp.concatenate([f[m], n[0:80]], axis=0) for f, n in ((fh, nh), (fm, nm), (fl, nl))]
        p = nt(a[0], pair)
        q = nt(a[1], pair)
        r = nt(a[0], nl) + nt(a[2], nh)
        cross = p[:, 0:128] + ((p[:, 128:256] + q[:, 0:128]) + (q[:, 128:256] + r))
        turned = to_rows(cross[0 : OWN + R], LANES).T[0:NEAR]
        z = mm_thirds([t[m] for t in (ah, am, al)], to_rows(cross[0:OWN], LANES))
        both = jnp.where(iotas((OWN, 128))[1] < NEAR, z, tail[m])
        x[m, 0:OWN] = both
        _, lane_n = iotas((NEAR, 128))
        start = jnp.where(lane_n < NEAR, cross[OWN + R : OWN + R + NEAR], turned[:, 256:LANES])
        start = jnp.where(lane_n < NEAR + R, start, 0.0)
        start = jnp.concatenate(
            [start[8 * i : 8 * i + 8] + jnp.where(lane == sub + 8 * i, lin, 0.0) for i in range(NEAR // 8)], axis=0
        )
        turned = jnp.where(iotas((NEAR, LANES))[1] < OWN, turned, 0.0)
        block[m, 0:NEAR] = start - mm_thirds(split3(turned), to_rows(both, LANES))
    for _ in invert(block, 9):
        pass
    for m in range(COLS):
        last = block[m, 0:NEAR]
        both = x[m, 0:OWN]
        x[m, 0:OWN] = both - mm(first_lanes(both), to_rows(last, 128))
        order[m, 0:1] = x[m, MIXED + 12 : MIXED + 13]
        order[m, 1:25] = x[m, NQ : NQ + R]
        order[m, 25:97] = last
        dst = 97
        for a in range(R):
            for b in range(a, R):
                d = b - a
                if d == 12:
                    src = MIXED + a
                elif d < 12:
                    src = R * d + a
                else:
                    src = R * (R - d) + b
                order[m, dst : dst + 1] = x[m, src : src + 1]
                dst += 1
        flat = order[m].T
        out[m] = flat[NEAR : NEAR + R, 0:NF]


def fit_near(adjacency, *rest):
    vm = pl.BlockSpec(memory_space=pltpu.VMEM)
    return pl.pallas_call(
        near_kernel,
        in_specs=[pl.BlockSpec(memory_space=pl.ANY)] + [vm] * len(rest),
        out_specs=[vm, vm],
        out_shape=[
            jax.ShapeDtypeStruct((COLS, R, NF), F32),
            jax.ShapeDtypeStruct((COLS, R, K), F32),
        ],
        scratch_shapes=[
            pltpu.SMEM((1, COLS, NB), jnp.int32),
            pltpu.VMEM((12, R, K), F32),
            pltpu.VMEM((COLS, 128, 128), F32),
            pltpu.VMEM((COLS, OWN, 128), F32),
            pltpu.VMEM((COLS, 512, 128), F32),
            pltpu.SemaphoreType.DMA,
        ],
        compiler_params=pltpu.CompilerParams(vmem_limit_bytes=ROOM),
        name="fit_near",
    )(pltpu.with_memory_space_constraint(adjacency, pltpu.HBM), *on_chip(*rest))


def shifts(axis, x, y):
    n = lax.axis_size(axis)
    return (
        lax.ppermute(x, axis, [(i, i + 1) for i in range(n - 1)]),
        lax.ppermute(y, axis, [(i + 1, i) for i in range(n - 1)]),
    )


def body(snapshots, basis, node_counts, adjacency):
    proj0, proj1, stats = local_pass(snapshots[0], basis[0], node_counts)
    everyone = lax.all_to_all(stats, GX_GY, 0, 0, tiled=True)
    left, right = shifts(GY, proj1, proj0)
    mid, gnorm = global_states(everyone, left, proj0, proj1, right)
    up, down = shifts(GX, mid, mid)
    parts = fit_own(gnorm, mid)
    operator, own = fit_near(adjacency, gnorm, mid, up, down, *parts)
    return (jnp.swapaxes(operator, 1, 2)[None], own[None])


def solution(mesh):
    split = Mesh(mesh.devices.reshape(4, 4, 4, 2), ("gx_0", "gx_1", "gy_0", "gy_1"))
    placed = (P(GX, GY, None, None, None), P(GX, GY, None, None, None), P(GX, GY), P(GX, GY, None))
    return jax.shard_map(
        body,
        mesh=split,
        in_specs=placed,
        out_specs=(P(GX, GY, None, None), P(GX, GY, None, None)),
        check_vma=False,
    )
```

```python
import jax
import jax.numpy as jnp
from jax import lax
from jax.experimental import pallas as pl
from jax.experimental.pallas import tpu as pltpu
from jax.sharding import Mesh
from jax.sharding import PartitionSpec as P

GX = ("gx_0", "gx_1")
GY = ("gy_0", "gy_1")
GX_GY = ("gx_0", "gx_1", "gy_0", "gy_1")

R = 24
NVAR = 4
K = 512
SLOTS = 2048
COLS = 2
NB = 3
NF = 397
HALF = 0.5
F32 = jnp.float32
BF = jnp.bfloat16


def iotas(shape):
    return lax.broadcasted_iota(jnp.int32, shape, 0), lax.broadcasted_iota(jnp.int32, shape, 1)


DEPTH = 3
CUTS = 1
BLOCK = 256


def fold_lanes(x):
    return (x[:, 0:128] + x[:, 128:256]) + (x[:, 256:384] + x[:, 384:512])


def local_kernel(counts, basis, snaps, proj0, proj1, stats, modes, data, proj, acc, basis_sem, sems):
    steps = COLS * NVAR
    rows = SLOTS // CUTS

    def copy(i, c):
        part = pl.ds(c * rows, rows)
        return pltpu.make_async_copy(snaps.at[i // NVAR, i % NVAR, part], data.at[i, part], sems.at[i, c])

    def modes_copy(i):
        return pltpu.make_async_copy(basis.at[i // NVAR, i % NVAR], modes.at[i], basis_sem.at[i])

    for i in range(DEPTH):
        modes_copy(i).start()
        for c in range(CUTS):
            copy(i, c).start()
    acc[...] = jnp.zeros_like(acc)

    def step(i, carry):
        count = counts[0, i // NVAR]
        v = i % NVAR

        @pl.when(i + DEPTH < steps)
        def _():
            modes_copy(i + DEPTH).start()
            for c in range(CUTS):
                copy(i + DEPTH, c).start()

        modes_copy(i).wait()
        for c in range(CUTS):
            copy(i, c).wait()
        lane = lax.broadcasted_iota(jnp.int32, (R, BLOCK), 1)
        row = lax.broadcasted_iota(jnp.int32, (BLOCK, 128), 0)
        parts = []
        prods = []
        for lo in range(0, SLOTS, BLOCK):
            kept = jnp.where(lane < count - lo, modes[i, :, lo : lo + BLOCK], jnp.zeros((), BF))
            prods.append(jnp.dot(kept, data[i, lo : lo + BLOCK], preferred_element_type=F32))
            x = data[i, lo : lo + BLOCK, :].astype(F32)
            t = jnp.where(row < count - lo, fold_lanes(x * x), 0.0)
            parts.append(jnp.sum(t.reshape(BLOCK // 8, 8, 128), axis=0))
        proj[i] = sum(prods)
        part = sum(parts)
        acc[v] += part
        return carry

    lax.fori_loop(0, steps, step, 0)
    q = NVAR
    for a in range(NVAR):
        for b in range(a, NVAR):
            t = fold_lanes(proj[a] * proj[b]) + fold_lanes(proj[NVAR + a] * proj[NVAR + b])
            acc[q] = t[0:8] + t[8:16] + t[16:24]
            q += 1
    for v in range(NVAR):
        proj0[v] = proj[v]
        proj1[v] = proj[NVAR + v]
    total = jnp.sum(jnp.sum(acc[...], axis=1), axis=1, keepdims=True)
    i, j = iotas((16, 128))
    flat = jnp.sum(jnp.where(i == j, total, 0.0), axis=0, keepdims=True)
    nodes = (counts[0, 0] + counts[0, 1]).astype(F32)
    _, lane1 = iotas((1, 128))
    stats[...] = jnp.broadcast_to(jnp.where(lane1 == 14, nodes, flat), (128, 128))


ROOM = 36 << 20


def on_chip(*xs):
    return [pltpu.with_memory_space_constraint(x, pltpu.VMEM) for x in xs]


def local_pass(snapshots, basis, counts):
    vm = pl.BlockSpec(memory_space=pltpu.VMEM)
    hbm = pl.BlockSpec(memory_space=pl.ANY)
    return pl.pallas_call(
        local_kernel,
        in_specs=[pl.BlockSpec(memory_space=pltpu.SMEM), hbm, hbm],
        out_specs=[vm, vm, vm],
        out_shape=[
            pltpu.VMEM((NVAR, R, K), F32),
            pltpu.VMEM((NVAR, R, K), F32),
            pltpu.VMEM((128, 128), F32),
        ],
        scratch_shapes=[
            pltpu.VMEM((COLS * NVAR, R, SLOTS), BF),
            pltpu.VMEM((COLS * NVAR, SLOTS, K), BF),
            pltpu.VMEM((COLS * NVAR, R, K), F32),
            pltpu.VMEM((16, 8, 128), F32),
            pltpu.SemaphoreType.DMA((COLS * NVAR,)),
            pltpu.SemaphoreType.DMA((COLS * NVAR, CUTS)),
        ],
        compiler_params=pltpu.CompilerParams(vmem_limit_bytes=ROOM),
        name="local",
    )(*[pltpu.with_memory_space_constraint(x, pltpu.HBM) for x in (counts, basis, snapshots)])


OWN = 328
NQ = 288
MIXED = 312
FUT = OWN
NEAR = 72
LANES = 384


def lane_copy(x, at):
    return jnp.take_along_axis(x, jnp.full((8, 128), at, jnp.int32), axis=1)


def sub_copy(x, j):
    return jnp.broadcast_to(x[j : j + 1, :], (8, 128))


def split3(x):
    h = x.astype(BF)
    r = x - h.astype(F32)
    m = r.astype(BF)
    return h, m, (r - m.astype(F32)).astype(BF)


def dot(a, b):
    return jnp.dot(a, b, preferred_element_type=F32)


def mm(a, b):
    ah, am, al = split3(a)
    bh, bm, bl = split3(b)
    n = b.shape[1]
    w = jnp.concatenate([bh, bm], axis=1)
    p = dot(jnp.concatenate([ah, am], axis=1), jnp.concatenate([w, w], axis=0))
    q = dot(jnp.concatenate([ah, al], axis=1), jnp.concatenate([bl, bh], axis=0))
    return p[:, :n] + (p[:, n:] + q)


def mm_thirds(a, b):
    bh, bm, bl = split3(b)
    n = b.shape[1]
    w = jnp.concatenate([bh, bm], axis=1)
    p = dot(a[0], w)
    q = dot(a[1], w)
    r = dot(a[0], bl) + dot(a[2], bh)
    return p[:, :n] + ((p[:, n:] + q[:, :n]) + (q[:, n:] + r))


def first_lanes(x):
    return jnp.where(iotas(x.shape)[1] < NEAR, x, 0.0)


def to_rows(x, rows):
    return jnp.concatenate([x, jnp.zeros((rows - x.shape[0], x.shape[1]), F32)], axis=0)


def tree(terms):
    while len(terms) > 1:
        terms = [terms[i] + terms[i + 1] for i in range(0, len(terms) - 1, 2)] + terms[len(terms) // 2 * 2 :]
    return terms[0]


def padded_dot(a, w, lo):
    ah, am, al = split3(a)
    n = w.shape[0]
    parts = [jnp.zeros((lo, 128), F32)] * (lo > 0) + [w] + [jnp.zeros((128 - lo - n, 128), F32)] * (lo + n < 128)
    wh, wm, wl = split3(jnp.concatenate(parts, axis=0) if len(parts) > 1 else w)
    pair = jnp.concatenate([wh, wm], axis=1)
    u = dot(jnp.concatenate([ah, am], axis=1), jnp.concatenate([pair, pair], axis=0))
    v = dot(jnp.concatenate([ah, al], axis=1), jnp.concatenate([wl, wh], axis=0))
    return u[:, :128] + (u[:, 128:] + v)


def pivots(col, riders, sub):
    recips = jnp.zeros((8, 128), F32)
    diag = sub_copy(col[0], 0)
    for j in range(8):
        r = 1.0 / diag
        bare = jnp.where(sub == j, 0.0, col[j])
        recips = jnp.where(sub == j, r, recips)
        heads = {k: sub_copy(col[k], j) for k in range(j + 1, 8)}
        if j < 7:
            diag = sub_copy(col[j + 1], j + 1) - (sub_copy(col[j], j + 1) * heads[j + 1]) * r
        mult = bare * r
        for k in range(j + 1, 8):
            col[k] = col[k] - mult * heads[k]
        riders = [x - mult * sub_copy(x, j) for x in riders]
    return [x * recips for x in riders]


def invert(block, tiles, strip=2, look=1):
    sub, lane = iotas((8, 128))
    for s in range(0, tiles, strip):
        own = list(range(s, min(s + strip, tiles)))
        ahead = list(range(s + strip, min(s + strip + look, tiles)))
        for p in own:
            base = 8 * p
            inside = (lane >= base) & (lane < base + 8)
            unit = jnp.where(lane - base == sub, 1.0, 0.0)
            ws = []
            for m in range(COLS):
                tile = block[m, base : base + 8, :]
                col = [lane_copy(tile, base + k) for k in range(8)]
                w = pivots(col, [jnp.where(inside, unit, tile)], sub)[0]
                block[m, base : base + 8, :] = w
                ws.append([sub_copy(w, j) for j in range(8)])
            for t in [t for t in own + ahead if t > p] + [t for t in own if t < p]:
                for m in range(COLS):
                    a = block[m, 8 * t : 8 * t + 8, :]
                    delta = tree([lane_copy(a, base + j) * ws[m][j] for j in range(8)])
                    block[m, 8 * t : 8 * t + 8, :] = jnp.where(inside, 0.0, a) - delta
            yield
        lo, hi = 8 * s, 8 * (own[-1] + 1)
        ranges = [(a, b) for a, b in ((hi + 8 * len(ahead), 8 * tiles), (0, lo)) if a < b]
        if ranges:
            for m in range(COLS):
                rest = [block[m, a:b, :] for a, b in ranges]
                rest = jnp.concatenate(rest, axis=0) if len(rest) > 1 else rest[0]
                _, wide_l = iotas(rest.shape)
                kept = jnp.where((wide_l >= lo) & (wide_l < hi), 0.0, rest)
                new = kept - padded_dot(rest, block[m, lo:hi, :], lo)
                at = 0
                for a, b in ranges:
                    block[m, a:b, :] = new[at : at + b - a]
                    at += b - a


def spread(panels, count, work):
    work = list(work)
    done = 0
    for i, _ in enumerate(panels):
        want = (i + 1) * len(work) // count if i + 1 < count else len(work)
        while done < min(want, len(work)):
            work[done]()
            done += 1
    for f in work[done:]:
        f()


def states_kernel(everyone, left, proj0, proj1, right, mid, gnorm):
    found = global_scales(everyone)
    gnorm[...] = jnp.broadcast_to(found[NVAR], (8, 128))
    inv = [x[:, 0:1] for x in found]
    for c, proj in enumerate((left, proj0, proj1, right)):
        mid[c] = scaled_sum(proj, inv)


def global_states(everyone, left, proj0, proj1, right):
    return pl.pallas_call(
        states_kernel,
        out_shape=[pltpu.VMEM((4, R, K), F32), pltpu.VMEM((8, 128), F32)],
        compiler_params=pltpu.CompilerParams(vmem_limit_bytes=ROOM),
        name="states",
    )(*on_chip(everyone, left, proj0, proj1, right))


def own_features(feats, twice, m, state, keep):
    past = jnp.where(keep, state, 0.0)
    twice[m, 0:R] = past
    twice[m, R : 2 * R] = past
    for d in range(12):
        feats(R * d, past * twice[m, d : d + R])
    feats(NQ, past)
    row, lane = iotas((16, K))
    one = jnp.where((row == 12) & (lane < K - 1), 1.0, 0.0)
    feats(MIXED, jnp.where(row < 12, twice[m, 0:16] * twice[m, 12:28], one))
    feats(FUT, pltpu.roll(state, K - 1, 1))


def global_scales(everyone):
    total = jnp.sum(everyone[...], axis=0, keepdims=True)
    nodes = total[:, 14:15]
    inv = []
    for v in range(NVAR):
        inv.append(1.0 / jnp.sqrt(total[:, v : v + 1] / (nodes * K) + 1e-06))
    g = jnp.zeros((1, 1), F32)
    q = NVAR
    for a in range(NVAR):
        for b in range(a, NVAR):
            term = total[:, q : q + 1] * inv[a] * inv[b]
            g = g + (term if a == b else 2.0 * term)
            q += 1
    return [jnp.broadcast_to(x, (1, 128)) for x in inv + [g * (1.0 / (256 * R * K))]]


def scaled_sum(proj, inv):
    t = proj[0] * inv[0]
    for v in range(1, NVAR):
        t = t + proj[v] * inv[v]
    return t


def ridge(g):
    return K * (HALF * g), K * (HALF * g * g)


def past_mask():
    return lax.broadcasted_iota(jnp.int32, (R, K), 1) < K - 1


def nt(a, b):
    return lax.dot_general(a, b, (((1,), (1,)), ((), ())), preferred_element_type=F32)


def own_kernel(gnorm, mid, fh, fm, fl, ah, am, al, tail, twice, h, block):
    keep = past_mask()
    for m in range(COLS):

        def put(at, x, m=m):
            n = x.shape[0]
            fh[m, at : at + n], fm[m, at : at + n], fl[m, at : at + n] = split3(x)

        own_features(put, twice, m, mid[1 + m], keep)
    lin, quad = ridge(gnorm[0:1])
    sub, lane = iotas((8, 128))

    def thirds(m, lo, hi):
        return [f[m, lo:hi] for f in (fh, fm, fl)]

    def gram(m, r0, r1, c0, c1):
        want = r1 - r0
        size = -(-want // 16) * 16
        a, b = thirds(m, r0, r0 + size), thirds(m, c0, c1)
        n = c1 - c0
        top, mid, low = slice(0, size), slice(size, 2 * size), slice(2 * size, 3 * size)
        if n > 128:
            x = nt(jnp.concatenate(a, axis=0), b[0])
            y = nt(jnp.concatenate(a[:2], axis=0), b[1])
            g = (((y[mid] + nt(a[0], b[2])) + x[low]) + (y[top] + x[mid])) + x[top]
            return g[0:want]
        gap = [jnp.zeros((128 - n, K), BF)] * (n < 128)
        pair = jnp.concatenate([b[0]] + gap + [b[1]] + gap, axis=0)
        p = nt(jnp.concatenate(a[:2], axis=0), pair)
        r = nt(a[0], b[2]) + nt(a[2], b[0])
        one, two = slice(0, n), slice(128, 128 + n)
        g = p[top, one] + ((p[top, two] + p[mid, one]) + (p[mid, two] + r))
        return g[0:want]

    def reg(row):
        if row < NQ or row == MIXED:
            return quad
        if row == MIXED + 8:
            return jnp.where(sub < 4, quad, jnp.where(sub == 4, lin, 1.0))
        return lin

    def ridged(x, row0):
        tiles = []
        for i in range(x.shape[0] // 8):
            tiles.append(x[8 * i : 8 * i + 8] + jnp.where(lane == sub + 8 * i, reg(row0 + 8 * i), 0.0))
        return jnp.concatenate(tiles, axis=0)

    for m in range(COLS):
        block[m] = ridged(gram(m, 0, 128, 0, 128), 0)

    def piece(m, kind):
        def go():
            if kind == 0:
                h[m, 0:128, 256:LANES] = jnp.zeros((128, 128), F32)
                h[m, 0:128, 128 : OWN + R] = gram(m, 0, 128, 128, OWN + R)
            elif kind == 1:
                g = gram(m, 128, 256, 0, 256)
                h[m, 128:256, 0:128] = g[:, 0:128]
                h[m, 128:256, 128:256] = ridged(g[:, 128:256], 128)
            elif kind == 2:
                h[m, 256:OWN, 0:256] = gram(m, 256, OWN, 0, 256)
            else:
                h[m, 128:OWN, 256:LANES] = jnp.zeros((OWN - 128, 128), F32)
                h[m, 128:OWN, 256 : OWN + R] = gram(m, 128, OWN, 256, OWN + R)
                h[m, 256:OWN, 256:LANES] = ridged(h[m, 256:OWN, 256:LANES], 256)

        return go

    spread(invert(block, 16), 14, [piece(m, k) for k in range(4) for m in range(COLS)])
    inv0 = [block[m] for m in range(COLS)]
    for m in range(COLS):
        w = mm(inv0[m], h[m, 0:128, 128:256])
        block[m] = h[m, 128:256, 128:256] - mm(h[m, 128:256, 0:128], w)
        h[m, 0:128, 128:256] = w
        h[m, 0:128, 0:128] = inv0[m]

    def after0(m, kind):
        def go():
            if kind == 0:
                h[m, 0:128, 256:LANES] = mm(h[m, 0:128, 0:128], h[m, 0:128, 256:LANES])
            elif kind == 1:
                rows = slice(128, OWN)
                h[m, rows, 256:LANES] -= mm(h[m, rows, 0:128], h[m, 0:128, 256:LANES])
            elif kind == 2:
                rows = slice(256, OWN)
                h[m, rows, 128:256] -= mm(h[m, rows, 0:128], h[m, 0:128, 128:256])
            else:
                rows = slice(128, OWN)
                h[m, rows, 0:128] = -mm(h[m, rows, 0:128], h[m, 0:128, 0:128])

        return go

    spread(invert(block, 16), 14, [after0(m, k) for k in range(4) for m in range(COLS)])
    for m in range(COLS):
        h[m, 128:256, 128:256] = block[m]
        w = mm(block[m], h[m, 128:256, 256:LANES])
        block[m, 0:NEAR] = h[m, 256:OWN, 256:LANES] - mm(h[m, 256:OWN, 128:256], w)
        h[m, 128:256, 256:LANES] = w

    def after1(m, kind):
        def go():
            if kind == 0:
                h[m, 128:256, 0:128] = mm(h[m, 128:256, 128:256], h[m, 128:256, 0:128])
            elif kind == 1:
                h[m, 0:128, 256:LANES] -= mm(h[m, 0:128, 128:256], h[m, 128:256, 256:LANES])
            elif kind == 2:
                for rows in (slice(0, 128), slice(256, OWN)):
                    h[m, rows, 0:128] -= mm(h[m, rows, 128:256], h[m, 128:256, 0:128])
            else:
                for rows in (slice(0, 128), slice(256, OWN)):
                    h[m, rows, 128:256] = -mm(h[m, rows, 128:256], h[m, 128:256, 128:256])

        return go

    spread(invert(block, 9), 8, [after1(m, k) for k in range(4) for m in range(COLS)])
    _, _ = iotas((256, 128))
    for m in range(COLS):

        def put(rows, lanes, x, m=m):
            ah[m, rows, lanes], am[m, rows, lanes], al[m, rows, lanes] = split3(x)

        last = block[m, 0:NEAR]
        w = mm(first_lanes(last), to_rows(h[m, 256:OWN, 0:256], 128))
        part = h[m, 0:256, 256:LANES]
        lead = first_lanes(part)
        top, low = slice(0, 256), slice(256, OWN)
        left, right = slice(0, 256), slice(256, LANES)
        put(top, left, h[m, 0:256, 0:256] - mm(lead, to_rows(w, 128)))
        end = (part - lead) - mm(lead, to_rows(last, 128))
        put(top, right, end)
        tail[m, top] = end
        put(low, left, w)
        put(low, right, last)
        tail[m, low] = last


def fit_own(gnorm, mid):
    thirds = [pltpu.VMEM((COLS, OWN + R, K), BF)] * 3 + [pltpu.VMEM((COLS, OWN, LANES), BF)] * 3
    return pl.pallas_call(
        own_kernel,
        out_shape=thirds + [pltpu.VMEM((COLS, OWN, 128), F32)],
        scratch_shapes=[
            pltpu.VMEM((COLS, 2 * R, K), F32),
            pltpu.VMEM((COLS, OWN, LANES), F32),
            pltpu.VMEM((COLS, 128, 128), F32),
        ],
        compiler_params=pltpu.CompilerParams(vmem_limit_bytes=ROOM),
        name="fit_own",
    )(*on_chip(gnorm, mid))


def near_kernel(
    adjacency, gnorm, mid, up, down, fh, fm, fl, ah, am, al, tail, out, own, links, patch, block, x, order, sem
):
    fetch = pltpu.make_async_copy(adjacency, links, sem)
    fetch.start()
    row0 = lax.axis_index("gx_0") * 4 + lax.axis_index("gx_1")
    col0 = (lax.axis_index("gy_0") * 2 + lax.axis_index("gy_1")) * COLS
    keep = past_mask()
    lin, _ = ridge(gnorm[0:1])
    sub, lane = iotas((8, 128))
    for c in range(4):
        for r, source in enumerate((up, mid, down)):
            patch[4 * r + c] = jnp.where(keep, source[c], 0.0)
    own[0] = mid[1]
    own[1] = mid[2]
    gap = jnp.zeros((128 - NEAR, K), F32)
    fetch.wait()
    for m in range(COLS):
        rows = []
        for b in range(NB):
            link = links[0, m, b]
            rows.append(patch[((link >> 4) - row0 + 1) * 4 + ((link & 15) - col0 + 1)])
        nh, nm, nl = split3(jnp.concatenate(rows + [gap], axis=0))
        pair = jnp.concatenate([nh, nm], axis=0)
        a = [jnp.concatenate([f[m], n[0:80]], axis=0) for f, n in ((fh, nh), (fm, nm), (fl, nl))]
        size = OWN + R + 80
        p = nt(jnp.concatenate(a[:2], axis=0), pair)
        r = nt(a[0], nl) + nt(a[2], nh)
        top, mid_rows = slice(0, size), slice(size, 2 * size)
        cross = p[top, 0:128] + ((p[top, 128:256] + p[mid_rows, 0:128]) + (p[mid_rows, 128:256] + r))
        turned = to_rows(cross[0 : OWN + R], LANES).T[0:NEAR]
        z = mm_thirds([t[m] for t in (ah, am, al)], to_rows(cross[0:OWN], LANES))
        both = jnp.where(iotas((OWN, 128))[1] < NEAR, z, tail[m])
        x[m, 0:OWN] = both
        _, lane_n = iotas((NEAR, 128))
        start = jnp.where(lane_n < NEAR, cross[OWN + R : OWN + R + NEAR], turned[:, 256:LANES])
        start = jnp.where(lane_n < NEAR + R, start, 0.0)
        start = jnp.concatenate(
            [start[8 * i : 8 * i + 8] + jnp.where(lane == sub + 8 * i, lin, 0.0) for i in range(NEAR // 8)], axis=0
        )
        turned = jnp.where(iotas((NEAR, LANES))[1] < OWN, turned, 0.0)
        block[m, 0:NEAR] = start - mm_thirds(split3(turned), to_rows(both, LANES))
    for _ in invert(block, 9):
        pass
    for m in range(COLS):
        last = block[m, 0:NEAR]
        both = x[m, 0:OWN]
        x[m, 0:OWN] = both - mm(first_lanes(both), to_rows(last, 128))
        order[m, 0:1] = x[m, MIXED + 12 : MIXED + 13]
        order[m, 1:25] = x[m, NQ : NQ + R]
        order[m, 25:97] = last
        dst = 97
        for a in range(R):
            for b in range(a, R):
                d = b - a
                if d == 12:
                    src = MIXED + a
                elif d < 12:
                    src = R * d + a
                else:
                    src = R * (R - d) + b
                order[m, dst : dst + 1] = x[m, src : src + 1]
                dst += 1
        flat = order[m].T
        out[m] = flat[NEAR : NEAR + R, 0:NF]


def fit_near(adjacency, *rest):
    vm = pl.BlockSpec(memory_space=pltpu.VMEM)
    return pl.pallas_call(
        near_kernel,
        in_specs=[pl.BlockSpec(memory_space=pl.ANY)] + [vm] * len(rest),
        out_specs=[vm, vm],
        out_shape=[
            jax.ShapeDtypeStruct((COLS, R, NF), F32),
            jax.ShapeDtypeStruct((COLS, R, K), F32),
        ],
        scratch_shapes=[
            pltpu.SMEM((1, COLS, NB), jnp.int32),
            pltpu.VMEM((12, R, K), F32),
            pltpu.VMEM((COLS, 128, 128), F32),
            pltpu.VMEM((COLS, OWN, 128), F32),
            pltpu.VMEM((COLS, 512, 128), F32),
            pltpu.SemaphoreType.DMA,
        ],
        compiler_params=pltpu.CompilerParams(vmem_limit_bytes=ROOM),
        name="fit_near",
    )(pltpu.with_memory_space_constraint(adjacency, pltpu.HBM), *on_chip(*rest))


def shifts(axis, x, y):
    n = lax.axis_size(axis)
    return (
        lax.ppermute(x, axis, [(i, i + 1) for i in range(n - 1)]),
        lax.ppermute(y, axis, [(i + 1, i) for i in range(n - 1)]),
    )


def body(snapshots, basis, node_counts, adjacency):
    proj0, proj1, stats = local_pass(snapshots[0], basis[0], node_counts)
    everyone = lax.all_to_all(stats, GX_GY, 0, 0, tiled=True)
    left, right = shifts(GY, proj1, proj0)
    mid, gnorm = global_states(everyone, left, proj0, proj1, right)
    up, down = shifts(GX, mid, mid)
    parts = fit_own(gnorm, mid)
    operator, own = fit_near(adjacency, gnorm, mid, up, down, *parts)
    return (jnp.swapaxes(operator, 1, 2)[None], own[None])


def solution(mesh):
    split = Mesh(mesh.devices.reshape(4, 4, 4, 2), ("gx_0", "gx_1", "gy_0", "gy_1"))
    placed = (P(GX, GY, None, None, None), P(GX, GY, None, None, None), P(GX, GY), P(GX, GY, None))
    return jax.shard_map(
        body,
        mesh=split,
        in_specs=placed,
        out_specs=(P(GX, GY, None, None), P(GX, GY, None, None)),
        check_vma=False,
    )
```

```python
import jax
import jax.numpy as jnp
from jax import lax
from jax.experimental import pallas as pl
from jax.experimental.pallas import tpu as pltpu
from jax.sharding import Mesh
from jax.sharding import PartitionSpec as P

GX = ("gx_0", "gx_1")
GY = ("gy_0", "gy_1")
GX_GY = ("gx_0", "gx_1", "gy_0", "gy_1")

R = 24
NVAR = 4
K = 512
SLOTS = 2048
COLS = 2
NB = 3
NF = 397
HALF = 0.5
F32 = jnp.float32
BF = jnp.bfloat16


def iotas(shape):
    return lax.broadcasted_iota(jnp.int32, shape, 0), lax.broadcasted_iota(jnp.int32, shape, 1)


DEPTH = 3
CUTS = 1
BLOCK = 256


def fold_lanes(x):
    return (x[:, 0:128] + x[:, 128:256]) + (x[:, 256:384] + x[:, 384:512])


def local_kernel(counts, basis, snaps, proj0, proj1, stats, modes, data, proj, acc, basis_sem, sems):
    steps = COLS * NVAR
    rows = SLOTS // CUTS

    def copy(i, c):
        part = pl.ds(c * rows, rows)
        return pltpu.make_async_copy(snaps.at[i // NVAR, i % NVAR, part], data.at[i, part], sems.at[i, c])

    def modes_copy(i):
        return pltpu.make_async_copy(basis.at[i // NVAR, i % NVAR], modes.at[i], basis_sem.at[i])

    for i in range(DEPTH):
        modes_copy(i).start()
        for c in range(CUTS):
            copy(i, c).start()
    acc[...] = jnp.zeros_like(acc)

    def step(i, carry):
        count = counts[0, i // NVAR]
        v = i % NVAR

        @pl.when(i + DEPTH < steps)
        def _():
            modes_copy(i + DEPTH).start()
            for c in range(CUTS):
                copy(i + DEPTH, c).start()

        modes_copy(i).wait()
        for c in range(CUTS):
            copy(i, c).wait()
        lane = lax.broadcasted_iota(jnp.int32, (R, BLOCK), 1)
        row = lax.broadcasted_iota(jnp.int32, (BLOCK, 128), 0)
        parts = []
        prods = []
        for lo in range(0, SLOTS, BLOCK):
            kept = jnp.where(lane < count - lo, modes[i, :, lo : lo + BLOCK], jnp.zeros((), BF))
            prods.append(jnp.dot(kept, data[i, lo : lo + BLOCK], preferred_element_type=F32))
            x = data[i, lo : lo + BLOCK, :].astype(F32)
            t = jnp.where(row < count - lo, fold_lanes(x * x), 0.0)
            parts.append(jnp.sum(t.reshape(BLOCK // 8, 8, 128), axis=0))
        proj[i] = sum(prods)
        part = sum(parts)
        acc[v] += part
        return carry

    lax.fori_loop(0, steps, step, 0)
    q = NVAR
    for a in range(NVAR):
        for b in range(a, NVAR):
            t = fold_lanes(proj[a] * proj[b]) + fold_lanes(proj[NVAR + a] * proj[NVAR + b])
            acc[q] = t[0:8] + t[8:16] + t[16:24]
            q += 1
    for v in range(NVAR):
        proj0[v] = proj[v]
        proj1[v] = proj[NVAR + v]
    total = jnp.sum(jnp.sum(acc[...], axis=1), axis=1, keepdims=True)
    i, j = iotas((16, 128))
    flat = jnp.sum(jnp.where(i == j, total, 0.0), axis=0, keepdims=True)
    nodes = (counts[0, 0] + counts[0, 1]).astype(F32)
    _, lane1 = iotas((1, 128))
    stats[...] = jnp.broadcast_to(jnp.where(lane1 == 14, nodes, flat), (128, 128))


ROOM = 36 << 20


def on_chip(*xs):
    return [pltpu.with_memory_space_constraint(x, pltpu.VMEM) for x in xs]


def local_pass(snapshots, basis, counts):
    vm = pl.BlockSpec(memory_space=pltpu.VMEM)
    hbm = pl.BlockSpec(memory_space=pl.ANY)
    return pl.pallas_call(
        local_kernel,
        in_specs=[pl.BlockSpec(memory_space=pltpu.SMEM), hbm, hbm],
        out_specs=[vm, vm, vm],
        out_shape=[
            pltpu.VMEM((NVAR, R, K), F32),
            pltpu.VMEM((NVAR, R, K), F32),
            pltpu.VMEM((128, 128), F32),
        ],
        scratch_shapes=[
            pltpu.VMEM((COLS * NVAR, R, SLOTS), BF),
            pltpu.VMEM((COLS * NVAR, SLOTS, K), BF),
            pltpu.VMEM((COLS * NVAR, R, K), F32),
            pltpu.VMEM((16, 8, 128), F32),
            pltpu.SemaphoreType.DMA((COLS * NVAR,)),
            pltpu.SemaphoreType.DMA((COLS * NVAR, CUTS)),
        ],
        compiler_params=pltpu.CompilerParams(vmem_limit_bytes=ROOM),
        name="local",
    )(*[pltpu.with_memory_space_constraint(x, pltpu.HBM) for x in (counts, basis, snapshots)])


OWN = 328
NQ = 288
MIXED = 312
FUT = OWN
NEAR = 72
LANES = 384


def lane_copy(x, at):
    return jnp.take_along_axis(x, jnp.full((8, 128), at, jnp.int32), axis=1)


def sub_copy(x, j):
    return jnp.broadcast_to(x[j : j + 1, :], (8, 128))


def split3(x):
    h = x.astype(BF)
    r = x - h.astype(F32)
    m = r.astype(BF)
    return h, m, (r - m.astype(F32)).astype(BF)


def dot(a, b):
    return jnp.dot(a, b, preferred_element_type=F32)


def mm(a, b):
    ah, am, al = split3(a)
    bh, bm, bl = split3(b)
    n = b.shape[1]
    w = jnp.concatenate([bh, bm], axis=1)
    p = dot(jnp.concatenate([ah, am], axis=1), jnp.concatenate([w, w], axis=0))
    q = dot(jnp.concatenate([ah, al], axis=1), jnp.concatenate([bl, bh], axis=0))
    return p[:, :n] + (p[:, n:] + q)


def mm_thirds(a, b):
    bh, bm, bl = split3(b)
    n = b.shape[1]
    w = jnp.concatenate([bh, bm], axis=1)
    p = dot(a[0], w)
    q = dot(a[1], w)
    r = dot(a[0], bl) + dot(a[2], bh)
    return p[:, :n] + ((p[:, n:] + q[:, :n]) + (q[:, n:] + r))


def first_lanes(x):
    return jnp.where(iotas(x.shape)[1] < NEAR, x, 0.0)


def to_rows(x, rows):
    return jnp.concatenate([x, jnp.zeros((rows - x.shape[0], x.shape[1]), F32)], axis=0)


def tree(terms):
    while len(terms) > 1:
        terms = [terms[i] + terms[i + 1] for i in range(0, len(terms) - 1, 2)] + terms[len(terms) // 2 * 2 :]
    return terms[0]


def padded_dot(a, w, lo):
    ah, am, al = split3(a)
    n = w.shape[0]
    parts = [jnp.zeros((lo, 128), F32)] * (lo > 0) + [w] + [jnp.zeros((128 - lo - n, 128), F32)] * (lo + n < 128)
    wh, wm, wl = split3(jnp.concatenate(parts, axis=0) if len(parts) > 1 else w)
    pair = jnp.concatenate([wh, wm], axis=1)
    u = dot(jnp.concatenate([ah, am], axis=1), jnp.concatenate([pair, pair], axis=0))
    v = dot(jnp.concatenate([ah, al], axis=1), jnp.concatenate([wl, wh], axis=0))
    return u[:, :128] + (u[:, 128:] + v)


def pivots(col, riders, sub):
    recips = jnp.zeros((8, 128), F32)
    diag = sub_copy(col[0], 0)
    for j in range(8):
        r = 1.0 / diag
        bare = jnp.where(sub == j, 0.0, col[j])
        recips = jnp.where(sub == j, r, recips)
        heads = {k: sub_copy(col[k], j) for k in range(j + 1, 8)}
        if j < 7:
            diag = sub_copy(col[j + 1], j + 1) - (sub_copy(col[j], j + 1) * heads[j + 1]) * r
        mult = bare * r
        for k in range(j + 1, 8):
            col[k] = col[k] - mult * heads[k]
        riders = [x - mult * sub_copy(x, j) for x in riders]
    return [x * recips for x in riders]


def invert(block, tiles, strip=2, look=1):
    sub, lane = iotas((8, 128))
    for s in range(0, tiles, strip):
        own = list(range(s, min(s + strip, tiles)))
        ahead = list(range(s + strip, min(s + strip + look, tiles)))
        for p in own:
            base = 8 * p
            inside = (lane >= base) & (lane < base + 8)
            unit = jnp.where(lane - base == sub, 1.0, 0.0)
            ws = []
            for m in range(COLS):
                tile = block[m, base : base + 8, :]
                col = [lane_copy(tile, base + k) for k in range(8)]
                w = pivots(col, [jnp.where(inside, unit, tile)], sub)[0]
                block[m, base : base + 8, :] = w
                ws.append([sub_copy(w, j) for j in range(8)])
            for t in [t for t in own + ahead if t > p] + [t for t in own if t < p]:
                for m in range(COLS):
                    a = block[m, 8 * t : 8 * t + 8, :]
                    delta = tree([lane_copy(a, base + j) * ws[m][j] for j in range(8)])
                    block[m, 8 * t : 8 * t + 8, :] = jnp.where(inside, 0.0, a) - delta
            yield
        lo, hi = 8 * s, 8 * (own[-1] + 1)
        ranges = [(a, b) for a, b in ((hi + 8 * len(ahead), 8 * tiles), (0, lo)) if a < b]
        if ranges:
            for m in range(COLS):
                rest = [block[m, a:b, :] for a, b in ranges]
                rest = jnp.concatenate(rest, axis=0) if len(rest) > 1 else rest[0]
                _, wide_l = iotas(rest.shape)
                kept = jnp.where((wide_l >= lo) & (wide_l < hi), 0.0, rest)
                new = kept - padded_dot(rest, block[m, lo:hi, :], lo)
                at = 0
                for a, b in ranges:
                    block[m, a:b, :] = new[at : at + b - a]
                    at += b - a


def spread(panels, count, work):
    work = list(work)
    done = 0
    for i, _ in enumerate(panels):
        want = (i + 1) * len(work) // count if i + 1 < count else len(work)
        while done < min(want, len(work)):
            work[done]()
            done += 1
    for f in work[done:]:
        f()


def states_kernel(everyone, left, proj0, proj1, right, mid, gnorm):
    found = global_scales(everyone)
    gnorm[...] = jnp.broadcast_to(found[NVAR], (8, 128))
    inv = [x[:, 0:1] for x in found]
    for c, proj in enumerate((left, proj0, proj1, right)):
        mid[c] = scaled_sum(proj, inv)


def global_states(everyone, left, proj0, proj1, right):
    return pl.pallas_call(
        states_kernel,
        out_shape=[pltpu.VMEM((4, R, K), F32), pltpu.VMEM((8, 128), F32)],
        compiler_params=pltpu.CompilerParams(vmem_limit_bytes=ROOM),
        name="states",
    )(*on_chip(everyone, left, proj0, proj1, right))


def own_features(feats, twice, m, state, keep):
    past = jnp.where(keep, state, 0.0)
    twice[m, 0:R] = past
    twice[m, R : 2 * R] = past
    for d in range(12):
        feats(R * d, past * twice[m, d : d + R])
    feats(NQ, past)
    row, lane = iotas((16, K))
    one = jnp.where((row == 12) & (lane < K - 1), 1.0, 0.0)
    feats(MIXED, jnp.where(row < 12, twice[m, 0:16] * twice[m, 12:28], one))
    feats(FUT, pltpu.roll(state, K - 1, 1))


def global_scales(everyone):
    total = jnp.sum(everyone[...], axis=0, keepdims=True)
    nodes = total[:, 14:15]
    inv = []
    for v in range(NVAR):
        inv.append(1.0 / jnp.sqrt(total[:, v : v + 1] / (nodes * K) + 1e-06))
    g = jnp.zeros((1, 1), F32)
    q = NVAR
    for a in range(NVAR):
        for b in range(a, NVAR):
            term = total[:, q : q + 1] * inv[a] * inv[b]
            g = g + (term if a == b else 2.0 * term)
            q += 1
    return [jnp.broadcast_to(x, (1, 128)) for x in inv + [g * (1.0 / (256 * R * K))]]


def scaled_sum(proj, inv):
    t = proj[0] * inv[0]
    for v in range(1, NVAR):
        t = t + proj[v] * inv[v]
    return t


def ridge(g):
    return K * (HALF * g), K * (HALF * g * g)


def past_mask():
    return lax.broadcasted_iota(jnp.int32, (R, K), 1) < K - 1


def nt(a, b):
    return lax.dot_general(a, b, (((1,), (1,)), ((), ())), preferred_element_type=F32)


def own_kernel(gnorm, mid, fh, fm, fl, h, block, twice):
    keep = past_mask()
    for m in range(COLS):

        def put(at, x, m=m):
            n = x.shape[0]
            fh[m, at : at + n], fm[m, at : at + n], fl[m, at : at + n] = split3(x)

        own_features(put, twice, m, mid[1 + m], keep)
    lin, quad = ridge(gnorm[0:1])
    sub, lane = iotas((8, 128))

    def thirds(m, lo, hi):
        return [f[m, lo:hi] for f in (fh, fm, fl)]

    def gram(m, r0, r1, c0, c1):
        want = r1 - r0
        size = -(-want // 16) * 16
        a, b = thirds(m, r0, r0 + size), thirds(m, c0, c1)
        n = c1 - c0
        top, mid, low = slice(0, size), slice(size, 2 * size), slice(2 * size, 3 * size)
        if n > 128:
            x = nt(jnp.concatenate(a, axis=0), b[0])
            y = nt(jnp.concatenate(a[:2], axis=0), b[1])
            g = (((y[mid] + nt(a[0], b[2])) + x[low]) + (y[top] + x[mid])) + x[top]
            return g[0:want]
        gap = [jnp.zeros((128 - n, K), BF)] * (n < 128)
        pair = jnp.concatenate([b[0]] + gap + [b[1]] + gap, axis=0)
        p = nt(jnp.concatenate(a[:2], axis=0), pair)
        r = nt(a[0], b[2]) + nt(a[2], b[0])
        one, two = slice(0, n), slice(128, 128 + n)
        g = p[top, one] + ((p[top, two] + p[mid, one]) + (p[mid, two] + r))
        return g[0:want]

    def reg(row):
        if row < NQ or row == MIXED:
            return quad
        if row == MIXED + 8:
            return jnp.where(sub < 4, quad, jnp.where(sub == 4, lin, 1.0))
        return lin

    def ridged(x, row0):
        tiles = []
        for i in range(x.shape[0] // 8):
            tiles.append(x[8 * i : 8 * i + 8] + jnp.where(lane == sub + 8 * i, reg(row0 + 8 * i), 0.0))
        return jnp.concatenate(tiles, axis=0)

    for m in range(COLS):
        block[m] = ridged(gram(m, 0, 128, 0, 128), 0)

    def piece(m, kind):
        def go():
            if kind == 0:
                h[m, 0:128, 256:LANES] = jnp.zeros((128, 128), F32)
                h[m, 0:128, 128 : OWN + R] = gram(m, 0, 128, 128, OWN + R)
            elif kind == 1:
                g = gram(m, 128, 256, 0, 256)
                h[m, 128:256, 0:128] = g[:, 0:128]
                h[m, 128:256, 128:256] = ridged(g[:, 128:256], 128)
            elif kind == 2:
                h[m, 256:OWN, 0:256] = gram(m, 256, OWN, 0, 256)
            else:
                h[m, 128:OWN, 256:LANES] = jnp.zeros((OWN - 128, 128), F32)
                h[m, 128:OWN, 256 : OWN + R] = gram(m, 128, OWN, 256, OWN + R)
                h[m, 256:OWN, 256:LANES] = ridged(h[m, 256:OWN, 256:LANES], 256)

        return go

    spread(invert(block, 16), 14, [piece(m, k) for k in range(4) for m in range(COLS)])
    inv0 = [block[m] for m in range(COLS)]
    for m in range(COLS):
        w = mm(inv0[m], h[m, 0:128, 128:256])
        block[m] = h[m, 128:256, 128:256] - mm(h[m, 128:256, 0:128], w)
        h[m, 0:128, 128:256] = w
        h[m, 0:128, 0:128] = inv0[m]

    def after0(m, kind):
        def go():
            if kind == 0:
                h[m, 0:128, 256:LANES] = mm(h[m, 0:128, 0:128], h[m, 0:128, 256:LANES])
            elif kind == 1:
                rows = slice(128, OWN)
                h[m, rows, 256:LANES] -= mm(h[m, rows, 0:128], h[m, 0:128, 256:LANES])
            elif kind == 2:
                rows = slice(256, OWN)
                h[m, rows, 128:256] -= mm(h[m, rows, 0:128], h[m, 0:128, 128:256])
            else:
                rows = slice(128, OWN)
                h[m, rows, 0:128] = -mm(h[m, rows, 0:128], h[m, 0:128, 0:128])

        return go

    spread(invert(block, 16), 14, [after0(m, k) for k in range(4) for m in range(COLS)])


def fit_own(gnorm, mid):
    return pl.pallas_call(
        own_kernel,
        out_shape=[pltpu.VMEM((COLS, OWN + R, K), BF)] * 3
        + [pltpu.VMEM((COLS, OWN, LANES), F32), pltpu.VMEM((COLS, 128, 128), F32)],
        scratch_shapes=[pltpu.VMEM((COLS, 2 * R, K), F32)],
        compiler_params=pltpu.CompilerParams(vmem_limit_bytes=ROOM),
        name="fit_own",
    )(*on_chip(gnorm, mid))


def near_kernel(
    adjacency, gnorm, mid, up, down, fh, fm, fl, h_in, block_in, out, own,
    links, patch, h, block, nb, cross, turned, x, order, sem,
):
    fetch = pltpu.make_async_copy(adjacency, links, sem)
    fetch.start()
    row0 = lax.axis_index("gx_0") * 4 + lax.axis_index("gx_1")
    col0 = (lax.axis_index("gy_0") * 2 + lax.axis_index("gy_1")) * COLS
    keep = past_mask()
    lin, _ = ridge(gnorm[0:1])
    sub, lane = iotas((8, 128))
    for m in range(COLS):
        w = mm(block_in[m], h_in[m, 128:256, 256:LANES])
        block[m, 0:NEAR] = h_in[m, 256:OWN, 256:LANES] - mm(h_in[m, 256:OWN, 128:256], w)
        h[m, 128:256, 256:LANES] = w
        h[m, 128:256, 128:256] = block_in[m]
        h[m, 128:256, 0:128] = h_in[m, 128:256, 0:128]
        h[m, 0:128] = h_in[m, 0:128]
        h[m, 256:OWN] = h_in[m, 256:OWN]
    for c in range(4):
        for r, source in enumerate((up, mid, down)):
            patch[4 * r + c] = jnp.where(keep, source[c], 0.0)
    own[0] = mid[1]
    own[1] = mid[2]
    gap = jnp.zeros((128 - NEAR, K), F32)
    fetch.wait()
    for m in range(COLS):
        rows = []
        for b in range(NB):
            link = links[0, m, b]
            rows.append(patch[((link >> 4) - row0 + 1) * 4 + ((link & 15) - col0 + 1)])
        nb[m, 0:128], nb[m, 128:256], nb[m, 256:384] = split3(jnp.concatenate(rows + [gap], axis=0))

    def after1(m, kind):
        def go():
            if kind == 0:
                h[m, 128:256, 0:128] = mm(h[m, 128:256, 128:256], h[m, 128:256, 0:128])
            elif kind == 1:
                h[m, 0:128, 256:LANES] -= mm(h[m, 0:128, 128:256], h[m, 128:256, 256:LANES])
            elif kind == 2:
                for rows in (slice(0, 128), slice(256, OWN)):
                    h[m, rows, 0:128] -= mm(h[m, rows, 128:256], h[m, 128:256, 0:128])
            else:
                for rows in (slice(0, 128), slice(256, OWN)):
                    h[m, rows, 128:256] = -mm(h[m, rows, 128:256], h[m, 128:256, 128:256])

        return go

    def near_products(m, part):
        def go():
            nh, nm, nl = (nb[m, 128 * i : 128 * i + 128] for i in range(3))
            if part == 0:
                a = [f[m, 0:176] for f in (fh, fm, fl)]
            else:
                pieces = ((fh, nh), (fm, nm), (fl, nl))
                a = [jnp.concatenate([f[m, 176 : OWN + R], n[0:80]], axis=0) for f, n in pieces]
            size = a[0].shape[0]
            p = nt(jnp.concatenate(a[:2], axis=0), nb[m, 0:256])
            r = nt(a[0], nl) + nt(a[2], nh)
            top, low = slice(0, size), slice(size, 2 * size)
            g = p[top, 0:128] + ((p[top, 128:256] + p[low, 0:128]) + (p[low, 128:256] + r))
            cross[m, 176 * part : 176 * part + size] = g

        return go

    def turn(m):
        def go():
            turned[m] = to_rows(cross[m, 0 : OWN + R], LANES).T[0:NEAR]

        return go

    def near_columns(m):
        def go():
            g = mm_thirds(split3(h[m, :, 0:256]), cross[m, 0:256])
            x[m, 0:256] = g[0:256]
            x[m, 256:OWN] = cross[m, 256:OWN] + g[256:OWN]

        return go

    work = []
    for k in range(4):
        for m in range(COLS):
            work.append(after1(m, k))
            if k < 2:
                work.append(near_products(m, k))
            else:
                work.append(turn(m) if k == 2 else near_columns(m))
    spread(invert(block, 9), 8, work)
    _, wide = iotas((256, 128))
    _, lane_n = iotas((NEAR, 128))
    for m in range(COLS):
        last = block[m, 0:NEAR]
        low = jnp.where(lane_n < NEAR, mm(first_lanes(last), to_rows(x[m, 256:OWN], 128)), last)
        part = h[m, 0:256, 256:LANES]
        top = jnp.where(wide < NEAR, x[m, 0:256], part) - mm(first_lanes(part), to_rows(low, 128))
        both = jnp.concatenate([top, low], axis=0)
        x[m] = both
        start = jnp.where(lane_n < NEAR, cross[m, OWN + R : OWN + R + NEAR], turned[m, :, 256:LANES])
        start = jnp.where(lane_n < NEAR + R, start, 0.0)
        start = jnp.concatenate(
            [start[8 * i : 8 * i + 8] + jnp.where(lane == sub + 8 * i, lin, 0.0) for i in range(NEAR // 8)], axis=0
        )
        flat = jnp.where(iotas((NEAR, LANES))[1] < OWN, turned[m], 0.0)
        block[m, 0:NEAR] = start - mm_thirds(split3(flat), to_rows(both, LANES))
    for _ in invert(block, 9):
        pass
    for m in range(COLS):
        last = block[m, 0:NEAR]
        both = x[m, 0:OWN]
        x[m, 0:OWN] = both - mm(first_lanes(both), to_rows(last, 128))
        order[m, 0:1] = x[m, MIXED + 12 : MIXED + 13]
        order[m, 1:25] = x[m, NQ : NQ + R]
        order[m, 25:97] = last
        dst = 97
        for a in range(R):
            for b in range(a, R):
                d = b - a
                if d == 12:
                    src = MIXED + a
                elif d < 12:
                    src = R * d + a
                else:
                    src = R * (R - d) + b
                order[m, dst : dst + 1] = x[m, src : src + 1]
                dst += 1
        flat = order[m].T
        out[m] = flat[NEAR : NEAR + R, 0:NF]


def fit_near(adjacency, *rest):
    vm = pl.BlockSpec(memory_space=pltpu.VMEM)
    return pl.pallas_call(
        near_kernel,
        in_specs=[pl.BlockSpec(memory_space=pl.ANY)] + [vm] * len(rest),
        out_specs=[vm, vm],
        out_shape=[
            jax.ShapeDtypeStruct((COLS, R, NF), F32),
            jax.ShapeDtypeStruct((COLS, R, K), F32),
        ],
        scratch_shapes=[
            pltpu.SMEM((1, COLS, NB), jnp.int32),
            pltpu.VMEM((12, R, K), F32),
            pltpu.VMEM((COLS, OWN, LANES), F32),
            pltpu.VMEM((COLS, 128, 128), F32),
            pltpu.VMEM((COLS, 384, K), BF),
            pltpu.VMEM((COLS, OWN + R + 80, 128), F32),
            pltpu.VMEM((COLS, NEAR, LANES), F32),
            pltpu.VMEM((COLS, OWN, 128), F32),
            pltpu.VMEM((COLS, 512, 128), F32),
            pltpu.SemaphoreType.DMA,
        ],
        compiler_params=pltpu.CompilerParams(vmem_limit_bytes=ROOM),
        name="fit_near",
    )(pltpu.with_memory_space_constraint(adjacency, pltpu.HBM), *on_chip(*rest))


def shifts(axis, x, y):
    n = lax.axis_size(axis)
    return (
        lax.ppermute(x, axis, [(i, i + 1) for i in range(n - 1)]),
        lax.ppermute(y, axis, [(i + 1, i) for i in range(n - 1)]),
    )


def body(snapshots, basis, node_counts, adjacency):
    proj0, proj1, stats = local_pass(snapshots[0], basis[0], node_counts)
    everyone = lax.all_to_all(stats, GX_GY, 0, 0, tiled=True)
    left, right = shifts(GY, proj1, proj0)
    mid, gnorm = global_states(everyone, left, proj0, proj1, right)
    up, down = shifts(GX, mid, mid)
    parts = fit_own(gnorm, mid)
    operator, own = fit_near(adjacency, gnorm, mid, up, down, *parts)
    return (jnp.swapaxes(operator, 1, 2)[None], own[None])


def solution(mesh):
    split = Mesh(mesh.devices.reshape(4, 4, 4, 2), ("gx_0", "gx_1", "gy_0", "gy_1"))
    placed = (P(GX, GY, None, None, None), P(GX, GY, None, None, None), P(GX, GY), P(GX, GY, None))
    return jax.shard_map(
        body,
        mesh=split,
        in_specs=placed,
        out_specs=(P(GX, GY, None, None), P(GX, GY, None, None)),
        check_vma=False,
    )
```

```python
import jax
import jax.numpy as jnp
from jax import lax
from jax.experimental import pallas as pl
from jax.experimental.pallas import tpu as pltpu
from jax.sharding import Mesh
from jax.sharding import PartitionSpec as P

GX = ("gx_0", "gx_1")
GY = ("gy_0", "gy_1")
GX_GY = ("gx_0", "gx_1", "gy_0", "gy_1")

R = 24
NVAR = 4
K = 512
SLOTS = 2048
COLS = 2
NB = 3
NF = 397
HALF = 0.5
F32 = jnp.float32
BF = jnp.bfloat16


def iotas(shape):
    return lax.broadcasted_iota(jnp.int32, shape, 0), lax.broadcasted_iota(jnp.int32, shape, 1)


DEPTH = 3
CUTS = 1
BLOCK = 256


def fold_lanes(x):
    return (x[:, 0:128] + x[:, 128:256]) + (x[:, 256:384] + x[:, 384:512])


def local_kernel(counts, basis, snaps, proj0, proj1, stats, modes, data, proj, acc, basis_sem, sems):
    steps = COLS * NVAR
    rows = SLOTS // CUTS

    def copy(i, c):
        part = pl.ds(c * rows, rows)
        return pltpu.make_async_copy(snaps.at[i // NVAR, i % NVAR, part], data.at[i, part], sems.at[i, c])

    def modes_copy(i):
        return pltpu.make_async_copy(basis.at[i // NVAR, i % NVAR], modes.at[i], basis_sem.at[i])

    for i in range(DEPTH):
        modes_copy(i).start()
        for c in range(CUTS):
            copy(i, c).start()
    acc[...] = jnp.zeros_like(acc)

    def step(i, carry):
        count = counts[0, i // NVAR]
        v = i % NVAR

        @pl.when(i + DEPTH < steps)
        def _():
            modes_copy(i + DEPTH).start()
            for c in range(CUTS):
                copy(i + DEPTH, c).start()

        modes_copy(i).wait()
        for c in range(CUTS):
            copy(i, c).wait()
        lane = lax.broadcasted_iota(jnp.int32, (R, BLOCK), 1)
        row = lax.broadcasted_iota(jnp.int32, (BLOCK, 128), 0)
        parts = []
        prods = []
        for lo in range(0, SLOTS, BLOCK):
            kept = jnp.where(lane < count - lo, modes[i, :, lo : lo + BLOCK], jnp.zeros((), BF))
            prods.append(jnp.dot(kept, data[i, lo : lo + BLOCK], preferred_element_type=F32))
            x = data[i, lo : lo + BLOCK, :].astype(F32)
            t = jnp.where(row < count - lo, fold_lanes(x * x), 0.0)
            parts.append(jnp.sum(t.reshape(BLOCK // 8, 8, 128), axis=0))
        proj[i] = sum(prods)
        part = sum(parts)
        acc[v] += part
        return carry

    lax.fori_loop(0, steps, step, 0)
    q = NVAR
    for a in range(NVAR):
        for b in range(a, NVAR):
            t = fold_lanes(proj[a] * proj[b]) + fold_lanes(proj[NVAR + a] * proj[NVAR + b])
            acc[q] = t[0:8] + t[8:16] + t[16:24]
            q += 1
    for v in range(NVAR):
        proj0[v] = proj[v]
        proj1[v] = proj[NVAR + v]
    total = jnp.sum(jnp.sum(acc[...], axis=1), axis=1, keepdims=True)
    i, j = iotas((16, 128))
    flat = jnp.sum(jnp.where(i == j, total, 0.0), axis=0, keepdims=True)
    nodes = (counts[0, 0] + counts[0, 1]).astype(F32)
    _, lane1 = iotas((1, 128))
    stats[...] = jnp.broadcast_to(jnp.where(lane1 == 14, nodes, flat), (128, 128))


ROOM = 36 << 20


def on_chip(*xs):
    return [pltpu.with_memory_space_constraint(x, pltpu.VMEM) for x in xs]


def local_pass(snapshots, basis, counts):
    vm = pl.BlockSpec(memory_space=pltpu.VMEM)
    hbm = pl.BlockSpec(memory_space=pl.ANY)
    return pl.pallas_call(
        local_kernel,
        in_specs=[pl.BlockSpec(memory_space=pltpu.SMEM), hbm, hbm],
        out_specs=[vm, vm, vm],
        out_shape=[
            pltpu.VMEM((NVAR, R, K), F32),
            pltpu.VMEM((NVAR, R, K), F32),
            pltpu.VMEM((128, 128), F32),
        ],
        scratch_shapes=[
            pltpu.VMEM((COLS * NVAR, R, SLOTS), BF),
            pltpu.VMEM((COLS * NVAR, SLOTS, K), BF),
            pltpu.VMEM((COLS * NVAR, R, K), F32),
            pltpu.VMEM((16, 8, 128), F32),
            pltpu.SemaphoreType.DMA((COLS * NVAR,)),
            pltpu.SemaphoreType.DMA((COLS * NVAR, CUTS)),
        ],
        compiler_params=pltpu.CompilerParams(vmem_limit_bytes=ROOM),
        name="local",
    )(*[pltpu.with_memory_space_constraint(x, pltpu.HBM) for x in (counts, basis, snapshots)])


OWN = 328
NQ = 288
MIXED = 312
FUT = OWN
NEAR = 72
LANES = 384


def lane_copy(x, at):
    return jnp.take_along_axis(x, jnp.full((8, 128), at, jnp.int32), axis=1)


def sub_copy(x, j):
    return jnp.broadcast_to(x[j : j + 1, :], (8, 128))


def split3(x):
    h = x.astype(BF)
    r = x - h.astype(F32)
    m = r.astype(BF)
    return h, m, (r - m.astype(F32)).astype(BF)


def dot(a, b):
    return jnp.dot(a, b, preferred_element_type=F32)


def mm(a, b):
    ah, am, al = split3(a)
    bh, bm, bl = split3(b)
    n = b.shape[1]
    w = jnp.concatenate([bh, bm], axis=1)
    p = dot(jnp.concatenate([ah, am], axis=1), jnp.concatenate([w, w], axis=0))
    q = dot(jnp.concatenate([ah, al], axis=1), jnp.concatenate([bl, bh], axis=0))
    return p[:, :n] + (p[:, n:] + q)


def mm_thirds(a, b):
    bh, bm, bl = split3(b)
    n = b.shape[1]
    w = jnp.concatenate([bh, bm], axis=1)
    p = dot(a[0], w)
    q = dot(a[1], w)
    r = dot(a[0], bl) + dot(a[2], bh)
    return p[:, :n] + ((p[:, n:] + q[:, :n]) + (q[:, n:] + r))


def first_lanes(x):
    return jnp.where(iotas(x.shape)[1] < NEAR, x, 0.0)


def to_rows(x, rows):
    return jnp.concatenate([x, jnp.zeros((rows - x.shape[0], x.shape[1]), F32)], axis=0)


def tree(terms):
    while len(terms) > 1:
        terms = [terms[i] + terms[i + 1] for i in range(0, len(terms) - 1, 2)] + terms[len(terms) // 2 * 2 :]
    return terms[0]


def padded_dot(a, w, lo):
    ah, am, al = split3(a)
    n = w.shape[0]
    parts = [jnp.zeros((lo, 128), F32)] * (lo > 0) + [w] + [jnp.zeros((128 - lo - n, 128), F32)] * (lo + n < 128)
    wh, wm, wl = split3(jnp.concatenate(parts, axis=0) if len(parts) > 1 else w)
    pair = jnp.concatenate([wh, wm], axis=1)
    u = dot(jnp.concatenate([ah, am], axis=1), jnp.concatenate([pair, pair], axis=0))
    v = dot(jnp.concatenate([ah, al], axis=1), jnp.concatenate([wl, wh], axis=0))
    return u[:, :128] + (u[:, 128:] + v)


def pivots(col, riders, sub):
    recips = jnp.zeros((8, 128), F32)
    diag = sub_copy(col[0], 0)
    for j in range(8):
        r = 1.0 / diag
        bare = jnp.where(sub == j, 0.0, col[j])
        recips = jnp.where(sub == j, r, recips)
        heads = {k: sub_copy(col[k], j) for k in range(j + 1, 8)}
        if j < 7:
            diag = sub_copy(col[j + 1], j + 1) - (sub_copy(col[j], j + 1) * heads[j + 1]) * r
        mult = bare * r
        for k in range(j + 1, 8):
            col[k] = col[k] - mult * heads[k]
        riders = [x - mult * sub_copy(x, j) for x in riders]
    return [x * recips for x in riders]


def invert(block, tiles, strip=2, look=1):
    sub, lane = iotas((8, 128))
    for s in range(0, tiles, strip):
        own = list(range(s, min(s + strip, tiles)))
        ahead = list(range(s + strip, min(s + strip + look, tiles)))
        for p in own:
            base = 8 * p
            inside = (lane >= base) & (lane < base + 8)
            unit = jnp.where(lane - base == sub, 1.0, 0.0)
            ws = []
            for m in range(COLS):
                tile = block[m, base : base + 8, :]
                col = [lane_copy(tile, base + k) for k in range(8)]
                w = pivots(col, [jnp.where(inside, unit, tile)], sub)[0]
                block[m, base : base + 8, :] = w
                ws.append([sub_copy(w, j) for j in range(8)])
            for t in [t for t in own + ahead if t > p] + [t for t in own if t < p]:
                for m in range(COLS):
                    a = block[m, 8 * t : 8 * t + 8, :]
                    delta = tree([lane_copy(a, base + j) * ws[m][j] for j in range(8)])
                    block[m, 8 * t : 8 * t + 8, :] = jnp.where(inside, 0.0, a) - delta
            yield
        lo, hi = 8 * s, 8 * (own[-1] + 1)
        ranges = [(a, b) for a, b in ((hi + 8 * len(ahead), 8 * tiles), (0, lo)) if a < b]
        if ranges:
            for m in range(COLS):
                rest = [block[m, a:b, :] for a, b in ranges]
                rest = jnp.concatenate(rest, axis=0) if len(rest) > 1 else rest[0]
                _, wide_l = iotas(rest.shape)
                kept = jnp.where((wide_l >= lo) & (wide_l < hi), 0.0, rest)
                new = kept - padded_dot(rest, block[m, lo:hi, :], lo)
                at = 0
                for a, b in ranges:
                    block[m, a:b, :] = new[at : at + b - a]
                    at += b - a


def spread(panels, count, work):
    work = list(work)
    done = 0
    for i, _ in enumerate(panels):
        want = (i + 1) * len(work) // count if i + 1 < count else len(work)
        while done < min(want, len(work)):
            work[done]()
            done += 1
    for f in work[done:]:
        f()


def states_kernel(everyone, left, proj0, proj1, right, mid, gnorm):
    found = global_scales(everyone)
    gnorm[...] = jnp.broadcast_to(found[NVAR], (8, 128))
    inv = [x[:, 0:1] for x in found]
    for c, proj in enumerate((left, proj0, proj1, right)):
        mid[c] = scaled_sum(proj, inv)


def global_states(everyone, left, proj0, proj1, right):
    return pl.pallas_call(
        states_kernel,
        out_shape=[pltpu.VMEM((4, R, K), F32), pltpu.VMEM((8, 128), F32)],
        compiler_params=pltpu.CompilerParams(vmem_limit_bytes=ROOM),
        name="states",
    )(*on_chip(everyone, left, proj0, proj1, right))


def own_features(feats, twice, m, state, keep):
    past = jnp.where(keep, state, 0.0)
    twice[m, 0:R] = past
    twice[m, R : 2 * R] = past
    for d in range(12):
        feats(R * d, past * twice[m, d : d + R])
    feats(NQ, past)
    row, lane = iotas((16, K))
    one = jnp.where((row == 12) & (lane < K - 1), 1.0, 0.0)
    feats(MIXED, jnp.where(row < 12, twice[m, 0:16] * twice[m, 12:28], one))
    feats(FUT, pltpu.roll(state, K - 1, 1))


def global_scales(everyone):
    total = jnp.sum(everyone[...], axis=0, keepdims=True)
    nodes = total[:, 14:15]
    inv = []
    for v in range(NVAR):
        inv.append(1.0 / jnp.sqrt(total[:, v : v + 1] / (nodes * K) + 1e-06))
    g = jnp.zeros((1, 1), F32)
    q = NVAR
    for a in range(NVAR):
        for b in range(a, NVAR):
            term = total[:, q : q + 1] * inv[a] * inv[b]
            g = g + (term if a == b else 2.0 * term)
            q += 1
    return [jnp.broadcast_to(x, (1, 128)) for x in inv + [g * (1.0 / (256 * R * K))]]


def scaled_sum(proj, inv):
    t = proj[0] * inv[0]
    for v in range(1, NVAR):
        t = t + proj[v] * inv[v]
    return t


def ridge(g):
    return K * (HALF * g), K * (HALF * g * g)


def past_mask():
    return lax.broadcasted_iota(jnp.int32, (R, K), 1) < K - 1


def nt(a, b):
    return lax.dot_general(a, b, (((1,), (1,)), ((), ())), preferred_element_type=F32)


def own_kernel(gnorm, mid, fh, fm, fl, h, block, twice):
    keep = past_mask()
    for m in range(COLS):

        def put(at, x, m=m):
            n = x.shape[0]
            fh[m, at : at + n], fm[m, at : at + n], fl[m, at : at + n] = split3(x)

        own_features(put, twice, m, mid[1 + m], keep)
    lin, quad = ridge(gnorm[0:1])
    sub, lane = iotas((8, 128))

    def thirds(m, lo, hi):
        return [f[m, lo:hi] for f in (fh, fm, fl)]

    def gram(m, r0, r1, c0, c1):
        want = r1 - r0
        size = -(-want // 16) * 16
        a, b = thirds(m, r0, r0 + size), thirds(m, c0, c1)
        n = c1 - c0
        top, mid, low = slice(0, size), slice(size, 2 * size), slice(2 * size, 3 * size)
        if n > 128:
            x = nt(jnp.concatenate(a, axis=0), b[0])
            y = nt(jnp.concatenate(a[:2], axis=0), b[1])
            g = (((y[mid] + nt(a[0], b[2])) + x[low]) + (y[top] + x[mid])) + x[top]
            return g[0:want]
        gap = [jnp.zeros((128 - n, K), BF)] * (n < 128)
        pair = jnp.concatenate([b[0]] + gap + [b[1]] + gap, axis=0)
        p = nt(jnp.concatenate(a[:2], axis=0), pair)
        r = nt(a[0], b[2]) + nt(a[2], b[0])
        one, two = slice(0, n), slice(128, 128 + n)
        g = p[top, one] + ((p[top, two] + p[mid, one]) + (p[mid, two] + r))
        return g[0:want]

    def reg(row):
        if row < NQ or row == MIXED:
            return quad
        if row == MIXED + 8:
            return jnp.where(sub < 4, quad, jnp.where(sub == 4, lin, 1.0))
        return lin

    def ridged(x, row0):
        tiles = []
        for i in range(x.shape[0] // 8):
            tiles.append(x[8 * i : 8 * i + 8] + jnp.where(lane == sub + 8 * i, reg(row0 + 8 * i), 0.0))
        return jnp.concatenate(tiles, axis=0)

    for m in range(COLS):
        block[m] = ridged(gram(m, 0, 128, 0, 128), 0)

    def piece(m, kind):
        def go():
            if kind == 0:
                h[m, 0:128, 256:LANES] = jnp.zeros((128, 128), F32)
                h[m, 0:128, 128 : OWN + R] = gram(m, 0, 128, 128, OWN + R)
            elif kind == 1:
                g = gram(m, 128, OWN, 0, 256)
                h[m, 128:256, 0:128] = g[0:128, 0:128]
                h[m, 128:256, 128:256] = ridged(g[0:128, 128:256], 128)
                h[m, 256:OWN, 0:256] = g[128:]
            else:
                h[m, 128:OWN, 256:LANES] = jnp.zeros((OWN - 128, 128), F32)
                h[m, 128:OWN, 256 : OWN + R] = gram(m, 128, OWN, 256, OWN + R)
                h[m, 256:OWN, 256:LANES] = ridged(h[m, 256:OWN, 256:LANES], 256)

        return go

    spread(invert(block, 16), 14, [piece(m, k) for k in range(2) for m in range(COLS)])
    inv0 = [block[m] for m in range(COLS)]
    for m in range(COLS):
        w = mm(inv0[m], h[m, 0:128, 128:256])
        block[m] = h[m, 128:256, 128:256] - mm(h[m, 128:256, 0:128], w)
        h[m, 0:128, 128:256] = w
        h[m, 0:128, 0:128] = inv0[m]

    def after0(m, kind):
        def go():
            if kind == 0:
                h[m, 0:128, 256:LANES] = mm(h[m, 0:128, 0:128], h[m, 0:128, 256:LANES])
            elif kind == 1:
                rows = slice(128, OWN)
                h[m, rows, 256:LANES] -= mm(h[m, rows, 0:128], h[m, 0:128, 256:LANES])
            elif kind == 2:
                rows = slice(256, OWN)
                h[m, rows, 128:256] -= mm(h[m, rows, 0:128], h[m, 0:128, 128:256])
            else:
                rows = slice(128, OWN)
                h[m, rows, 0:128] = -mm(h[m, rows, 0:128], h[m, 0:128, 0:128])

        return go

    late = [piece(m, 2) for m in range(COLS)]
    spread(invert(block, 16), 14, late + [after0(m, k) for k in range(4) for m in range(COLS)])


def fit_own(gnorm, mid):
    return pl.pallas_call(
        own_kernel,
        out_shape=[pltpu.VMEM((COLS, OWN + R, K), BF)] * 3
        + [pltpu.VMEM((COLS, OWN, LANES), F32), pltpu.VMEM((COLS, 128, 128), F32)],
        scratch_shapes=[pltpu.VMEM((COLS, 2 * R, K), F32)],
        compiler_params=pltpu.CompilerParams(vmem_limit_bytes=ROOM),
        name="fit_own",
    )(*on_chip(gnorm, mid))


def near_kernel(
    adjacency, gnorm, mid, up, down, fh, fm, fl, h_in, block_in, out, own,
    links, patch, h, block, nb, cross, turned, x, order, flat_out, sem, own_sem, out_sems,
):
    fetch = pltpu.make_async_copy(adjacency, links, sem)
    fetch.start()
    save = pltpu.make_async_copy(mid.at[pl.ds(1, COLS)], own, own_sem)
    save.start()
    row0 = lax.axis_index("gx_0") * 4 + lax.axis_index("gx_1")
    col0 = (lax.axis_index("gy_0") * 2 + lax.axis_index("gy_1")) * COLS
    keep = past_mask()
    lin, _ = ridge(gnorm[0:1])
    sub, lane = iotas((8, 128))
    for m in range(COLS):
        w = mm(block_in[m], h_in[m, 128:256, 256:LANES])
        block[m, 0:NEAR] = h_in[m, 256:OWN, 256:LANES] - mm(h_in[m, 256:OWN, 128:256], w)
        h[m, 128:256, 256:LANES] = w
        h[m, 128:256, 128:256] = block_in[m]
        h[m, 128:256, 0:128] = h_in[m, 128:256, 0:128]
        h[m, 0:128] = h_in[m, 0:128]
        h[m, 256:OWN] = h_in[m, 256:OWN]
    for c in range(4):
        for r, source in enumerate((up, mid, down)):
            patch[4 * r + c] = jnp.where(keep, source[c], 0.0)
    gap = jnp.zeros((128 - NEAR, K), F32)
    fetch.wait()
    for m in range(COLS):
        rows = []
        for b in range(NB):
            link = links[0, m, b]
            rows.append(patch[((link >> 4) - row0 + 1) * 4 + ((link & 15) - col0 + 1)])
        nb[m, 0:128], nb[m, 128:256], nb[m, 256:384] = split3(jnp.concatenate(rows + [gap], axis=0))

    def after1(m, kind):
        def go():
            if kind == 0:
                h[m, 128:256, 0:128] = mm(h[m, 128:256, 128:256], h[m, 128:256, 0:128])
            elif kind == 1:
                h[m, 0:128, 256:LANES] -= mm(h[m, 0:128, 128:256], h[m, 128:256, 256:LANES])
            elif kind == 2:
                for rows in (slice(0, 128), slice(256, OWN)):
                    h[m, rows, 0:128] -= mm(h[m, rows, 128:256], h[m, 128:256, 0:128])
            else:
                for rows in (slice(0, 128), slice(256, OWN)):
                    h[m, rows, 128:256] = -mm(h[m, rows, 128:256], h[m, 128:256, 128:256])

        return go

    def near_products(m, part):
        def go():
            nh, nm, nl = (nb[m, 128 * i : 128 * i + 128] for i in range(3))
            if part == 0:
                a = [f[m, 0:176] for f in (fh, fm, fl)]
            else:
                pieces = ((fh, nh), (fm, nm), (fl, nl))
                a = [jnp.concatenate([f[m, 176 : OWN + R], n[0:80]], axis=0) for f, n in pieces]
            size = a[0].shape[0]
            p = nt(jnp.concatenate(a[:2], axis=0), nb[m, 0:256])
            r = nt(a[0], nl) + nt(a[2], nh)
            top, low = slice(0, size), slice(size, 2 * size)
            g = p[top, 0:128] + ((p[top, 128:256] + p[low, 0:128]) + (p[low, 128:256] + r))
            cross[m, 176 * part : 176 * part + size] = g

        return go

    def turn(m):
        def go():
            turned[m] = to_rows(cross[m, 0 : OWN + R], LANES).T[0:NEAR]

        return go

    def near_columns(m):
        def go():
            g = mm_thirds(split3(h[m, :, 0:256]), cross[m, 0:256])
            x[m, 0:256] = g[0:256]
            x[m, 256:OWN] = cross[m, 256:OWN] + g[256:OWN]

        return go

    work = []
    for k in range(4):
        for m in range(COLS):
            work.append(after1(m, k))
            if k < 2:
                work.append(near_products(m, k))
            else:
                work.append(turn(m) if k == 2 else near_columns(m))
    spread(invert(block, 9), 8, work)
    _, wide = iotas((256, 128))
    _, lane_n = iotas((NEAR, 128))
    for m in range(COLS):
        last = block[m, 0:NEAR]
        low = jnp.where(lane_n < NEAR, mm(first_lanes(last), to_rows(x[m, 256:OWN], 128)), last)
        part = h[m, 0:256, 256:LANES]
        top = jnp.where(wide < NEAR, x[m, 0:256], part) - mm(first_lanes(part), to_rows(low, 128))
        both = jnp.concatenate([top, low], axis=0)
        x[m] = both
        start = jnp.where(lane_n < NEAR, cross[m, OWN + R : OWN + R + NEAR], turned[m, :, 256:LANES])
        start = jnp.where(lane_n < NEAR + R, start, 0.0)
        start = jnp.concatenate(
            [start[8 * i : 8 * i + 8] + jnp.where(lane == sub + 8 * i, lin, 0.0) for i in range(NEAR // 8)], axis=0
        )
        flat = jnp.where(iotas((NEAR, LANES))[1] < OWN, turned[m], 0.0)
        block[m, 0:NEAR] = start - mm_thirds(split3(flat), to_rows(both, LANES))
    for _ in invert(block, 9):
        pass
    for m in range(COLS):
        last = block[m, 0:NEAR]
        both = x[m, 0:OWN]
        x[m, 0:OWN] = both - mm(first_lanes(both), to_rows(last, 128))
        order[m, 0:1] = x[m, MIXED + 12 : MIXED + 13]
        order[m, 1:25] = x[m, NQ : NQ + R]
        order[m, 25:97] = last
        dst = 97
        for a in range(R):
            near_count = min(12, R - a)
            order[m, dst : dst + near_count] = x[m, pl.ds(a, near_count, stride=R), :]
            dst += near_count
            for b in range(a + 12, R):
                src = MIXED + a if b - a == 12 else R * (R - b + a) + b
                order[m, dst : dst + 1] = x[m, src : src + 1]
                dst += 1
        flat_out[m] = order[m].T[NEAR : NEAR + R, 0:NF]
        pltpu.make_async_copy(flat_out.at[m], out.at[m], out_sems.at[m]).start()
    for m in range(COLS):
        pltpu.make_async_copy(flat_out.at[m], out.at[m], out_sems.at[m]).wait()
    save.wait()


def fit_near(adjacency, *rest):
    vm = pl.BlockSpec(memory_space=pltpu.VMEM)
    return pl.pallas_call(
        near_kernel,
        in_specs=[pl.BlockSpec(memory_space=pl.ANY)] + [vm] * len(rest),
        out_specs=[pl.BlockSpec(memory_space=pl.ANY)] * 2,
        out_shape=[
            jax.ShapeDtypeStruct((COLS, R, NF), F32),
            jax.ShapeDtypeStruct((COLS, R, K), F32),
        ],
        scratch_shapes=[
            pltpu.SMEM((1, COLS, NB), jnp.int32),
            pltpu.VMEM((12, R, K), F32),
            pltpu.VMEM((COLS, OWN, LANES), F32),
            pltpu.VMEM((COLS, 128, 128), F32),
            pltpu.VMEM((COLS, 384, K), BF),
            pltpu.VMEM((COLS, OWN + R + 80, 128), F32),
            pltpu.VMEM((COLS, NEAR, LANES), F32),
            pltpu.VMEM((COLS, OWN, 128), F32),
            pltpu.VMEM((COLS, 512, 128), F32),
            pltpu.VMEM((COLS, R, NF), F32),
            pltpu.SemaphoreType.DMA,
            pltpu.SemaphoreType.DMA,
            pltpu.SemaphoreType.DMA((COLS,)),
        ],
        compiler_params=pltpu.CompilerParams(vmem_limit_bytes=ROOM),
        name="fit_near",
    )(pltpu.with_memory_space_constraint(adjacency, pltpu.HBM), *on_chip(*rest))


def shifts(axis, x, y):
    n = lax.axis_size(axis)
    return (
        lax.ppermute(x, axis, [(i, i + 1) for i in range(n - 1)]),
        lax.ppermute(y, axis, [(i + 1, i) for i in range(n - 1)]),
    )


def body(snapshots, basis, node_counts, adjacency):
    proj0, proj1, stats = local_pass(snapshots[0], basis[0], node_counts)
    everyone = lax.all_to_all(stats, GX_GY, 0, 0, tiled=True)
    left, right = shifts(GY, proj1, proj0)
    mid, gnorm = global_states(everyone, left, proj0, proj1, right)
    up, down = shifts(GX, mid, mid)
    parts = fit_own(gnorm, mid)
    operator, own = fit_near(adjacency, gnorm, mid, up, down, *parts)
    return (jnp.swapaxes(operator, 1, 2)[None], own[None])


def solution(mesh):
    split = Mesh(mesh.devices.reshape(4, 4, 4, 2), ("gx_0", "gx_1", "gy_0", "gy_1"))
    placed = (P(GX, GY, None, None, None), P(GX, GY, None, None, None), P(GX, GY), P(GX, GY, None))
    return jax.shard_map(
        body,
        mesh=split,
        in_specs=placed,
        out_specs=(P(GX, GY, None, None), P(GX, GY, None, None)),
        check_vma=False,
    )
```

```python
import jax
import jax.numpy as jnp
from jax import lax
from jax.experimental import pallas as pl
from jax.experimental.pallas import tpu as pltpu
from jax.sharding import Mesh
from jax.sharding import PartitionSpec as P

GX = ("gx_0", "gx_1")
GY = ("gy_0", "gy_1")
GX_GY = ("gx_0", "gx_1", "gy_0", "gy_1")

R = 24
NVAR = 4
K = 512
SLOTS = 2048
COLS = 2
NB = 3
NF = 397
HALF = 0.5
F32 = jnp.float32
BF = jnp.bfloat16


def iotas(shape):
    return lax.broadcasted_iota(jnp.int32, shape, 0), lax.broadcasted_iota(jnp.int32, shape, 1)


DEPTH = 3
CUTS = 1
BLOCK = 256


def fold_lanes(x):
    return (x[:, 0:128] + x[:, 128:256]) + (x[:, 256:384] + x[:, 384:512])


def local_kernel(counts, basis, snaps, proj0, proj1, stats, modes, data, proj, acc, basis_sem, sems):
    steps = COLS * NVAR
    rows = SLOTS // CUTS

    def copy(i, c):
        part = pl.ds(c * rows, rows)
        return pltpu.make_async_copy(snaps.at[i // NVAR, i % NVAR, part], data.at[i, part], sems.at[i, c])

    def modes_copy(i):
        return pltpu.make_async_copy(basis.at[i // NVAR, i % NVAR], modes.at[i], basis_sem.at[i])

    for i in range(DEPTH):
        modes_copy(i).start()
        for c in range(CUTS):
            copy(i, c).start()
    acc[...] = jnp.zeros_like(acc)

    def step(i, carry):
        count = counts[0, i // NVAR]
        v = i % NVAR

        @pl.when(i + DEPTH < steps)
        def _():
            modes_copy(i + DEPTH).start()
            for c in range(CUTS):
                copy(i + DEPTH, c).start()

        modes_copy(i).wait()
        for c in range(CUTS):
            copy(i, c).wait()
        lane = lax.broadcasted_iota(jnp.int32, (R, BLOCK), 1)
        row = lax.broadcasted_iota(jnp.int32, (BLOCK, 128), 0)
        parts = []
        prods = []
        for lo in range(0, SLOTS, BLOCK):
            kept = jnp.where(lane < count - lo, modes[i, :, lo : lo + BLOCK], jnp.zeros((), BF))
            prods.append(jnp.dot(kept, data[i, lo : lo + BLOCK], preferred_element_type=F32))
            x = data[i, lo : lo + BLOCK, :].astype(F32)
            t = jnp.where(row < count - lo, fold_lanes(x * x), 0.0)
            parts.append(jnp.sum(t.reshape(BLOCK // 8, 8, 128), axis=0))
        proj[i] = sum(prods)
        part = sum(parts)
        acc[v] += part
        return carry

    lax.fori_loop(0, steps, step, 0)
    q = NVAR
    for a in range(NVAR):
        for b in range(a, NVAR):
            t = fold_lanes(proj[a] * proj[b]) + fold_lanes(proj[NVAR + a] * proj[NVAR + b])
            acc[q] = t[0:8] + t[8:16] + t[16:24]
            q += 1
    for v in range(NVAR):
        proj0[v] = proj[v]
        proj1[v] = proj[NVAR + v]
    total = jnp.sum(jnp.sum(acc[...], axis=1), axis=1, keepdims=True)
    i, j = iotas((16, 128))
    flat = jnp.sum(jnp.where(i == j, total, 0.0), axis=0, keepdims=True)
    nodes = (counts[0, 0] + counts[0, 1]).astype(F32)
    _, lane1 = iotas((1, 128))
    stats[...] = jnp.broadcast_to(jnp.where(lane1 == 14, nodes, flat), (128, 128))


ROOM = 36 << 20


def on_chip(*xs):
    return [pltpu.with_memory_space_constraint(x, pltpu.VMEM) for x in xs]


def local_pass(snapshots, basis, counts):
    vm = pl.BlockSpec(memory_space=pltpu.VMEM)
    hbm = pl.BlockSpec(memory_space=pl.ANY)
    return pl.pallas_call(
        local_kernel,
        in_specs=[pl.BlockSpec(memory_space=pltpu.SMEM), hbm, hbm],
        out_specs=[vm, vm, vm],
        out_shape=[
            pltpu.VMEM((NVAR, R, K), F32),
            pltpu.VMEM((NVAR, R, K), F32),
            pltpu.VMEM((128, 128), F32),
        ],
        scratch_shapes=[
            pltpu.VMEM((COLS * NVAR, R, SLOTS), BF),
            pltpu.VMEM((COLS * NVAR, SLOTS, K), BF),
            pltpu.VMEM((COLS * NVAR, R, K), F32),
            pltpu.VMEM((16, 8, 128), F32),
            pltpu.SemaphoreType.DMA((COLS * NVAR,)),
            pltpu.SemaphoreType.DMA((COLS * NVAR, CUTS)),
        ],
        compiler_params=pltpu.CompilerParams(vmem_limit_bytes=ROOM),
        name="local",
    )(*[pltpu.with_memory_space_constraint(x, pltpu.HBM) for x in (counts, basis, snapshots)])


OWN = 328
NQ = 288
MIXED = 312
FUT = OWN
NEAR = 72
LANES = 384


def lane_copy(x, at):
    return jnp.take_along_axis(x, jnp.full((8, 128), at, jnp.int32), axis=1)


def sub_copy(x, j):
    return jnp.broadcast_to(x[j : j + 1, :], (8, 128))


def split3(x):
    h = x.astype(BF)
    r = x - h.astype(F32)
    m = r.astype(BF)
    return h, m, (r - m.astype(F32)).astype(BF)


def dot(a, b):
    return jnp.dot(a, b, preferred_element_type=F32)


def mm(a, b):
    ah, am, al = split3(a)
    bh, bm, bl = split3(b)
    n = b.shape[1]
    w = jnp.concatenate([bh, bm], axis=1)
    p = dot(jnp.concatenate([ah, am], axis=1), jnp.concatenate([w, w], axis=0))
    q = dot(jnp.concatenate([ah, al], axis=1), jnp.concatenate([bl, bh], axis=0))
    return p[:, :n] + (p[:, n:] + q)


def mm_thirds(a, b):
    bh, bm, bl = split3(b)
    n = b.shape[1]
    w = jnp.concatenate([bh, bm], axis=1)
    p = dot(a[0], w)
    q = dot(a[1], w)
    r = dot(a[0], bl) + dot(a[2], bh)
    return p[:, :n] + ((p[:, n:] + q[:, :n]) + (q[:, n:] + r))


def first_lanes(x):
    return jnp.where(iotas(x.shape)[1] < NEAR, x, 0.0)


def to_rows(x, rows):
    return jnp.concatenate([x, jnp.zeros((rows - x.shape[0], x.shape[1]), F32)], axis=0)


def tree(terms):
    while len(terms) > 1:
        terms = [terms[i] + terms[i + 1] for i in range(0, len(terms) - 1, 2)] + terms[len(terms) // 2 * 2 :]
    return terms[0]


def padded_dot(a, w, lo):
    ah, am, al = split3(a)
    n = w.shape[0]
    parts = [jnp.zeros((lo, 128), F32)] * (lo > 0) + [w] + [jnp.zeros((128 - lo - n, 128), F32)] * (lo + n < 128)
    wh, wm, wl = split3(jnp.concatenate(parts, axis=0) if len(parts) > 1 else w)
    pair = jnp.concatenate([wh, wm], axis=1)
    u = dot(jnp.concatenate([ah, am], axis=1), jnp.concatenate([pair, pair], axis=0))
    v = dot(jnp.concatenate([ah, al], axis=1), jnp.concatenate([wl, wh], axis=0))
    return u[:, :128] + (u[:, 128:] + v)


def pivots(col, riders, sub):
    recips = jnp.zeros((8, 128), F32)
    diag = sub_copy(col[0], 0)
    for j in range(8):
        r = 1.0 / diag
        bare = jnp.where(sub == j, 0.0, col[j])
        recips = jnp.where(sub == j, r, recips)
        heads = {k: sub_copy(col[k], j) for k in range(j + 1, 8)}
        if j < 7:
            diag = sub_copy(col[j + 1], j + 1) - (sub_copy(col[j], j + 1) * heads[j + 1]) * r
        mult = bare * r
        for k in range(j + 1, 8):
            col[k] = col[k] - mult * heads[k]
        riders = [x - mult * sub_copy(x, j) for x in riders]
    return [x * recips for x in riders]


def invert(block, tiles, strip=2, look=1):
    sub, lane = iotas((8, 128))
    for s in range(0, tiles, strip):
        own = list(range(s, min(s + strip, tiles)))
        ahead = list(range(s + strip, min(s + strip + look, tiles)))
        for p in own:
            base = 8 * p
            inside = (lane >= base) & (lane < base + 8)
            unit = jnp.where(lane - base == sub, 1.0, 0.0)
            ws = []
            for m in range(COLS):
                tile = block[m, base : base + 8, :]
                col = [lane_copy(tile, base + k) for k in range(8)]
                w = pivots(col, [jnp.where(inside, unit, tile)], sub)[0]
                block[m, base : base + 8, :] = w
                ws.append([sub_copy(w, j) for j in range(8)])
            for t in [t for t in own + ahead if t > p] + [t for t in own if t < p]:
                for m in range(COLS):
                    a = block[m, 8 * t : 8 * t + 8, :]
                    delta = tree([lane_copy(a, base + j) * ws[m][j] for j in range(8)])
                    block[m, 8 * t : 8 * t + 8, :] = jnp.where(inside, 0.0, a) - delta
            yield
        lo, hi = 8 * s, 8 * (own[-1] + 1)
        ranges = [(a, b) for a, b in ((hi + 8 * len(ahead), 8 * tiles), (0, lo)) if a < b]
        if ranges:
            for m in range(COLS):
                rest = [block[m, a:b, :] for a, b in ranges]
                rest = jnp.concatenate(rest, axis=0) if len(rest) > 1 else rest[0]
                _, wide_l = iotas(rest.shape)
                kept = jnp.where((wide_l >= lo) & (wide_l < hi), 0.0, rest)
                new = kept - padded_dot(rest, block[m, lo:hi, :], lo)
                at = 0
                for a, b in ranges:
                    block[m, a:b, :] = new[at : at + b - a]
                    at += b - a


def spread(panels, count, work):
    work = list(work)
    done = 0
    for i, _ in enumerate(panels):
        want = (i + 1) * len(work) // count if i + 1 < count else len(work)
        while done < min(want, len(work)):
            work[done]()
            done += 1
    for f in work[done:]:
        f()


def states_kernel(everyone, left, proj0, proj1, right, mid, gnorm):
    found = global_scales(everyone)
    gnorm[...] = jnp.broadcast_to(found[NVAR], (8, 128))
    inv = [x[:, 0:1] for x in found]
    for c, proj in enumerate((left, proj0, proj1, right)):
        mid[c] = scaled_sum(proj, inv)


def global_states(everyone, left, proj0, proj1, right):
    return pl.pallas_call(
        states_kernel,
        out_shape=[pltpu.VMEM((4, R, K), F32), pltpu.VMEM((8, 128), F32)],
        compiler_params=pltpu.CompilerParams(vmem_limit_bytes=ROOM),
        name="states",
    )(*on_chip(everyone, left, proj0, proj1, right))


def own_features(feats, twice, m, state, keep):
    past = jnp.where(keep, state, 0.0)
    twice[m, 0:R] = past
    twice[m, R : 2 * R] = past
    for d in range(12):
        feats(R * d, past * twice[m, d : d + R])
    feats(NQ, past)
    row, lane = iotas((16, K))
    one = jnp.where((row == 12) & (lane < K - 1), 1.0, 0.0)
    feats(MIXED, jnp.where(row < 12, twice[m, 0:16] * twice[m, 12:28], one))
    feats(FUT, pltpu.roll(state, K - 1, 1))


def global_scales(everyone):
    total = jnp.sum(everyone[...], axis=0, keepdims=True)
    nodes = total[:, 14:15]
    inv = []
    for v in range(NVAR):
        inv.append(1.0 / jnp.sqrt(total[:, v : v + 1] / (nodes * K) + 1e-06))
    g = jnp.zeros((1, 1), F32)
    q = NVAR
    for a in range(NVAR):
        for b in range(a, NVAR):
            term = total[:, q : q + 1] * inv[a] * inv[b]
            g = g + (term if a == b else 2.0 * term)
            q += 1
    return [jnp.broadcast_to(x, (1, 128)) for x in inv + [g * (1.0 / (256 * R * K))]]


def scaled_sum(proj, inv):
    t = proj[0] * inv[0]
    for v in range(1, NVAR):
        t = t + proj[v] * inv[v]
    return t


def ridge(g):
    return K * (HALF * g), K * (HALF * g * g)


def past_mask():
    return lax.broadcasted_iota(jnp.int32, (R, K), 1) < K - 1


def nt(a, b):
    return lax.dot_general(a, b, (((1,), (1,)), ((), ())), preferred_element_type=F32)


def own_kernel(gnorm, mid, fh, fm, fl, h, block, twice):
    keep = past_mask()
    for m in range(COLS):

        def put(at, x, m=m):
            n = x.shape[0]
            fh[m, at : at + n], fm[m, at : at + n], fl[m, at : at + n] = split3(x)

        own_features(put, twice, m, mid[1 + m], keep)
    lin, quad = ridge(gnorm[0:1])
    sub, lane = iotas((8, 128))

    def thirds(m, lo, hi):
        return [f[m, lo:hi] for f in (fh, fm, fl)]

    def gram(m, r0, r1, c0, c1):
        want = r1 - r0
        size = -(-want // 16) * 16
        a, b = thirds(m, r0, r0 + size), thirds(m, c0, c1)
        n = c1 - c0
        top, mid, low = slice(0, size), slice(size, 2 * size), slice(2 * size, 3 * size)
        if n > 128:
            x = nt(jnp.concatenate(a, axis=0), b[0])
            y = nt(jnp.concatenate(a[:2], axis=0), b[1])
            g = (((y[mid] + nt(a[0], b[2])) + x[low]) + (y[top] + x[mid])) + x[top]
            return g[0:want]
        gap = [jnp.zeros((128 - n, K), BF)] * (n < 128)
        pair = jnp.concatenate([b[0]] + gap + [b[1]] + gap, axis=0)
        p = nt(jnp.concatenate(a[:2], axis=0), pair)
        r = nt(a[0], b[2]) + nt(a[2], b[0])
        one, two = slice(0, n), slice(128, 128 + n)
        g = p[top, one] + ((p[top, two] + p[mid, one]) + (p[mid, two] + r))
        return g[0:want]

    def reg(row):
        if row < NQ or row == MIXED:
            return quad
        if row == MIXED + 8:
            return jnp.where(sub < 4, quad, jnp.where(sub == 4, lin, 1.0))
        return lin

    def ridged(x, row0):
        tiles = []
        for i in range(x.shape[0] // 8):
            tiles.append(x[8 * i : 8 * i + 8] + jnp.where(lane == sub + 8 * i, reg(row0 + 8 * i), 0.0))
        return jnp.concatenate(tiles, axis=0)

    for m in range(COLS):
        block[m] = ridged(gram(m, 0, 128, 0, 128), 0)

    def piece(m, kind):
        def go():
            if kind == 0:
                h[m, 0:128, 256:LANES] = jnp.zeros((128, 128), F32)
                h[m, 0:128, 128 : OWN + R] = gram(m, 0, 128, 128, OWN + R)
            elif kind == 1:
                g = gram(m, 128, OWN, 0, 256)
                h[m, 128:256, 0:128] = g[0:128, 0:128]
                h[m, 128:256, 128:256] = ridged(g[0:128, 128:256], 128)
                h[m, 256:OWN, 0:256] = g[128:]
            else:
                h[m, 128:OWN, 256:LANES] = jnp.zeros((OWN - 128, 128), F32)
                h[m, 128:OWN, 256 : OWN + R] = gram(m, 128, OWN, 256, OWN + R)
                h[m, 256:OWN, 256:LANES] = ridged(h[m, 256:OWN, 256:LANES], 256)

        return go

    spread(invert(block, 16), 14, [piece(m, k) for k in range(2) for m in range(COLS)])
    inv0 = [block[m] for m in range(COLS)]
    for m in range(COLS):
        w = mm(inv0[m], h[m, 0:128, 128:256])
        block[m] = h[m, 128:256, 128:256] - mm(h[m, 128:256, 0:128], w)
        h[m, 0:128, 128:256] = w
        h[m, 0:128, 0:128] = inv0[m]

    def after0(m, kind):
        def go():
            if kind == 0:
                h[m, 0:128, 256:LANES] = mm(h[m, 0:128, 0:128], h[m, 0:128, 256:LANES])
            elif kind == 1:
                rows = slice(128, OWN)
                h[m, rows, 256:LANES] -= mm(h[m, rows, 0:128], h[m, 0:128, 256:LANES])
            elif kind == 2:
                rows = slice(256, OWN)
                h[m, rows, 128:256] -= mm(h[m, rows, 0:128], h[m, 0:128, 128:256])
            else:
                rows = slice(128, OWN)
                h[m, rows, 0:128] = -mm(h[m, rows, 0:128], h[m, 0:128, 0:128])

        return go

    late = [piece(m, 2) for m in range(COLS)]
    spread(invert(block, 16), 14, late + [after0(m, k) for k in range(4) for m in range(COLS)])


def fit_own(gnorm, mid):
    return pl.pallas_call(
        own_kernel,
        out_shape=[pltpu.VMEM((COLS, OWN + R, K), BF)] * 3
        + [pltpu.VMEM((COLS, OWN, LANES), F32), pltpu.VMEM((COLS, 128, 128), F32)],
        scratch_shapes=[pltpu.VMEM((COLS, 2 * R, K), F32)],
        compiler_params=pltpu.CompilerParams(vmem_limit_bytes=ROOM),
        name="fit_own",
    )(*on_chip(gnorm, mid))


def near_kernel(
    adjacency, gnorm, mid, up, down, fh, fm, fl, h_in, block_in, out, own,
    links, patch, h, block, nb, cross, turned, x, order, flat_out, sem, own_sem, out_sems,
):
    fetch = pltpu.make_async_copy(adjacency, links, sem)
    fetch.start()
    save = pltpu.make_async_copy(mid.at[pl.ds(1, COLS)], own, own_sem)
    save.start()
    row0 = lax.axis_index("gx_0") * 4 + lax.axis_index("gx_1")
    col0 = (lax.axis_index("gy_0") * 2 + lax.axis_index("gy_1")) * COLS
    keep = past_mask()
    lin, _ = ridge(gnorm[0:1])
    sub, lane = iotas((8, 128))
    for m in range(COLS):
        w = mm(block_in[m], h_in[m, 128:256, 256:LANES])
        block[m, 0:NEAR] = h_in[m, 256:OWN, 256:LANES] - mm(h_in[m, 256:OWN, 128:256], w)
        h[m, 128:256, 256:LANES] = w
        h[m, 128:256, 128:256] = block_in[m]
        h[m, 128:256, 0:128] = h_in[m, 128:256, 0:128]
        h[m, 0:128] = h_in[m, 0:128]
        h[m, 256:OWN] = h_in[m, 256:OWN]
    for c in range(4):
        for r, source in enumerate((up, mid, down)):
            patch[4 * r + c] = jnp.where(keep, source[c], 0.0)
    gap = jnp.zeros((128 - NEAR, K), F32)

    def select(m):
        def go():
            if m == 0:
                fetch.wait()
            rows = []
            for b in range(NB):
                link = links[0, m, b]
                rows.append(patch[((link >> 4) - row0 + 1) * 4 + ((link & 15) - col0 + 1)])
            nb[m, 0:128], nb[m, 128:256], nb[m, 256:384] = split3(jnp.concatenate(rows + [gap], axis=0))

        return go

    def after1(m, kind):
        def go():
            if kind == 0:
                h[m, 128:256, 0:128] = mm(h[m, 128:256, 128:256], h[m, 128:256, 0:128])
            elif kind == 1:
                h[m, 0:128, 256:LANES] -= mm(h[m, 0:128, 128:256], h[m, 128:256, 256:LANES])
            elif kind == 2:
                for rows in (slice(0, 128), slice(256, OWN)):
                    h[m, rows, 0:128] -= mm(h[m, rows, 128:256], h[m, 128:256, 0:128])
            else:
                for rows in (slice(0, 128), slice(256, OWN)):
                    h[m, rows, 128:256] = -mm(h[m, rows, 128:256], h[m, 128:256, 128:256])

        return go

    def near_products(m, part):
        def go():
            nh, nm, nl = (nb[m, 128 * i : 128 * i + 128] for i in range(3))
            if part == 0:
                a = [f[m, 0:176] for f in (fh, fm, fl)]
            else:
                pieces = ((fh, nh), (fm, nm), (fl, nl))
                a = [jnp.concatenate([f[m, 176 : OWN + R], n[0:80]], axis=0) for f, n in pieces]
            size = a[0].shape[0]
            p = nt(jnp.concatenate(a[:2], axis=0), nb[m, 0:256])
            r = nt(a[0], nl) + nt(a[2], nh)
            top, low = slice(0, size), slice(size, 2 * size)
            g = p[top, 0:128] + ((p[top, 128:256] + p[low, 0:128]) + (p[low, 128:256] + r))
            cross[m, 176 * part : 176 * part + size] = g

        return go

    def turn(m):
        def go():
            turned[m] = to_rows(cross[m, 0 : OWN + R], LANES).T[0:NEAR]

        return go

    def near_columns(m):
        def go():
            g = mm_thirds(split3(h[m, :, 0:256]), cross[m, 0:256])
            x[m, 0:256] = g[0:256]
            x[m, 256:OWN] = cross[m, 256:OWN] + g[256:OWN]

        return go

    both = range(COLS)
    work = [after1(m, k) for k in (0, 1) for m in both] + [select(m) for m in both]
    work += [near_products(m, 0) for m in both] + [after1(m, 2) for m in both]
    work += [near_products(m, 1) for m in both] + [after1(m, 3) for m in both]
    work += [turn(m) for m in both] + [near_columns(m) for m in both]
    spread(invert(block, 9), 8, work)
    _, wide = iotas((256, 128))
    _, lane_n = iotas((NEAR, 128))
    for m in range(COLS):
        last = block[m, 0:NEAR]
        low = jnp.where(lane_n < NEAR, mm(first_lanes(last), to_rows(x[m, 256:OWN], 128)), last)
        part = h[m, 0:256, 256:LANES]
        top = jnp.where(wide < NEAR, x[m, 0:256], part) - mm(first_lanes(part), to_rows(low, 128))
        both = jnp.concatenate([top, low], axis=0)
        x[m] = both
        start = jnp.where(lane_n < NEAR, cross[m, OWN + R : OWN + R + NEAR], turned[m, :, 256:LANES])
        start = jnp.where(lane_n < NEAR + R, start, 0.0)
        start = jnp.concatenate(
            [start[8 * i : 8 * i + 8] + jnp.where(lane == sub + 8 * i, lin, 0.0) for i in range(NEAR // 8)], axis=0
        )
        flat = jnp.where(iotas((NEAR, LANES))[1] < OWN, turned[m], 0.0)
        block[m, 0:NEAR] = start - mm_thirds(split3(flat), to_rows(both, LANES))
    for _ in invert(block, 9):
        pass
    for m in range(COLS):
        last = block[m, 0:NEAR]
        both = x[m, 0:OWN]
        x[m, 0:OWN] = both - mm(first_lanes(both), to_rows(last, 128))
        order[m, 0:1] = x[m, MIXED + 12 : MIXED + 13]
        order[m, 1:25] = x[m, NQ : NQ + R]
        order[m, 25:97] = last
        dst = 97
        for a in range(R):
            near_count = min(12, R - a)
            order[m, dst : dst + near_count] = x[m, pl.ds(a, near_count, stride=R), :]
            dst += near_count
            for b in range(a + 12, R):
                src = MIXED + a if b - a == 12 else R * (R - b + a) + b
                order[m, dst : dst + 1] = x[m, src : src + 1]
                dst += 1
        flat_out[m] = order[m].T[NEAR : NEAR + R, 0:NF]
        pltpu.make_async_copy(flat_out.at[m], out.at[m], out_sems.at[m]).start()
    for m in range(COLS):
        pltpu.make_async_copy(flat_out.at[m], out.at[m], out_sems.at[m]).wait()
    save.wait()


def fit_near(adjacency, *rest):
    vm = pl.BlockSpec(memory_space=pltpu.VMEM)
    return pl.pallas_call(
        near_kernel,
        in_specs=[pl.BlockSpec(memory_space=pl.ANY)] + [vm] * len(rest),
        out_specs=[pl.BlockSpec(memory_space=pl.ANY)] * 2,
        out_shape=[
            jax.ShapeDtypeStruct((COLS, R, NF), F32),
            jax.ShapeDtypeStruct((COLS, R, K), F32),
        ],
        scratch_shapes=[
            pltpu.SMEM((1, COLS, NB), jnp.int32),
            pltpu.VMEM((12, R, K), F32),
            pltpu.VMEM((COLS, OWN, LANES), F32),
            pltpu.VMEM((COLS, 128, 128), F32),
            pltpu.VMEM((COLS, 384, K), BF),
            pltpu.VMEM((COLS, OWN + R + 80, 128), F32),
            pltpu.VMEM((COLS, NEAR, LANES), F32),
            pltpu.VMEM((COLS, OWN, 128), F32),
            pltpu.VMEM((COLS, 512, 128), F32),
            pltpu.VMEM((COLS, R, NF), F32),
            pltpu.SemaphoreType.DMA,
            pltpu.SemaphoreType.DMA,
            pltpu.SemaphoreType.DMA((COLS,)),
        ],
        compiler_params=pltpu.CompilerParams(vmem_limit_bytes=ROOM),
        name="fit_near",
    )(pltpu.with_memory_space_constraint(adjacency, pltpu.HBM), *on_chip(*rest))


def shifts(axis, x, y):
    n = lax.axis_size(axis)
    return (
        lax.ppermute(x, axis, [(i, i + 1) for i in range(n - 1)]),
        lax.ppermute(y, axis, [(i + 1, i) for i in range(n - 1)]),
    )


def body(snapshots, basis, node_counts, adjacency):
    proj0, proj1, stats = local_pass(snapshots[0], basis[0], node_counts)
    everyone = lax.all_to_all(stats, GX_GY, 0, 0, tiled=True)
    left, right = shifts(GY, proj1, proj0)
    mid, gnorm = global_states(everyone, left, proj0, proj1, right)
    up, down = shifts(GX, mid, mid)
    parts = fit_own(gnorm, mid)
    operator, own = fit_near(adjacency, gnorm, mid, up, down, *parts)
    return (jnp.swapaxes(operator, 1, 2)[None], own[None])


def solution(mesh):
    split = Mesh(mesh.devices.reshape(4, 4, 4, 2), ("gx_0", "gx_1", "gy_0", "gy_1"))
    placed = (P(GX, GY, None, None, None), P(GX, GY, None, None, None), P(GX, GY), P(GX, GY, None))
    return jax.shard_map(
        body,
        mesh=split,
        in_specs=placed,
        out_specs=(P(GX, GY, None, None), P(GX, GY, None, None)),
        check_vma=False,
    )
```
